8 devices in a mesh: slab: 1 (over z), coil: 2 (over y), rows: 4 (over x, core).
Axes of the slice: x: 2, y: 2, z: 1, core: 2. Of those that a mesh axis runs over, the one named last changes fastest.
Arguments:
- kspace: float32 [2, 16, 20480], P(None, 'coil', ('slab', 'rows'))
- weight_row: float32 [4, 20480], P(None, ('slab', 'rows'))
- weight_col: float32 [4, 20480], P(None, ('slab', 'rows'))
- grid_row: int32 [20480], P(('slab', 'rows'))
- grid_col: int32 [20480], P(('slab', 'rows'))
- valid_count: int32 [4], P(('slab', 'rows'))
- coil_maps: float32 [2, 16, 320, 320], P(None, 'coil', 'slab', 'rows')
- deapod: float32 [320], replicated
Outputs:
- output: float32 [2, 320, 320], P(None, ('slab', 'coil'), 'rows')
All inputs are finite; a program needn't handle non-finite values.
Results may differ from the reference program's by a relative error of at most 0.001.
Values are sent between devices in bfloat16 or wider.
A program may use at most 1 GiB of HBM per device.

```python
import math
import jax
import jax.numpy as jnp
from jax import lax

IMAGE_SIZE = 320
KERNEL_WIDTH = 4
NUM_COILS = 16
ROW_BLOCKS = 4
PER_BLOCK = 5120

GRID_SIZE = 2 * IMAGE_SIZE
HALF_WIDTH = KERNEL_WIDTH // 2
BLOCK_ROWS = GRID_SIZE // ROW_BLOCKS
SAMPLES = ROW_BLOCKS * PER_BLOCK


def draw_layout(layout_key):
    key_count, key_short, key_ra, key_rb, key_ca, key_cb, key_sign = jax.random.split(layout_key, 7)
    blocks = jnp.arange(ROW_BLOCKS)
    centre_block = ROW_BLOCKS // 2
    low_counts = jax.random.randint(key_count, (ROW_BLOCKS,), PER_BLOCK // 8, PER_BLOCK // 2 + 1)
    short_by = jax.random.randint(key_short, (), 0, PER_BLOCK // 4 + 1)
    counts = jnp.where(blocks == centre_block, PER_BLOCK, jnp.where(blocks == centre_block - 1, PER_BLOCK - short_by, low_counts))
    row_depth = (jax.random.randint(key_ra, (ROW_BLOCKS, PER_BLOCK), 0, BLOCK_ROWS) * jax.random.randint(key_rb, (ROW_BLOCKS, PER_BLOCK), 0, BLOCK_ROWS)) // BLOCK_ROWS
    upper_half = blocks >= centre_block
    edge_row = jnp.where(upper_half, blocks * BLOCK_ROWS, (blocks + 1) * BLOCK_ROWS - 1)
    direction = jnp.where(upper_half, 1, -1)
    grid_row = (edge_row[:, None] + direction[:, None] * row_depth).reshape(SAMPLES)
    spread_col = (jax.random.randint(key_ca, (SAMPLES,), 0, IMAGE_SIZE) * jax.random.randint(key_cb, (SAMPLES,), 0, IMAGE_SIZE)) // IMAGE_SIZE
    col_sign = 2 * jax.random.randint(key_sign, (SAMPLES,), 0, 2) - 1
    grid_col = jnp.mod(IMAGE_SIZE + col_sign * spread_col, GRID_SIZE)
    return counts.astype(jnp.int32), grid_row.astype(jnp.int32), grid_col.astype(jnp.int32)


def kernel_weights(weight_key):
    tap_pos = jnp.arange(KERNEL_WIDTH, dtype=jnp.float32) - (KERNEL_WIDTH - 1) / 2.0
    profile = jnp.exp(-(tap_pos / (0.35 * KERNEL_WIDTH)) ** 2)
    jitter = jax.random.uniform(weight_key, (KERNEL_WIDTH, SAMPLES), jnp.float32, 0.5, 1.5)
    return (profile / jnp.sum(profile))[:, None] * jitter


def draw_maps(map_key):
    key_angle, key_phase, key_grad_y, key_grad_x, key_noise = jax.random.split(map_key, 5)
    pixel_pos = (jnp.arange(IMAGE_SIZE, dtype=jnp.float32) - IMAGE_SIZE // 2) / IMAGE_SIZE
    coil_angle = 2.0 * math.pi * (jnp.arange(NUM_COILS, dtype=jnp.float32) + jax.random.uniform(key_angle, (NUM_COILS,), jnp.float32)) / NUM_COILS
    centre_y = 0.6 * jnp.cos(coil_angle)
    centre_x = 0.6 * jnp.sin(coil_angle)
    dist_sq = (pixel_pos[None, :, None] - centre_y[:, None, None]) ** 2 + (pixel_pos[None, None, :] - centre_x[:, None, None]) ** 2
    magnitude = jnp.exp(-dist_sq / 0.4) * (1.0 + 0.1 * jax.random.normal(key_noise, (NUM_COILS, IMAGE_SIZE, IMAGE_SIZE), jnp.float32))
    grad_y = jax.random.uniform(key_grad_y, (NUM_COILS,), jnp.float32, -1.0, 1.0)
    grad_x = jax.random.uniform(key_grad_x, (NUM_COILS,), jnp.float32, -1.0, 1.0)
    base_phase = 2.0 * math.pi * jax.random.uniform(key_phase, (NUM_COILS,), jnp.float32)
    coil_phase = base_phase[:, None, None] + math.pi * (grad_y[:, None, None] * pixel_pos[None, :, None] + grad_x[:, None, None] * pixel_pos[None, None, :])
    return jnp.stack([magnitude * jnp.cos(coil_phase), magnitude * jnp.sin(coil_phase)])


def setup_inputs(seed: int = 0, part: int = 0) -> dict:
    base_key = jax.random.key(seed)
    shared_key, root_key = jax.random.split(base_key)
    part_key = jax.random.fold_in(root_key, part)
    key_layout, key_y, key_wr, key_wc, key_map = jax.random.split(part_key, 5)
    valid_count, grid_row, grid_col = draw_layout(key_layout)
    centre_dist = (jnp.abs(grid_row - IMAGE_SIZE) + jnp.abs(grid_col - IMAGE_SIZE)).astype(jnp.float32) / GRID_SIZE
    amplitude = 1.0 / (1.0 + 8.0 * centre_dist)
    kspace = jax.random.normal(key_y, (2, NUM_COILS, SAMPLES), jnp.float32) * amplitude[None, None, :] * (3.0 / math.sqrt(NUM_COILS * SAMPLES))
    pixel_pos = (jnp.arange(IMAGE_SIZE, dtype=jnp.float32) - IMAGE_SIZE // 2) / IMAGE_SIZE
    deapod = (1.0 + 2.0 * pixel_pos * pixel_pos) * jax.random.uniform(shared_key, (IMAGE_SIZE,), jnp.float32, 0.8, 1.2)
    return dict(kspace=kspace, weight_row=kernel_weights(key_wr), weight_col=kernel_weights(key_wc), grid_row=grid_row, grid_col=grid_col, valid_count=valid_count, coil_maps=draw_maps(key_map), deapod=deapod)


def make_table():
    freq_index = jnp.arange(GRID_SIZE, dtype=jnp.int32) - IMAGE_SIZE
    pixel_index = jnp.arange(IMAGE_SIZE, dtype=jnp.int32) - IMAGE_SIZE // 2
    angle_grid = jnp.mod(freq_index[:, None] * pixel_index[None, :], GRID_SIZE).astype(jnp.float32) * (2.0 * math.pi / GRID_SIZE)
    cos_part = jnp.cos(angle_grid)
    sin_part = jnp.sin(angle_grid)
    return jnp.stack([jnp.stack([cos_part, sin_part], axis=1), jnp.stack([-sin_part, cos_part], axis=1)], axis=0).astype(jnp.bfloat16)


def reference(kspace, weight_row, weight_col, grid_row, grid_col, valid_count, coil_maps, deapod):
    slot_index = jnp.tile(jnp.arange(PER_BLOCK), ROW_BLOCKS)
    keep_mask = (slot_index < jnp.repeat(valid_count, PER_BLOCK)).astype(jnp.float32)
    row_coef = (kspace[:, :, None, :] * (weight_row * keep_mask)[None, None, :, :]).astype(jnp.bfloat16).astype(jnp.float32)
    col_coef = weight_col.astype(jnp.bfloat16).astype(jnp.float32)
    dft_table = make_table().astype(jnp.float32)
    offsets = jnp.arange(KERNEL_WIDTH * KERNEL_WIDTH)

    def one_coil(coil_args):
        coil_coef, coil_map = coil_args

        def add_offset(flat_grid, offset):
            row_off = offset // KERNEL_WIDTH
            col_off = offset % KERNEL_WIDTH
            row_index = jnp.mod(grid_row + row_off - HALF_WIDTH, GRID_SIZE)
            col_index = jnp.mod(grid_col + col_off - HALF_WIDTH, GRID_SIZE)
            contrib = lax.dynamic_index_in_dim(coil_coef, row_off, axis=1, keepdims=False) * lax.dynamic_index_in_dim(col_coef, col_off, axis=0, keepdims=False)[None, :]
            flat_grid = flat_grid + jax.ops.segment_sum(contrib.T, row_index * GRID_SIZE + col_index, num_segments=GRID_SIZE * GRID_SIZE)
            return flat_grid, None

        flat_grid = lax.scan(add_offset, jnp.zeros((GRID_SIZE * GRID_SIZE, 2), jnp.float32), offsets)[0]
        grid_bf = flat_grid.T.reshape(2, GRID_SIZE, GRID_SIZE).astype(jnp.bfloat16).astype(jnp.float32)
        half_image = jnp.einsum('qyk,qkbj->byj', grid_bf, dft_table).astype(jnp.bfloat16).astype(jnp.float32)
        coil_image = jnp.einsum('byj,byei->eij', half_image, dft_table)
        real_part = coil_map[0] * coil_image[0] + coil_map[1] * coil_image[1]
        imag_part = coil_map[0] * coil_image[1] - coil_map[1] * coil_image[0]
        return jnp.stack([real_part, imag_part])

    per_coil = lax.map(one_coil, (jnp.swapaxes(row_coef, 0, 1), jnp.swapaxes(coil_maps, 0, 1)))
    return jnp.sum(per_coil, axis=0) * (deapod[:, None] * deapod[None, :])[None]
```

```python
import functools
import numpy as np
import jax
import jax.numpy as jnp
from jax import lax
from jax.experimental import pallas as pl
from jax.experimental.pallas import tpu as pltpu
from jax.sharding import PartitionSpec as P

MESH = pl.DeviceIdType.MESH
BF = jnp.bfloat16
F32 = jnp.float32

N_IMG = 320
N_GRID = 640
ROWS = 4
BLK = 160
COLS = 80
NC = 8
SLOTS = 5120
KC = 1280
NK = SLOTS // KC
LANES = 384
B_FIRST = 64
B_ROWS = 32


def row_order():
    pos = np.arange(128)
    rows = pos + np.where(pos >= B_FIRST, B_ROWS, 0)
    rows[126], rows[16] = 16, 158
    rows[127], rows[32] = 32, 159
    return rows


def constants():
    k = np.arange(N_GRID)
    j = np.arange(N_IMG)
    ang = np.mod((k[:, None] - N_IMG) * (j[None, :] - N_IMG // 2), N_GRID) * (2.0 * np.pi / N_GRID)
    cos_t = np.cos(ang)
    sin_t = np.sin(ang)
    lanes = np.full((LANES,), -1)
    lanes[0:N_IMG] = np.arange(N_IMG)
    used = (lanes >= 0)[None, :]
    src = np.maximum(lanes, 0)
    pick = lambda t: np.where(used, t[:, src], 0.0)
    base = np.arange(ROWS)[:, None] * BLK
    ra = (base + row_order()[None, :]).reshape(-1)
    rb = (base + B_FIRST + np.arange(B_ROWS)[None, :]).reshape(-1)
    bf = jnp.bfloat16
    t3a = np.stack([pick(cos_t)[ra], pick(sin_t)[ra]]).reshape(2, ROWS, 128, LANES).astype(bf)
    t3b = np.stack([pick(cos_t)[rb], pick(sin_t)[rb]]).reshape(2, ROWS * B_ROWS, LANES).astype(bf)
    t2 = np.stack([cos_t.T, sin_t.T]).reshape(2, ROWS, COLS, N_GRID).astype(bf)
    return t2, t3a, t3b


def body(y_h, wr_h, wc_h, gr_h, gc_h, vc, s_h, dd_h, t2_h, t3a_h, t3b_h, out_ref,
         y, wr, wc, gr, gc, s_v, dd, rt0, rt1, rt2, rt3, wd, l0, l1, lh, acc, gb, hbuf, recv,
         hs, hr, hrt, t2, t3a, t3b, ib, ia, img, yrecv, ctmp,
         in_sem, t_sem, s_sem, send_sem, recv_sem, hsend_sem, hrecv_sem, ysend_sem, yrecv_sem):
    rts = (rt0, rt1, rt2, rt3)
    lefts = (l0, l1)
    me = lax.axis_index('rows')
    cid = lax.axis_index('coil')
    nxt = lax.rem(me + 1, ROWS)
    prv = lax.rem(me + ROWS - 1, ROWS)
    other = 1 - cid

    barrier = pltpu.get_barrier_semaphore()
    for d in range(1, ROWS):
        pl.semaphore_signal(barrier, inc=1, device_id={'rows': lax.rem(me + d, ROWS)}, device_id_type=MESH)
    pl.semaphore_signal(barrier, inc=1, device_id={'coil': other}, device_id_type=MESH)

    ins = [pltpu.make_async_copy(a, b, in_sem.at[n]) for n, (a, b) in enumerate(
        ((gr_h, gr), (gc_h, gc), (wr_h, wr), (wc_h, wc), (y_h, y)))]
    for c in ins:
        c.start()
    tabs = [
        pltpu.make_async_copy(t2_h.at[0], t2.at[:, 0, :, 0:N_GRID], t_sem.at[0]),
        pltpu.make_async_copy(t2_h.at[1], t2.at[:, 1, :, 0:N_GRID], t_sem.at[1]),
        pltpu.make_async_copy(t2_h.at[0], t2.at[:, 1, :, N_GRID:], t_sem.at[2]),
        pltpu.make_async_copy(t3b_h.at[0], t3b.at[0, :, 0:LANES], t_sem.at[3]),
        pltpu.make_async_copy(t3b_h.at[1], t3b.at[0, :, LANES:], t_sem.at[4]),
        pltpu.make_async_copy(t3b_h.at[0], t3b.at[1, :, LANES:], t_sem.at[5]),
        pltpu.make_async_copy(t3a_h.at[0], t3a.at[:, 0, :, 0:LANES], t_sem.at[6]),
        pltpu.make_async_copy(t3a_h.at[1], t3a.at[:, 0, :, LANES:], t_sem.at[7]),
        pltpu.make_async_copy(t3a_h.at[0], t3a.at[:, 1, :, LANES:], t_sem.at[8]),
    ]
    for c in tabs:
        c.start()
    big = [pltpu.make_async_copy(s_h, s_v, s_sem.at[0]), pltpu.make_async_copy(dd_h, dd, s_sem.at[1])]
    for c in big:
        c.start()
    for c in ins:
        c.wait()

    def build_wd(k):
        sl = pl.ds(k * KC, KC)
        ids = lax.broadcasted_iota(jnp.int32, (168, 1), 0)
        r = ids + jnp.where((ids >= B_FIRST) & (ids < 128), B_ROWS, 0)
        r = jnp.where(ids >= 128, ids - 128 + B_FIRST, r)
        for a, b in ((126, 16), (127, 32), (16, 158), (32, 159), (160, BLK), (161, -2), (162, -1)):
            r = jnp.where(ids == a, b, r)
        keep = (lax.broadcasted_iota(jnp.int32, (1, KC), 1) + k * KC < vc[0]).astype(F32)
        first = gr[:, sl] - me * BLK
        w = jnp.zeros((168, KC), F32)
        for a in range(4):
            w = jnp.where(r == first + (a - 2), wr[a:a + 1, sl] * keep, w)
        wd[:, sl] = w

    def build_rt(k):
        sl = pl.ds(k * KC, KC)
        col = gc[:, sl]
        for n in range(5):
            ids = lax.broadcasted_iota(jnp.int32, (128, 1), 0) + n * 128
            w = jnp.zeros((128, KC), F32)
            for b in range(4):
                t = col + (b - 2)
                t = jnp.where(t < 0, t + N_GRID, jnp.where(t >= N_GRID, t - N_GRID, t))
                w = jnp.where(ids == t, wc[b:b + 1, sl], w)
            rts[k][n * 128:(n + 1) * 128, :] = w.astype(BF)

    def build_left_b(k):
        sl = pl.ds(k * KC, KC)
        w = wd[128:160, sl]
        for q in range(2):
            for c in range(NC):
                lefts[k % 2][q * 256 + c * 32:q * 256 + c * 32 + 32, :] = (y[q, c:c + 1, sl] * w).astype(BF)

    def build_halo(k):
        sl = pl.ds(k * KC, KC)
        for h in range(3):
            for q in range(2):
                lh[k, h * 16 + q * 8:h * 16 + q * 8 + 8, :] = (y[q, :, sl] * wd[160 + h:161 + h, sl])

    def build_left_a(s, k):
        sl = pl.ds(k * KC, KC)
        w = wd[0:128, sl]
        for q in range(2):
            for c in range(2):
                lefts[k % 2][q * 256 + c * 128:q * 256 + c * 128 + 128, :] = (y[q, pl.ds(2 * s + c, 1), sl] * w).astype(BF)

    def nt(a, b):
        return lax.dot_general(a, b, (((1,), (1,)), ((), ())), preferred_element_type=F32)

    def spread(k):
        for q in range(2):
            cs = slice(q * 256, q * 256 + 256)
            part = nt(rts[k][...], lefts[k % 2][cs, :])
            if k == 0:
                acc[:, cs] = part
            else:
                acc[:, cs] += part

    def exchange(stage):
        return [pltpu.make_async_remote_copy(
            src_ref=hbuf.at[stage, lax.rem(me + d, ROWS)], dst_ref=recv.at[stage, me],
            send_sem=send_sem.at[stage, d - 1], recv_sem=recv_sem.at[stage, 3 - d],
            device_id={'rows': lax.rem(me + d, ROWS)}, device_id_type=MESH) for d in (1, 2, 3)]

    def received(stage):
        return [pltpu.make_async_remote_copy(
            src_ref=hbuf.at[stage, 0], dst_ref=recv.at[stage, lax.rem(me + d, ROWS)],
            send_sem=send_sem.at[stage, d - 1], recv_sem=recv_sem.at[stage, d - 1],
            device_id={'rows': lax.rem(me + d, ROWS)}, device_id_type=MESH) for d in (1, 2, 3)]

    def transform(stage):
        for n in range(ROWS):
            hbuf[stage, n] = jnp.dot(t2[n].reshape(2 * COLS, 2 * N_GRID), gb[...], preferred_element_type=F32).astype(BF)
        for c in exchange(stage):
            c.start()
        recv[stage, me] = hbuf[stage, me]

    build_wd(0)
    build_rt(0)
    build_left_b(0)
    for k in range(NK):
        spread(k)
        if k + 1 < NK:
            build_wd(k + 1)
            build_rt(k + 1)
            build_left_b(k + 1)
    for q in range(2):
        gb[q * N_GRID:(q + 1) * N_GRID, :] = acc[:, q * 256:q * 256 + 256].astype(BF)
    for c in tabs:
        c.wait()
    t2[:, 0, :, N_GRID:] = -t2[:, 1, :, 0:N_GRID]
    t3b[1, :, 0:LANES] = -t3b[0, :, LANES:]
    t3a[:, 1, :, 0:LANES] = -t3a[:, 0, :, LANES:]
    pl.semaphore_wait(barrier, 4)
    transform(0)

    for k in range(NK):
        build_halo(k)
    halo = jnp.zeros((N_GRID, 48), F32)
    for k in range(NK):
        halo = halo + nt(rts[k][...], lh[k].astype(BF))
    hs[...] = halo.T
    to_next = pltpu.make_async_remote_copy(
        src_ref=hs.at[0:16], dst_ref=hr.at[0:16], send_sem=hsend_sem.at[0], recv_sem=hrecv_sem.at[0],
        device_id={'rows': nxt}, device_id_type=MESH)
    to_prev = pltpu.make_async_remote_copy(
        src_ref=hs.at[16:48], dst_ref=hr.at[16:48], send_sem=hsend_sem.at[1], recv_sem=hrecv_sem.at[1],
        device_id={'rows': prv}, device_id_type=MESH)
    to_next.start()
    to_prev.start()
    big[0].wait()
    big[1].wait()
    build_left_a(0, 0)

    def image_first():
        for c in received(0):
            c.wait_recv()
        for c in range(NC):
            lo = (c // 4) * 128
            parts = []
            for b in range(2):
                for p in range(ROWS):
                    parts.append(recv[0, p, b * COLS:(b + 1) * COLS, c * 32:c * 32 + 32])
            lhs = jnp.concatenate(parts, axis=1)
            ib[c] = jnp.dot(lhs, t3b[...].reshape(256, 2 * LANES), preferred_element_type=F32)

    def image_coils(s):
        stage = s + 1
        for c in received(stage):
            c.wait_recv()
        for c in range(2):
            tot = ib[2 * s + c]
            for p in range(ROWS):
                lhs = jnp.concatenate([recv[stage, p, b * COLS:(b + 1) * COLS, c * 128:c * 128 + 128] for b in range(2)], axis=1)
                tot = tot + jnp.dot(lhs, t3a[p].reshape(256, 2 * LANES), preferred_element_type=F32)
            ia[c] = tot
        for c in range(2):
            sr = s_v[0, 2 * s + c]
            si = s_v[1, 2 * s + c]
            re = ia[c, :, 0:N_IMG]
            im = ia[c, :, LANES:LANES + N_IMG]
            img[0, :, 0:N_IMG] += sr * re + si * im
            img[1, :, 0:N_IMG] += sr * im - si * re

    img[...] = jnp.zeros_like(img)

    @pl.loop(0, NC // 2)
    def _(s):
        for k in range(NK):
            spread(k)
            build_left_a(jnp.minimum(s + 1, NC // 2 - 1) if k + 1 == NK else s, (k + 1) % NK)

        @pl.when(s == 0)
        def _():
            to_next.wait()
            to_prev.wait()
            hrt[...] = jnp.concatenate([hr[...], jnp.zeros((80, N_GRID), F32)], axis=0).T

        lane = lax.broadcasted_iota(jnp.int32, (1, 128), 1)
        edge = (lane == 0) | (lane == 16) | (lane == 32)
        for q in range(2):
            for c in range(2):
                rolled = pltpu.roll(hrt[...], 128 - (q * 8 + 2 * s + c), 1)
                cs = slice(q * 256 + c * 128, q * 256 + c * 128 + 128)
                gb[q * N_GRID:(q + 1) * N_GRID, c * 128:c * 128 + 128] = (acc[:, cs] + jnp.where(edge, rolled, 0.0)).astype(BF)
        transform(s + 1)

        @pl.when(s == 0)
        def _():
            image_first()

        @pl.when(s > 0)
        def _():
            image_coils(s - 1)

    image_coils(NC // 2 - 1)

    sends = [pltpu.make_async_remote_copy(
        src_ref=img.at[e, :, pl.ds(pl.multiple_of(other * 128, 128), 256)], dst_ref=yrecv.at[e],
        send_sem=ysend_sem.at[e], recv_sem=yrecv_sem.at[e],
        device_id={'coil': other}, device_id_type=MESH) for e in range(2)]
    for c in sends:
        c.start()
    for c in sends:
        c.wait()
    for e in range(2):
        total = img[e, :, pl.ds(pl.multiple_of(cid * 128, 128), 256)] + yrecv[e]
        ctmp[e] = total.T
        out_ref[e] = ctmp[e, pl.ds(pl.multiple_of(cid * 32, 32), BLK), :] * dd[...]
    for stage in range(5):
        for c in received(stage):
            c.wait_send()


def solution(mesh):
    t2c, t3ac, t3bc = constants()

    def local_part(kspace, weight_row, weight_col, grid_row, grid_col, valid_count, coil_maps, deapod):
        row_scale = lax.dynamic_slice_in_dim(deapod, lax.axis_index('coil') * BLK, BLK)
        col_scale = lax.dynamic_slice_in_dim(deapod, lax.axis_index('rows') * COLS, COLS)
        dd = row_scale[:, None] * col_scale[None, :]
        any_spec = pl.BlockSpec(memory_space=pl.ANY)
        dma = pltpu.SemaphoreType.DMA
        return pl.pallas_call(
            body,
            out_shape=jax.ShapeDtypeStruct((2, BLK, COLS), F32),
            in_specs=[any_spec] * 5 + [pl.BlockSpec(memory_space=pltpu.SMEM)] + [any_spec] * 5,
            out_specs=pl.BlockSpec(memory_space=pltpu.VMEM),
            scratch_shapes=[
                pltpu.VMEM((2, NC, SLOTS), F32),
                pltpu.VMEM((4, SLOTS), F32),
                pltpu.VMEM((4, SLOTS), F32),
                pltpu.VMEM((1, SLOTS), jnp.int32),
                pltpu.VMEM((1, SLOTS), jnp.int32),
                pltpu.VMEM((2, NC, COLS, N_IMG), F32),
                pltpu.VMEM((BLK, COLS), F32),
            ] + [pltpu.VMEM((N_GRID, KC), BF)] * 4 + [
                pltpu.VMEM((168, SLOTS), F32),
                pltpu.VMEM((512, KC), BF),
                pltpu.VMEM((512, KC), BF),
                pltpu.VMEM((NK, 48, KC), F32),
                pltpu.VMEM((N_GRID, 512), F32),
                pltpu.VMEM((2 * N_GRID, 256), BF),
                pltpu.VMEM((5, ROWS, 2 * COLS, 256), BF),
                pltpu.VMEM((5, ROWS, 2 * COLS, 256), BF),
                pltpu.VMEM((48, N_GRID), F32),
                pltpu.VMEM((48, N_GRID), F32),
                pltpu.VMEM((N_GRID, 128), F32),
                pltpu.VMEM((ROWS, 2, COLS, 2 * N_GRID), BF),
                pltpu.VMEM((ROWS, 2, 128, 2 * LANES), BF),
                pltpu.VMEM((2, ROWS * B_ROWS, 2 * LANES), BF),
                pltpu.VMEM((NC, COLS, 2 * LANES), F32),
                pltpu.VMEM((2, COLS, 2 * LANES), F32),
                pltpu.VMEM((2, COLS, LANES), F32),
                pltpu.VMEM((2, COLS, 256), F32),
                pltpu.VMEM((2, 256, COLS), F32),
                dma((5,)), dma((9,)), dma((2,)), dma((5, 3)), dma((5, 3)), dma((2,)), dma((2,)), dma((2,)), dma((2,)),
            ],
            compiler_params=pltpu.CompilerParams(collective_id=0, has_side_effects=True, vmem_limit_bytes=60 * 1024 * 1024),
            name='nufft_adjoint',
        )(kspace, weight_row, weight_col, grid_row.reshape(1, SLOTS), grid_col.reshape(1, SLOTS), valid_count,
          jnp.swapaxes(coil_maps, 2, 3), dd, jnp.asarray(t2c), jnp.asarray(t3ac), jnp.asarray(t3bc))

    spec_samples = P(None, 'coil', ('slab', 'rows'))
    spec_weights = P(None, ('slab', 'rows'))
    spec_index = P(('slab', 'rows'))
    return jax.shard_map(local_part, mesh=mesh, in_specs=(spec_samples, spec_weights, spec_weights, spec_index, spec_index, spec_index, P(None, 'coil', 'slab', 'rows'), P()), out_specs=P(None, ('slab', 'coil'), 'rows'), check_vma=False)
```

```python
import functools
import numpy as np
import jax
import jax.numpy as jnp
from jax import lax
from jax.experimental import pallas as pl
from jax.experimental.pallas import tpu as pltpu
from jax.sharding import PartitionSpec as P

MESH = pl.DeviceIdType.MESH
BF = jnp.bfloat16
F32 = jnp.float32

N_IMG = 320
N_GRID = 640
ROWS = 4
BLK = 160
COLS = 80
NC = 8
SLOTS = 5120
KC = 1280
NK = SLOTS // KC
LANES = 384
B_FIRST = 64
B_ROWS = 32


def row_order():
    pos = np.arange(128)
    rows = pos + np.where(pos >= B_FIRST, B_ROWS, 0)
    rows[126], rows[16] = 16, 158
    rows[127], rows[32] = 32, 159
    return rows


def constants():
    k = np.arange(N_GRID)
    j = np.arange(N_IMG)
    ang = np.mod((k[:, None] - N_IMG) * (j[None, :] - N_IMG // 2), N_GRID) * (2.0 * np.pi / N_GRID)
    cos_t = np.cos(ang)
    sin_t = np.sin(ang)
    lanes = np.full((LANES,), -1)
    lanes[0:N_IMG] = np.arange(N_IMG)
    used = (lanes >= 0)[None, :]
    src = np.maximum(lanes, 0)
    pick = lambda t: np.where(used, t[:, src], 0.0)
    base = np.arange(ROWS)[:, None] * BLK
    ra = (base + row_order()[None, :]).reshape(-1)
    rb = (base + B_FIRST + np.arange(B_ROWS)[None, :]).reshape(-1)
    bf = jnp.bfloat16
    t3a = np.stack([pick(cos_t)[ra], pick(sin_t)[ra]]).reshape(2, ROWS, 128, LANES).astype(bf)
    t3b = np.stack([pick(cos_t)[rb], pick(sin_t)[rb]]).reshape(2, ROWS * B_ROWS, LANES).astype(bf)
    t2 = np.stack([cos_t.T, sin_t.T]).reshape(2, ROWS, COLS, N_GRID).astype(bf)
    return t2, t3a, t3b


def body(y_h, wr_h, wc_h, gr_h, gc_h, vc, s_h, d_h, t2_h, t3a_h, t3b_h, out_ref,
         y, wr, wc, gr, gc, s_v, din, drow, dcol, dd, rt0, rt1, rt2, rt3, wd, l0, l1, lh, acc, gb, hbuf, recv,
         hs, hr, hrt, t2, t3a, t3b, ib, img, yrecv, ctmp,
         in_sem, t2_sem, t3_sem, s_sem, send_sem, recv_sem, hsend_sem, hrecv_sem, ysend_sem, yrecv_sem):
    rts = (rt0, rt1, rt2, rt3)
    lefts = (l0, l1)
    me = lax.axis_index('rows')
    cid = lax.axis_index('coil')
    nxt = lax.rem(me + 1, ROWS)
    prv = lax.rem(me + ROWS - 1, ROWS)
    other = 1 - cid

    ins = [pltpu.make_async_copy(a, b, in_sem.at[n]) for n, (a, b) in enumerate(
        ((gc_h, gc), (wc_h, wc), (gr_h, gr), (wr_h, wr), (y_h.at[0], y.at[0:8]), (y_h.at[1], y.at[8:16])))]
    for c in ins:
        c.start()
    tab2 = [
        pltpu.make_async_copy(t2_h.at[0], t2.at[:, 0, :, 0:N_GRID], t2_sem.at[0]),
        pltpu.make_async_copy(t2_h.at[1], t2.at[:, 1, :, 0:N_GRID], t2_sem.at[1]),
        pltpu.make_async_copy(t2_h.at[0], t2.at[:, 1, :, N_GRID:], t2_sem.at[2]),
    ]
    tab3 = []
    for g in range(3):
        src = slice(g * 128, g * 128 + 128)
        re = slice(g * 256, g * 256 + 128)
        im = slice(g * 256 + 128, g * 256 + 256)
        tab3 += [
            (t3b_h.at[0, :, src], t3b.at[0, :, re]),
            (t3b_h.at[1, :, src], t3b.at[0, :, im]),
            (t3b_h.at[0, :, src], t3b.at[1, :, im]),
            (t3a_h.at[0, :, :, src], t3a.at[:, 0, :, re]),
            (t3a_h.at[1, :, :, src], t3a.at[:, 0, :, im]),
            (t3a_h.at[0, :, :, src], t3a.at[:, 1, :, im]),
        ]
    tab3 = [pltpu.make_async_copy(a, b, t3_sem.at[n]) for n, (a, b) in enumerate(tab3)]
    big = [pltpu.make_async_copy(s_h, s_v, s_sem.at[0]),
           pltpu.make_async_copy(d_h, din, s_sem.at[1])]
    for c in tab2 + tab3 + big:
        c.start()

    barrier = pltpu.get_barrier_semaphore()
    for d in range(1, ROWS):
        pl.semaphore_signal(barrier, inc=1, device_id={'rows': lax.rem(me + d, ROWS)}, device_id_type=MESH)
    pl.semaphore_signal(barrier, inc=1, device_id={'coil': other}, device_id_type=MESH)
    for c in ins:
        c.wait()

    pieces = [(k * KC + o, 256) for k in range(NK) for o in range(0, KC, 256)]

    def build_wd(lo, groups):
        sl = pl.ds(lo, 256)
        keep = (lax.broadcasted_iota(jnp.int32, (1, 256), 1) + lo < vc[0]).astype(F32)
        first = gr[:, sl] - me * BLK
        taps = [(jnp.broadcast_to(first + (a - 2), (8, 256)), jnp.broadcast_to(wr[a:a + 1, sl] * keep, (8, 256)))
                for a in range(4)]
        ids = lax.broadcasted_iota(jnp.int32, (8, 1), 0)
        for n in groups:
            if n < 16:
                r = ids + (n * 8 + (B_ROWS if n * 8 >= B_FIRST else 0))
            elif n < 20:
                r = ids + (n * 8 - 128 + B_FIRST)
            else:
                r = jnp.where(ids == 0, BLK, ids - 3)
            for p, v in ((126, 16), (127, 32), (16, 158), (32, 159)):
                if p // 8 == n:
                    r = jnp.where(ids == p % 8, v, r)
            w = jnp.zeros((8, 256), F32)
            for t, v in taps:
                w = jnp.where(r == t, v, w)
            wd[n * 8:n * 8 + 8, sl] = w

    def build_rt(k, off):
        sl = pl.ds(k * KC + off, 256)
        col = gc[:, sl]
        taps = []
        for b in range(4):
            t = col + (b - 2)
            t = jnp.where(t < 0, t + N_GRID, jnp.where(t >= N_GRID, t - N_GRID, t))
            taps.append((jnp.broadcast_to(t, (16, 256)).astype(jnp.int16),
                         jnp.broadcast_to(wc[b:b + 1, sl], (16, 256)).astype(BF)))
        base = lax.broadcasted_iota(jnp.int16, (16, 256), 0)
        for n in range(N_GRID // 16):
            ids = base + jnp.int16(n * 16)
            w = jnp.zeros((16, 256), BF)
            for t, v in taps:
                w = jnp.where(ids == t, v, w)
            rts[k][n * 16:(n + 1) * 16, off:off + 256] = w

    def build_left_b(k, off):
        sl = pl.ds(k * KC + off, 256)
        w = wd[128:160, sl]
        for q in range(2):
            for c in range(NC):
                lo = q * 256 + c * 32
                lefts[k % 2][lo:lo + 32, off:off + 256] = (y[q * 8 + c:q * 8 + c + 1, sl] * w).astype(BF)

    def build_halo(lo):
        sl = pl.ds(lo, 256)
        for h in range(3):
            lh[h * 16:h * 16 + 16, sl] = (y[:, sl] * wd[160 + h:161 + h, sl]).astype(BF)

    def build_left_a(s, k):
        for off in range(0, KC, 256):
            sl = pl.ds(k * KC + off, 256)
            rows = [jnp.broadcast_to(y[pl.ds(q * 8 + 2 * s + c, 1), sl], (16, 256)) for q in range(2) for c in range(2)]
            for n in range(8):
                w = wd[n * 16:n * 16 + 16, sl]
                for m, row in enumerate(rows):
                    lefts[k % 2][m * 128 + n * 16:m * 128 + n * 16 + 16, off:off + 256] = (row * w).astype(BF)

    def nt(a, b):
        return lax.dot_general(a, b, (((1,), (1,)), ((), ())), preferred_element_type=F32)

    def exchange(stage):
        return [pltpu.make_async_remote_copy(
            src_ref=hbuf.at[stage, lax.rem(me + d, ROWS)], dst_ref=recv.at[stage, me],
            send_sem=send_sem.at[stage, d - 1], recv_sem=recv_sem.at[stage, 3 - d],
            device_id={'rows': lax.rem(me + d, ROWS)}, device_id_type=MESH) for d in (1, 2, 3)]

    def received(stage):
        return [pltpu.make_async_remote_copy(
            src_ref=hbuf.at[stage, 0], dst_ref=recv.at[stage, lax.rem(me + d, ROWS)],
            send_sem=send_sem.at[stage, d - 1], recv_sem=recv_sem.at[stage, d - 1],
            device_id={'rows': lax.rem(me + d, ROWS)}, device_id_type=MESH) for d in (1, 2, 3)]

    def transform(stage):
        for n in range(ROWS):
            hbuf[stage, n] = jnp.dot(t2[n].reshape(2 * COLS, 2 * N_GRID), gb[...], preferred_element_type=F32).astype(BF)
        for c in exchange(stage):
            c.start()
        recv[stage, me] = hbuf[stage, me]

    parts = [(0, 0, 256), (0, 256, KC - 256)] + [(k, 0, KC) for k in range(1, NK)]

    def build_first(k, off, size):
        for o in range(off, off + size, 256):
            build_rt(k, o)
            build_wd(k * KC + o, (16, 17, 18, 19, 20))
            build_left_b(k, o)

    build_first(*parts[0])
    for n, (k, off, size) in enumerate(parts):
        for q in range(2):
            cs = slice(q * 256, q * 256 + 256)
            part = nt(rts[k][:, off:off + size], lefts[k % 2][cs, off:off + size])
            if n == 0:
                acc[:, cs] = part
            elif n + 1 < len(parts):
                acc[:, cs] += part
            else:
                gb[q * N_GRID:(q + 1) * N_GRID, :] = (acc[:, cs] + part).astype(BF)
        if n + 1 < len(parts):
            build_first(*parts[n + 1])
    for c in tab2:
        c.wait()
    t2[:, 0, :, N_GRID:] = -t2[:, 1, :, 0:N_GRID]
    pl.semaphore_wait(barrier, 4)
    transform(0)

    for c in tab3 + big:
        c.wait()
    for lo, _ in pieces:
        build_halo(lo)
    for h in range(2):
        rows = slice(h * 320, h * 320 + 320)
        halo = nt(rts[0][rows, :], lh[:, 0:KC])
        for k in range(1, NK):
            halo = halo + nt(rts[k][rows, :], lh[:, k * KC:(k + 1) * KC])
        hrt[rows, 0:48] = halo
    for lo, _ in pieces:
        build_wd(lo, range(16))
    for g in range(3):
        lanes = slice(g * 256, g * 256 + 128)
        t3b[1, :, lanes] = -t3b[0, :, g * 256 + 128:g * 256 + 256]
        t3a[:, 1, :, lanes] = -t3a[:, 0, :, g * 256 + 128:g * 256 + 256]
    drow[:, 0:N_IMG] = din[...].reshape(1, N_IMG)
    dcol[...] = jnp.broadcast_to(din[...].reshape(1, N_IMG), (8, N_IMG)).T
    dd[...] = dcol[pl.ds(pl.multiple_of(me * COLS, COLS), COLS), 0:1] * drow[:, pl.ds(pl.multiple_of(cid * 128, 128), 256)]
    img[...] = jnp.zeros_like(img)
    hs[...] = hrt[...].T[0:48]
    build_left_a(0, 0)
    to_next = pltpu.make_async_remote_copy(
        src_ref=hs.at[0:16], dst_ref=hr.at[0:16], send_sem=hsend_sem.at[0], recv_sem=hrecv_sem.at[0],
        device_id={'rows': nxt}, device_id_type=MESH)
    to_prev = pltpu.make_async_remote_copy(
        src_ref=hs.at[16:48], dst_ref=hr.at[16:48], send_sem=hsend_sem.at[1], recv_sem=hrecv_sem.at[1],
        device_id={'rows': prv}, device_id_type=MESH)
    to_next.start()
    to_prev.start()

    def image_first():
        for c in received(0):
            c.wait_recv()
        for c in range(NC):
            blocks = [recv[0, p, b * COLS:(b + 1) * COLS, c * 32:c * 32 + 32] for b in range(2) for p in range(ROWS)]
            lhs = jnp.concatenate(blocks, axis=1)
            ib[c // 2, (c % 2) * COLS:(c % 2 + 1) * COLS] = jnp.dot(lhs, t3b[...].reshape(256, 2 * LANES), preferred_element_type=F32)

    def image_coils(s):
        stage = s + 1
        for c in received(stage):
            c.wait_recv()
        lhs = jnp.concatenate([jnp.concatenate(
            [recv[stage, p, b * COLS:(b + 1) * COLS, c * 128:c * 128 + 128] for p in range(ROWS) for b in range(2)], axis=1)
            for c in range(2)], axis=0)
        for g in range(3):
            lanes = slice(g * 256, g * 256 + 256)
            tot = ib[s, :, lanes] + jnp.dot(lhs, t3a[:, :, :, lanes].reshape(1024, 256), preferred_element_type=F32)
            n = min(128, N_IMG - g * 128)
            at = slice(g * 128, g * 128 + n)
            add_re = img[0, :, at]
            add_im = img[1, :, at]
            for c in range(2):
                sr = s_v[0, 2 * s + c, :, at]
                si = s_v[1, 2 * s + c, :, at]
                re = tot[c * COLS:(c + 1) * COLS, 0:n]
                im = tot[c * COLS:(c + 1) * COLS, 128:128 + n]
                add_re = add_re + (sr * re + si * im)
                add_im = add_im + (sr * im - si * re)
            img[0, :, at] = add_re
            img[1, :, at] = add_im

    @pl.loop(0, NC // 2)
    def _(s):
        for k in range(NK - 1):
            for q in range(2):
                cs = slice(q * 256, q * 256 + 256)
                part = nt(rts[k][...], lefts[k % 2][cs, :])
                if k == 0:
                    acc[:, cs] = part
                else:
                    acc[:, cs] += part
            build_left_a(s, k + 1)

        @pl.when(s == 0)
        def _():
            to_next.wait()
            to_prev.wait()
            hrt[...] = jnp.concatenate([hr[...], jnp.zeros((80, N_GRID), F32)], axis=0).T

        k = NK - 1
        lane = lax.broadcasted_iota(jnp.int32, (1, 128), 1)
        edge = (lane == 0) | (lane == 16) | (lane == 32)
        for q in range(2):
            part = nt(rts[k][...], lefts[k % 2][q * 256:q * 256 + 256, :])
            for c in range(2):
                rolled = pltpu.roll(hrt[...], 128 - (q * 8 + 2 * s + c), 1)
                lo = q * 256 + c * 128
                whole = acc[:, lo:lo + 128] + part[:, c * 128:c * 128 + 128] + jnp.where(edge, rolled, 0.0)
                gb[q * N_GRID:(q + 1) * N_GRID, c * 128:c * 128 + 128] = whole.astype(BF)
        build_left_a(jnp.minimum(s + 1, NC // 2 - 1), 0)
        transform(s + 1)

        @pl.when(s == 0)
        def _():
            image_first()

        @pl.when(s > 0)
        def _():
            image_coils(s - 1)

    image_coils(NC // 2 - 1)

    sends = [pltpu.make_async_remote_copy(
        src_ref=img.at[e, :, pl.ds(pl.multiple_of(other * 128, 128), 256)], dst_ref=yrecv.at[e],
        send_sem=ysend_sem.at[e], recv_sem=yrecv_sem.at[e],
        device_id={'coil': other}, device_id_type=MESH) for e in range(2)]
    for c in sends:
        c.start()
    for e in range(2):
        sends[e].wait()
        total = (img[e, :, pl.ds(pl.multiple_of(cid * 128, 128), 256)] + yrecv[e]) * dd[...]
        ctmp[e] = total.T
        out_ref[e] = ctmp[e, pl.ds(pl.multiple_of(cid * 32, 32), BLK), :]
    for stage in range(5):
        for c in received(stage):
            c.wait_send()


def solution(mesh):
    t2c, t3ac, t3bc = constants()

    def local_part(kspace, weight_row, weight_col, grid_row, grid_col, valid_count, coil_maps, deapod):
        any_spec = pl.BlockSpec(memory_space=pl.ANY)
        dma = pltpu.SemaphoreType.DMA
        return pl.pallas_call(
            body,
            out_shape=pltpu.VMEM((2, BLK, COLS), F32),
            in_specs=[any_spec] * 5 + [pl.BlockSpec(memory_space=pltpu.SMEM)] + [any_spec] * 5,
            out_specs=pl.BlockSpec(memory_space=pltpu.VMEM),
            scratch_shapes=[
                pltpu.VMEM((2 * NC, SLOTS), F32),
                pltpu.VMEM((4, SLOTS), F32),
                pltpu.VMEM((4, SLOTS), F32),
                pltpu.VMEM((1, SLOTS), jnp.int32),
                pltpu.VMEM((1, SLOTS), jnp.int32),
                pltpu.VMEM((2, NC, COLS, N_IMG), F32),
                pltpu.VMEM((N_IMG,), F32),
                pltpu.VMEM((1, LANES), F32),
                pltpu.VMEM((N_IMG, 8), F32),
                pltpu.VMEM((COLS, 256), F32),
            ] + [pltpu.VMEM((N_GRID, KC), BF)] * 4 + [
                pltpu.VMEM((168, SLOTS), F32),
                pltpu.VMEM((512, KC), BF),
                pltpu.VMEM((512, KC), BF),
                pltpu.VMEM((48, SLOTS), BF),
                pltpu.VMEM((N_GRID, 512), F32),
                pltpu.VMEM((2 * N_GRID, 256), BF),
                pltpu.VMEM((5, ROWS, 2 * COLS, 256), BF),
                pltpu.VMEM((5, ROWS, 2 * COLS, 256), BF),
                pltpu.VMEM((48, N_GRID), F32),
                pltpu.VMEM((48, N_GRID), F32),
                pltpu.VMEM((N_GRID, 128), F32),
                pltpu.VMEM((ROWS, 2, COLS, 2 * N_GRID), BF),
                pltpu.VMEM((ROWS, 2, 128, 2 * LANES), BF),
                pltpu.VMEM((2, ROWS * B_ROWS, 2 * LANES), BF),
                pltpu.VMEM((NC // 2, 2 * COLS, 2 * LANES), F32),
                pltpu.VMEM((2, COLS, LANES), F32),
                pltpu.VMEM((2, COLS, 256), F32),
                pltpu.VMEM((2, 256, COLS), F32),
                dma((6,)), dma((3,)), dma((18,)), dma((2,)), dma((5, 3)), dma((5, 3)), dma((2,)), dma((2,)), dma((2,)), dma((2,)),
            ],
            compiler_params=pltpu.CompilerParams(collective_id=0, has_side_effects=True, vmem_limit_bytes=60 * 1024 * 1024),
            name='nufft_adjoint',
        )(kspace, weight_row, weight_col, grid_row.reshape(1, SLOTS), grid_col.reshape(1, SLOTS), valid_count,
          jnp.swapaxes(coil_maps, 2, 3), deapod, jnp.asarray(t2c), jnp.asarray(t3ac), jnp.asarray(t3bc))

    spec_samples = P(None, 'coil', ('slab', 'rows'))
    spec_weights = P(None, ('slab', 'rows'))
    spec_index = P(('slab', 'rows'))
    return jax.shard_map(local_part, mesh=mesh, in_specs=(spec_samples, spec_weights, spec_weights, spec_index, spec_index, spec_index, P(None, 'coil', 'slab', 'rows'), P()), out_specs=P(None, ('slab', 'coil'), 'rows'), check_vma=False)
```

```python
import functools
import numpy as np
import jax
import jax.numpy as jnp
from jax import lax
from jax.experimental import pallas as pl
from jax.experimental.pallas import tpu as pltpu
from jax.sharding import PartitionSpec as P

MESH = pl.DeviceIdType.MESH
BF = jnp.bfloat16
F32 = jnp.float32

N_IMG = 320
N_GRID = 640
ROWS = 4
BLK = 160
COLS = 80
NC = 8
SLOTS = 5120
KC = 1280
NK = SLOTS // KC
LANES = 384
HALF = SLOTS // 2
LAG = 3
B_FIRST = 64
B_ROWS = 32


def row_order():
    pos = np.arange(128)
    rows = pos + np.where(pos >= B_FIRST, B_ROWS, 0)
    rows[126], rows[16] = 16, 158
    rows[127], rows[32] = 32, 159
    return rows


def constants():
    k = np.arange(N_GRID)
    j = np.arange(N_IMG)
    ang = np.mod((k[:, None] - N_IMG) * (j[None, :] - N_IMG // 2), N_GRID) * (2.0 * np.pi / N_GRID)
    cos_t = np.cos(ang)
    sin_t = np.sin(ang)
    lanes = np.full((LANES,), -1)
    lanes[0:N_IMG] = np.arange(N_IMG)
    used = (lanes >= 0)[None, :]
    src = np.maximum(lanes, 0)
    pick = lambda t: np.where(used, t[:, src], 0.0)
    base = np.arange(ROWS)[:, None] * BLK
    ra = (base + row_order()[None, :]).reshape(-1)
    rb = (base + B_FIRST + np.arange(B_ROWS)[None, :]).reshape(-1)
    bf = jnp.bfloat16
    t3a = np.stack([pick(cos_t)[ra], pick(sin_t)[ra]]).reshape(2, ROWS, 128, LANES).astype(bf)
    t3b = np.stack([pick(cos_t)[rb], pick(sin_t)[rb]]).reshape(2, ROWS * B_ROWS, LANES).astype(bf)
    t2 = np.stack([cos_t.T, sin_t.T]).reshape(2, ROWS, COLS, N_GRID).astype(bf)
    return t2, t3a, t3b


def body(y_h, wr_h, wc_h, gr_h, gc_h, vc, s_h, d_h, t2_h, t3a_h, t3b_h, out_ref,
         y, wr, wc, gr, gc, s_v, din, drow, dcol, dd, rt0, rt1, wd, lb0, lb1, la0, la1, lh, accb, acc, gbb, gb,
         hbufb, recvb, hbuf, recv,
         hs, hr, hrt, t2, t3a, t3b, ib, img, yrecv, ctmp,
         in_sem, tab_sem, send_sem, recv_sem, hsend_sem, hrecv_sem, ysend_sem, yrecv_sem):
    rts = (rt0, rt1)
    lefts_b = (lb0, lb1)
    lefts = (la0, la1)
    me = lax.axis_index('rows')
    cid = lax.axis_index('coil')
    nxt = lax.rem(me + 1, ROWS)
    prv = lax.rem(me + ROWS - 1, ROWS)
    other = 1 - cid

    ins = [pltpu.make_async_copy(a, b, in_sem.at[n]) for n, (a, b) in enumerate(
        ((gc_h, gc), (wc_h, wc), (gr_h, gr), (wr_h, wr), (y_h.at[0], y.at[0:8]), (y_h.at[1], y.at[8:16])))]
    for c in ins:
        c.start()
    tabs = [(t2_h.at[0], t2.at[:, 0]), (t2_h.at[1], t2.at[:, 1])]
    for g in range(3):
        src = slice(g * 128, g * 128 + 128)
        re = slice(g * 256, g * 256 + 128)
        im = slice(g * 256 + 128, g * 256 + 256)
        tabs += [
            (t3b_h.at[0, :, src], t3b.at[0, :, re]),
            (t3b_h.at[1, :, src], t3b.at[0, :, im]),
            (t3b_h.at[0, :, src], t3b.at[1, :, im]),
            (t3a_h.at[0, :, :, src], t3a.at[:, :, re]),
            (t3a_h.at[1, :, :, src], t3a.at[:, :, im]),
        ]
    tabs += [(s_h, s_v), (d_h, din)]
    tabs = [pltpu.make_async_copy(a, b, tab_sem.at[n]) for n, (a, b) in enumerate(tabs)]
    for c in tabs:
        c.start()

    barrier = pltpu.get_barrier_semaphore()
    for d in range(1, ROWS):
        pl.semaphore_signal(barrier, inc=1, device_id={'rows': lax.rem(me + d, ROWS)}, device_id_type=MESH)
    pl.semaphore_signal(barrier, inc=1, device_id={'coil': other}, device_id_type=MESH)
    for c in ins:
        c.wait()
    pl.semaphore_wait(barrier, 4)

    pieces = [(k * KC + o, 256) for k in range(NK) for o in range(0, KC, 256)]

    def build_wd(lo, groups):
        sl = pl.ds(lo, 256)
        keep = (lax.broadcasted_iota(jnp.int32, (1, 256), 1) + lo < vc[0]).astype(F32)
        first = gr[:, sl] - me * BLK
        taps = [(jnp.broadcast_to(first + (a - 2), (8, 256)), jnp.broadcast_to(wr[a:a + 1, sl] * keep, (8, 256)))
                for a in range(4)]
        ids = lax.broadcasted_iota(jnp.int32, (8, 1), 0)
        for n in groups:
            if n < 16:
                r = ids + (n * 8 + (B_ROWS if n * 8 >= B_FIRST else 0))
            elif n < 20:
                r = ids + (n * 8 - 128 + B_FIRST)
            else:
                r = jnp.where(ids == 0, BLK, ids - 3)
            for p, v in ((126, 16), (127, 32), (16, 158), (32, 159)):
                if p // 8 == n:
                    r = jnp.where(ids == p % 8, v, r)
            w = jnp.zeros((8, 256), F32)
            for t, v in taps:
                w = jnp.where(r == t, v, w)
            wd[n * 8:n * 8 + 8, sl] = w

    def build_rt(lo):
        sl = pl.ds(lo, 256)
        k, off = lo // HALF, lo % HALF
        col = gc[:, sl]
        taps = []
        for b in range(4):
            t = col + (b - 2)
            t = jnp.where(t < 0, t + N_GRID, jnp.where(t >= N_GRID, t - N_GRID, t))
            taps.append((jnp.broadcast_to(t, (16, 256)).astype(jnp.int16),
                         jnp.broadcast_to(wc[b:b + 1, sl], (16, 256)).astype(BF)))
        base = lax.broadcasted_iota(jnp.int16, (16, 256), 0)
        for n in range(N_GRID // 16):
            ids = base + jnp.int16(n * 16)
            w = jnp.zeros((16, 256), BF)
            for t, v in taps:
                w = jnp.where(ids == t, v, w)
            rts[k][n * 16:(n + 1) * 16, off:off + 256] = w

    def build_left_b(k, off):
        sl = pl.ds(k * KC + off, 256)
        w = wd[128:160, sl]
        for q in range(2):
            for c in range(NC):
                lo = q * 256 + c * 32
                lefts_b[k % 2][lo:lo + 32, off:off + 256] = (y[q * 8 + c:q * 8 + c + 1, sl] * w).astype(BF)

    def build_halo(lo):
        sl = pl.ds(lo, 256)
        for h in range(3):
            lh[h * 16:h * 16 + 16, sl] = (y[:, sl] * wd[160 + h:161 + h, sl]).astype(BF)

    def left_a_piece(c, lo):
        k, off = lo // HALF, lo % HALF
        sl = pl.ds(lo, 256)
        rows = [jnp.broadcast_to(y[pl.ds(q * 8 + c, 1), sl], (16, 256)) for q in range(2)]
        for n in range(8):
            w = wd[n * 16:n * 16 + 16, sl]
            for q, row in enumerate(rows):
                lefts[k][q * 128 + n * 16:q * 128 + n * 16 + 16, off:off + 256] = (row * w).astype(BF)

    def build_left_a(c, k):
        for off in range(0, HALF, 256):
            left_a_piece(c, k * HALF + off)

    def nt(a, b):
        return lax.dot_general(a, b, (((1,), (1,)), ((), ())), preferred_element_type=F32)

    def exchange(stage):
        if stage is None:
            src, dst, idx = hbufb, recvb, NC
        else:
            src, dst, idx = hbuf.at[stage], recv.at[stage], stage
        return [pltpu.make_async_remote_copy(
            src_ref=src.at[lax.rem(me + d, ROWS)], dst_ref=dst.at[me],
            send_sem=send_sem.at[idx, d - 1], recv_sem=recv_sem.at[idx, 3 - d],
            device_id={'rows': lax.rem(me + d, ROWS)}, device_id_type=MESH) for d in (1, 2, 3)]

    def received(stage):
        if stage is None:
            src, dst, idx = hbufb, recvb, NC
        else:
            src, dst, idx = hbuf.at[stage], recv.at[stage], stage
        return [pltpu.make_async_remote_copy(
            src_ref=src.at[0], dst_ref=dst.at[lax.rem(me + d, ROWS)],
            send_sem=send_sem.at[idx, d - 1], recv_sem=recv_sem.at[idx, d - 1],
            device_id={'rows': lax.rem(me + d, ROWS)}, device_id_type=MESH) for d in (1, 2, 3)]

    def transform(stage):
        g_ref, h_ref, r_ref = (gbb, hbufb, recvb) if stage is None else (gb, hbuf.at[stage], recv.at[stage])
        n = g_ref.shape[1] // 2
        for h in range(2):
            table = t2[2 * h:2 * h + 2].reshape(N_IMG, N_GRID)
            with_re = jnp.dot(table, g_ref[:, 0:n], preferred_element_type=F32) if n == 256 else None
            with_im = jnp.dot(table, g_ref[:, n:], preferred_element_type=F32) if n == 256 else None
            if n < 256:
                both = jnp.dot(table, g_ref[...], preferred_element_type=F32)
                with_re, with_im = both[:, 0:n], both[:, n:]
            for p in range(2):
                lo = p * 2 * COLS
                mid = lo + COLS
                end = mid + COLS
                h_ref[2 * h + p, 0:COLS] = (with_re[lo:mid] - with_im[mid:end]).astype(BF)
                h_ref[2 * h + p, COLS:] = (with_re[mid:end] + with_im[lo:mid]).astype(BF)

    def send(stage):
        h_ref, r_ref = (hbufb, recvb) if stage is None else (hbuf.at[stage], recv.at[stage])
        for c in exchange(stage):
            c.start()
        r_ref[me] = h_ref[me]

    halo = [None, None]
    for k in range(NK):
        for o in range(k * KC, (k + 1) * KC, 256):
            build_rt(o)
            build_wd(o, (20,))
            build_halo(o)
        off = (k % 2) * KC
        for h in range(2):
            part = nt(rts[k // 2][h * 320:h * 320 + 320, off:off + KC], lh[:, k * KC:(k + 1) * KC])
            halo[h] = part if k == 0 else halo[h] + part
    for o in range(0, KC, 256):
        build_wd(o, (16, 17, 18, 19))
        build_left_b(0, o)
    for h in range(2):
        hrt[h * 320:h * 320 + 320, 0:48] = halo[h]
    hs[...] = hrt[...].T[0:48]
    to_next = pltpu.make_async_remote_copy(
        src_ref=hs.at[0:16], dst_ref=hr.at[0:16], send_sem=hsend_sem.at[0], recv_sem=hrecv_sem.at[0],
        device_id={'rows': nxt}, device_id_type=MESH)
    to_prev = pltpu.make_async_remote_copy(
        src_ref=hs.at[16:48], dst_ref=hr.at[16:48], send_sem=hsend_sem.at[1], recv_sem=hrecv_sem.at[1],
        device_id={'rows': prv}, device_id_type=MESH)
    to_next.start()
    to_prev.start()
    for c in tabs:
        c.wait()

    for k in range(NK):
        off = (k % 2) * KC
        for q in range(2):
            cs = slice(q * 256, q * 256 + 256)
            part = nt(rts[k // 2][:, off:off + KC], lefts_b[k % 2][cs, :])
            if k == 0:
                accb[:, cs] = part
            elif k + 1 < NK:
                accb[:, cs] += part
            else:
                gbb[:, cs] = (accb[:, cs] + part).astype(BF)
        if k >= NK // 2:
            for o in range((k - NK // 2) * KC, (k - NK // 2 + 1) * KC, 256):
                build_wd(o, range(16))
                left_a_piece(0, o)
        if k + 1 < NK:
            for o in range(0, KC, 256):
                build_wd((k + 1) * KC + o, (16, 17, 18, 19))
                build_left_b(k + 1, o)
    for g in range(3):
        t3b[1, :, g * 256:g * 256 + 128] = -t3b[0, :, g * 256 + 128:g * 256 + 256]
    drow[:, 0:N_IMG] = din[...].reshape(1, N_IMG)
    dcol[...] = jnp.broadcast_to(din[...].reshape(1, N_IMG), (8, N_IMG)).T
    dd[...] = dcol[pl.ds(pl.multiple_of(me * COLS, COLS), COLS), 0:1] * drow[:, pl.ds(pl.multiple_of(cid * 128, 128), 256)]
    img[...] = jnp.zeros_like(img)
    transform(None)
    send(None)

    def spread_head(c, first=False):
        for h in range(2):
            rows = slice(h * 320, h * 320 + 320)
            acc[rows, :] = nt(rts[0][rows, :], lefts[0][...])
        for lo in range(HALF, SLOTS, 256):
            if first:
                build_wd(lo, range(16))
            left_a_piece(c, lo)

    lane = lax.broadcasted_iota(jnp.int32, (1, 128), 1)
    edge = (lane == 0) | (lane == 16) | (lane == 32)

    def spread_tail(c):
        for h in range(2):
            rows = slice(h * 320, h * 320 + 320)
            part = nt(rts[1][rows, :], lefts[1][...])
            for q in range(2):
                cs = slice(q * 128, q * 128 + 128)
                rolled = pltpu.roll(hrt[rows, :], 128 - (q * 8 + c), 1)
                gb[rows, cs] = (acc[rows, cs] + part[:, cs] + jnp.where(edge, rolled, 0.0)).astype(BF)

    def image_first():
        for c in received(None):
            c.wait_recv()
        for c in range(NC):
            blocks = [recvb[p, b * COLS:(b + 1) * COLS, c * 32:c * 32 + 32] for b in range(2) for p in range(ROWS)]
            lhs = jnp.concatenate(blocks, axis=1)
            ib[c] = jnp.dot(lhs, t3b[...].reshape(256, 2 * LANES), preferred_element_type=F32)

    def image_wait(c):
        for x in received(c):
            x.wait_recv()

    def image_coil(c):
        lhs = jnp.concatenate([recv[c, p] for p in range(ROWS)], axis=1)
        for g in range(3):
            lanes = slice(g * 256, g * 256 + 256)
            tot = jnp.dot(lhs, t3a[:, :, lanes].reshape(4 * 128, 256), preferred_element_type=F32)
            re = ib[c, :, g * 256:g * 256 + 128] + (tot[0:COLS, 0:128] - tot[COLS:, 128:])
            im = ib[c, :, g * 256 + 128:g * 256 + 256] + (tot[0:COLS, 128:] + tot[COLS:, 0:128])
            n = min(128, N_IMG - g * 128)
            at = slice(g * 128, g * 128 + n)
            sr = s_v[0, c, :, at]
            si = s_v[1, c, :, at]
            img[0, :, at] += sr * re[:, 0:n] + si * im[:, 0:n]
            img[1, :, at] += sr * im[:, 0:n] - si * re[:, 0:n]

    spread_head(0, True)

    @pl.loop(0, LAG)
    def _(c):
        @pl.when(c == 0)
        def _():
            to_next.wait()
            to_prev.wait()
            hrt[...] = jnp.concatenate([hr[...], jnp.zeros((80, N_GRID), F32)], axis=0).T

        spread_tail(c)
        build_left_a(c + 1, 0)
        transform(c)
        spread_head(c + 1)
        send(c)

    image_first()

    @pl.loop(LAG, NC - 1)
    def _(c):
        image_wait(c - LAG)
        spread_tail(c)
        build_left_a(c + 1, 0)
        image_coil(c - LAG)
        transform(c)
        spread_head(c + 1)
        send(c)

    spread_tail(NC - 1)
    transform(NC - 1)
    send(NC - 1)

    @pl.loop(NC - 1 - LAG, NC)
    def _(c):
        image_wait(c)
        image_coil(c)

    sends = [pltpu.make_async_remote_copy(
        src_ref=img.at[e, :, pl.ds(pl.multiple_of(other * 128, 128), 256)], dst_ref=yrecv.at[e],
        send_sem=ysend_sem.at[e], recv_sem=yrecv_sem.at[e],
        device_id={'coil': other}, device_id_type=MESH) for e in range(2)]
    for c in sends:
        c.start()
    for e in range(2):
        sends[e].wait()
        total = (img[e, :, pl.ds(pl.multiple_of(cid * 128, 128), 256)] + yrecv[e]) * dd[...]
        ctmp[e] = total.T
        out_ref[e] = ctmp[e, pl.ds(pl.multiple_of(cid * 32, 32), BLK), :]
    for stage in [None] + list(range(NC)):
        for c in received(stage):
            c.wait_send()


def solution(mesh):
    t2c, t3ac, t3bc = constants()

    def local_part(kspace, weight_row, weight_col, grid_row, grid_col, valid_count, coil_maps, deapod):
        any_spec = pl.BlockSpec(memory_space=pl.ANY)
        dma = pltpu.SemaphoreType.DMA
        return pl.pallas_call(
            body,
            out_shape=pltpu.VMEM((2, BLK, COLS), F32),
            in_specs=[any_spec] * 5 + [pl.BlockSpec(memory_space=pltpu.SMEM)] + [any_spec] * 5,
            out_specs=pl.BlockSpec(memory_space=pltpu.VMEM),
            scratch_shapes=[
                pltpu.VMEM((2 * NC, SLOTS), F32),
                pltpu.VMEM((4, SLOTS), F32),
                pltpu.VMEM((4, SLOTS), F32),
                pltpu.VMEM((1, SLOTS), jnp.int32),
                pltpu.VMEM((1, SLOTS), jnp.int32),
                pltpu.VMEM((2, NC, COLS, N_IMG), F32),
                pltpu.VMEM((N_IMG,), F32),
                pltpu.VMEM((1, LANES), F32),
                pltpu.VMEM((N_IMG, 8), F32),
                pltpu.VMEM((COLS, 256), F32),
                pltpu.VMEM((N_GRID, HALF), BF),
                pltpu.VMEM((N_GRID, HALF), BF),
                pltpu.VMEM((168, SLOTS), F32),
                pltpu.VMEM((512, KC), BF),
                pltpu.VMEM((512, KC), BF),
                pltpu.VMEM((256, HALF), BF),
                pltpu.VMEM((256, HALF), BF),
                pltpu.VMEM((48, SLOTS), BF),
                pltpu.VMEM((N_GRID, 512), F32),
                pltpu.VMEM((N_GRID, 256), F32),
                pltpu.VMEM((N_GRID, 512), BF),
                pltpu.VMEM((N_GRID, 256), BF),
                pltpu.VMEM((ROWS, 2 * COLS, 256), BF),
                pltpu.VMEM((ROWS, 2 * COLS, 256), BF),
                pltpu.VMEM((NC, ROWS, 2 * COLS, 128), BF),
                pltpu.VMEM((NC, ROWS, 2 * COLS, 128), BF),
                pltpu.VMEM((48, N_GRID), F32),
                pltpu.VMEM((48, N_GRID), F32),
                pltpu.VMEM((N_GRID, 128), F32),
                pltpu.VMEM((ROWS, 2, COLS, N_GRID), BF),
                pltpu.VMEM((ROWS, 128, 2 * LANES), BF),
                pltpu.VMEM((2, ROWS * B_ROWS, 2 * LANES), BF),
                pltpu.VMEM((NC, COLS, 2 * LANES), F32),
                pltpu.VMEM((2, COLS, LANES), F32),
                pltpu.VMEM((2, COLS, 256), F32),
                pltpu.VMEM((2, 256, COLS), F32),
                dma((6,)), dma((19,)), dma((9, 3)), dma((9, 3)), dma((2,)), dma((2,)), dma((2,)), dma((2,)),
            ],
            compiler_params=pltpu.CompilerParams(collective_id=0, has_side_effects=True, vmem_limit_bytes=60 * 1024 * 1024),
            name='nufft_adjoint',
        )(kspace, weight_row, weight_col, grid_row.reshape(1, SLOTS), grid_col.reshape(1, SLOTS), valid_count,
          jnp.swapaxes(coil_maps, 2, 3), deapod, jnp.asarray(t2c), jnp.asarray(t3ac), jnp.asarray(t3bc))

    spec_samples = P(None, 'coil', ('slab', 'rows'))
    spec_weights = P(None, ('slab', 'rows'))
    spec_index = P(('slab', 'rows'))
    return jax.shard_map(local_part, mesh=mesh, in_specs=(spec_samples, spec_weights, spec_weights, spec_index, spec_index, spec_index, P(None, 'coil', 'slab', 'rows'), P()), out_specs=P(None, ('slab', 'coil'), 'rows'), check_vma=False)
```

```python
import functools
import numpy as np
import jax
import jax.numpy as jnp
from jax import lax
from jax.experimental import pallas as pl
from jax.experimental.pallas import tpu as pltpu
from jax.sharding import PartitionSpec as P

MESH = pl.DeviceIdType.MESH
BF = jnp.bfloat16
F32 = jnp.float32

N_IMG = 320
N_GRID = 640
ROWS = 4
BLK = 160
COLS = 80
NC = 8
SLOTS = 5120
KC = 1280
NK = SLOTS // KC
LANES = 384
HALF = SLOTS // 2
LAG = 3
B_FIRST = 64
B_ROWS = 32


def row_order():
    pos = np.arange(128)
    rows = pos + np.where(pos >= B_FIRST, B_ROWS, 0)
    rows[126], rows[16] = 16, 158
    rows[127], rows[32] = 32, 159
    return rows


def constants():
    k = np.arange(N_GRID)
    j = np.arange(N_IMG)
    ang = np.mod((k[:, None] - N_IMG) * (j[None, :] - N_IMG // 2), N_GRID) * (2.0 * np.pi / N_GRID)
    cos_t = np.cos(ang)
    sin_t = np.sin(ang)
    lanes = np.full((LANES,), -1)
    lanes[0:N_IMG] = np.arange(N_IMG)
    used = (lanes >= 0)[None, :]
    src = np.maximum(lanes, 0)
    pick = lambda t: np.where(used, t[:, src], 0.0)
    base = np.arange(ROWS)[:, None] * BLK
    ra = (base + row_order()[None, :]).reshape(-1)
    rb = (base + B_FIRST + np.arange(B_ROWS)[None, :]).reshape(-1)
    bf = jnp.bfloat16
    t3a = np.stack([pick(cos_t)[ra], pick(sin_t)[ra]]).reshape(2, ROWS, 128, LANES).astype(bf)
    t3b = np.stack([pick(cos_t)[rb], pick(sin_t)[rb]]).reshape(2, ROWS * B_ROWS, LANES).astype(bf)
    t2 = np.stack([cos_t.T, sin_t.T]).reshape(2, ROWS, COLS, N_GRID).astype(bf)
    return t2, t3a, t3b


def body(y_h, wr_h, wc_h, gr_h, gc_h, vc, s_h, d_h, t2_h, t3a_h, t3b_h, out_ref,
         y, wr, wc, gr, gc, s_v, din, drow, dcol, dd, rt0, rt1, wd, lb0, lb1, la0, la1, lh, accb, acc, gbb, gb,
         hbufb, recvb, hbuf, recv,
         hs, hr, hrt, t2, t3a, t3b, ib, img, ysend, yrecv,
         in_sem, tab_sem, send_sem, recv_sem, hsend_sem, hrecv_sem, ysend_sem, yrecv_sem):
    rts = (rt0, rt1)
    lefts_b = (lb0, lb1)
    lefts = (la0, la1)
    me = lax.axis_index('rows')
    cid = lax.axis_index('coil')
    nxt = lax.rem(me + 1, ROWS)
    prv = lax.rem(me + ROWS - 1, ROWS)
    other = 1 - cid

    ins = [pltpu.make_async_copy(a, b, in_sem.at[n]) for n, (a, b) in enumerate(
        ((gc_h, gc), (wc_h, wc), (gr_h, gr), (wr_h, wr), (y_h.at[0], y.at[0:8]), (y_h.at[1], y.at[8:16])))]
    for c in ins:
        c.start()
    tabs = [(t2_h.at[0], t2.at[:, 0]), (t2_h.at[1], t2.at[:, 1])]
    for g in range(3):
        src = slice(g * 128, g * 128 + 128)
        re = slice(g * 256, g * 256 + 128)
        im = slice(g * 256 + 128, g * 256 + 256)
        tabs += [
            (t3b_h.at[0, :, src], t3b.at[0, :, re]),
            (t3b_h.at[1, :, src], t3b.at[0, :, im]),
            (t3b_h.at[0, :, src], t3b.at[1, :, im]),
            (t3a_h.at[0, :, :, src], t3a.at[:, :, re]),
            (t3a_h.at[1, :, :, src], t3a.at[:, :, im]),
        ]
    tabs += [(s_h, s_v), (d_h, din)]
    tabs = [pltpu.make_async_copy(a, b, tab_sem.at[n]) for n, (a, b) in enumerate(tabs)]
    for c in tabs:
        c.start()

    barrier = pltpu.get_barrier_semaphore()
    for d in range(1, ROWS):
        pl.semaphore_signal(barrier, inc=1, device_id={'rows': lax.rem(me + d, ROWS)}, device_id_type=MESH)
    pl.semaphore_signal(barrier, inc=1, device_id={'coil': other}, device_id_type=MESH)
    for c in ins:
        c.wait()
    pl.semaphore_wait(barrier, 4)

    pieces = [(k * KC + o, 256) for k in range(NK) for o in range(0, KC, 256)]

    def build_wd(lo, groups):
        sl = pl.ds(lo, 256)
        keep = (lax.broadcasted_iota(jnp.int32, (1, 256), 1) + lo < vc[0]).astype(F32)
        first = gr[:, sl] - me * BLK
        taps = [(jnp.broadcast_to(first + (a - 2), (8, 256)), jnp.broadcast_to(wr[a:a + 1, sl] * keep, (8, 256)))
                for a in range(4)]
        ids = lax.broadcasted_iota(jnp.int32, (8, 1), 0)
        for n in groups:
            if n < 16:
                r = ids + (n * 8 + (B_ROWS if n * 8 >= B_FIRST else 0))
            elif n < 20:
                r = ids + (n * 8 - 128 + B_FIRST)
            else:
                r = jnp.where(ids == 0, BLK, ids - 3)
            for p, v in ((126, 16), (127, 32), (16, 158), (32, 159)):
                if p // 8 == n:
                    r = jnp.where(ids == p % 8, v, r)
            w = jnp.zeros((8, 256), F32)
            for t, v in taps:
                w = jnp.where(r == t, v, w)
            wd[n * 8:n * 8 + 8, sl] = w

    def build_rt(lo):
        sl = pl.ds(lo, 256)
        k, off = lo // HALF, lo % HALF
        col = gc[:, sl]
        taps = []
        for b in range(4):
            t = col + (b - 2)
            t = jnp.where(t < 0, t + N_GRID, jnp.where(t >= N_GRID, t - N_GRID, t))
            taps.append((jnp.broadcast_to(t, (16, 256)).astype(jnp.int16),
                         jnp.broadcast_to(wc[b:b + 1, sl], (16, 256)).astype(BF)))
        base = lax.broadcasted_iota(jnp.int16, (16, 256), 0)
        for n in range(N_GRID // 16):
            ids = base + jnp.int16(n * 16)
            w = jnp.zeros((16, 256), BF)
            for t, v in taps:
                w = jnp.where(ids == t, v, w)
            rts[k][n * 16:(n + 1) * 16, off:off + 256] = w

    def build_left_b(k, off):
        sl = pl.ds(k * KC + off, 256)
        w = wd[128:160, sl]
        for q in range(2):
            for c in range(NC):
                lo = q * 256 + c * 32
                lefts_b[k % 2][lo:lo + 32, off:off + 256] = (y[q * 8 + c:q * 8 + c + 1, sl] * w).astype(BF)

    def build_halo(lo):
        sl = pl.ds(lo, 256)
        for h in range(3):
            lh[h * 16:h * 16 + 16, sl] = (y[:, sl] * wd[160 + h:161 + h, sl]).astype(BF)

    def left_a_piece(c, lo):
        k, off = lo // HALF, lo % HALF
        sl = pl.ds(lo, 256)
        rows = [jnp.broadcast_to(y[pl.ds(q * 8 + c, 1), sl], (16, 256)) for q in range(2)]
        for n in range(8):
            w = wd[n * 16:n * 16 + 16, sl]
            for q, row in enumerate(rows):
                lefts[k][q * 128 + n * 16:q * 128 + n * 16 + 16, off:off + 256] = (row * w).astype(BF)

    def build_left_a(c, k):
        for off in range(0, HALF, 256):
            left_a_piece(c, k * HALF + off)

    def nt(a, b):
        return lax.dot_general(a, b, (((1,), (1,)), ((), ())), preferred_element_type=F32)

    def exchange(stage):
        if stage is None:
            src, dst, idx = hbufb, recvb, NC
        else:
            src, dst, idx = hbuf.at[stage], recv.at[stage], stage
        return [pltpu.make_async_remote_copy(
            src_ref=src.at[lax.rem(me + d, ROWS)], dst_ref=dst.at[me],
            send_sem=send_sem.at[idx, d - 1], recv_sem=recv_sem.at[idx, 3 - d],
            device_id={'rows': lax.rem(me + d, ROWS)}, device_id_type=MESH) for d in (1, 2, 3)]

    def received(stage):
        if stage is None:
            src, dst, idx = hbufb, recvb, NC
        else:
            src, dst, idx = hbuf.at[stage], recv.at[stage], stage
        return [pltpu.make_async_remote_copy(
            src_ref=src.at[0], dst_ref=dst.at[lax.rem(me + d, ROWS)],
            send_sem=send_sem.at[idx, d - 1], recv_sem=recv_sem.at[idx, d - 1],
            device_id={'rows': lax.rem(me + d, ROWS)}, device_id_type=MESH) for d in (1, 2, 3)]

    def transform(stage):
        g_ref, h_ref, r_ref = (gbb, hbufb, recvb) if stage is None else (gb, hbuf.at[stage], recv.at[stage])
        n = g_ref.shape[1] // 2
        for h in range(2):
            table = t2[2 * h:2 * h + 2].reshape(N_IMG, N_GRID)
            with_re = jnp.dot(table, g_ref[:, 0:n], preferred_element_type=F32) if n == 256 else None
            with_im = jnp.dot(table, g_ref[:, n:], preferred_element_type=F32) if n == 256 else None
            if n < 256:
                both = jnp.dot(table, g_ref[...], preferred_element_type=F32)
                with_re, with_im = both[:, 0:n], both[:, n:]
            for p in range(2):
                lo = p * 2 * COLS
                mid = lo + COLS
                end = mid + COLS
                h_ref[2 * h + p, 0:COLS] = (with_re[lo:mid] - with_im[mid:end]).astype(BF)
                h_ref[2 * h + p, COLS:] = (with_re[mid:end] + with_im[lo:mid]).astype(BF)

    def send(stage):
        h_ref, r_ref = (hbufb, recvb) if stage is None else (hbuf.at[stage], recv.at[stage])
        for c in exchange(stage):
            c.start()
        r_ref[me] = h_ref[me]

    parts = [(0, 0, 256), (0, 256, KC - 256)] + [(k, 0, KC) for k in range(1, NK)]

    def build_first(k, off, size):
        for o in range(off, off + size, 256):
            build_rt(k * KC + o)
            build_wd(k * KC + o, (16, 17, 18, 19, 20))
            build_left_b(k, o)
            build_halo(k * KC + o)

    def first_stage(n):
        k, off, size = parts[n]
        lo = (k % 2) * KC + off
        for q in range(2):
            cs = slice(q * 256, q * 256 + 256)
            part = nt(rts[k // 2][:, lo:lo + size], lefts_b[k % 2][cs, off:off + size])
            if n == 0:
                accb[:, cs] = part
            elif n + 1 < len(parts):
                accb[:, cs] += part
            else:
                gbb[:, cs] = (accb[:, cs] + part).astype(BF)

    build_first(*parts[0])
    for n in range(len(parts) - 1):
        first_stage(n)
        build_first(*parts[n + 1])

    for h in range(2):
        rows = slice(h * 320, h * 320 + 320)
        halo = nt(rts[0][rows, :], lh[:, 0:HALF]) + nt(rts[1][rows, :], lh[:, HALF:])
        hrt[rows, 0:48] = halo
    for lo in range(0, HALF, 256):
        build_wd(lo, range(16))
        left_a_piece(0, lo)
    hs[...] = hrt[...].T[0:48]
    to_next = pltpu.make_async_remote_copy(
        src_ref=hs.at[0:16], dst_ref=hr.at[0:16], send_sem=hsend_sem.at[0], recv_sem=hrecv_sem.at[0],
        device_id={'rows': nxt}, device_id_type=MESH)
    to_prev = pltpu.make_async_remote_copy(
        src_ref=hs.at[16:48], dst_ref=hr.at[16:48], send_sem=hsend_sem.at[1], recv_sem=hrecv_sem.at[1],
        device_id={'rows': prv}, device_id_type=MESH)
    to_next.start()
    to_prev.start()
    for c in tabs:
        c.wait()

    first_stage(len(parts) - 1)
    for g in range(3):
        t3b[1, :, g * 256:g * 256 + 128] = -t3b[0, :, g * 256 + 128:g * 256 + 256]
    drow[...] = din[...].reshape(1, N_IMG)
    dcol[...] = jnp.broadcast_to(din[...].reshape(1, N_IMG), (8, N_IMG)).T
    mine = jnp.where(cid == 0, drow[:, 0:BLK], drow[:, BLK:])
    dd[...] = dcol[pl.ds(pl.multiple_of(me * COLS, COLS), COLS), 0:1] * mine
    img[...] = jnp.zeros_like(img)
    transform(None)
    send(None)

    def spread_head(c, first=False):
        for h in range(2):
            rows = slice(h * 320, h * 320 + 320)
            acc[rows, :] = nt(rts[0][rows, :], lefts[0][...])
        for lo in range(HALF, SLOTS, 256):
            if first:
                build_wd(lo, range(16))
            left_a_piece(c, lo)

    lane = lax.broadcasted_iota(jnp.int32, (1, 128), 1)
    edge = (lane == 0) | (lane == 16) | (lane == 32)

    def spread_tail(c):
        for h in range(2):
            rows = slice(h * 320, h * 320 + 320)
            part = nt(rts[1][rows, :], lefts[1][...])
            for q in range(2):
                cs = slice(q * 128, q * 128 + 128)
                rolled = pltpu.roll(hrt[rows, :], 128 - (q * 8 + c), 1)
                gb[rows, cs] = (acc[rows, cs] + part[:, cs] + jnp.where(edge, rolled, 0.0)).astype(BF)

    def image_first():
        for c in received(None):
            c.wait_recv()
        for c in range(NC):
            blocks = [recvb[p, b * COLS:(b + 1) * COLS, c * 32:c * 32 + 32] for b in range(2) for p in range(ROWS)]
            lhs = jnp.concatenate(blocks, axis=1)
            ib[c] = jnp.dot(lhs, t3b[...].reshape(256, 2 * LANES), preferred_element_type=F32)

    def image_wait(c):
        for x in received(c):
            x.wait_recv()

    def image_coil(c):
        lhs = jnp.concatenate([recv[c, p] for p in range(ROWS)], axis=1)
        for g in range(3):
            lanes = slice(g * 256, g * 256 + 256)
            tot = jnp.dot(lhs, t3a[:, :, lanes].reshape(4 * 128, 256), preferred_element_type=F32)
            re = ib[c, :, g * 256:g * 256 + 128] + (tot[0:COLS, 0:128] - tot[COLS:, 128:])
            im = ib[c, :, g * 256 + 128:g * 256 + 256] + (tot[0:COLS, 128:] + tot[COLS:, 0:128])
            n = min(128, N_IMG - g * 128)
            at = slice(g * 128, g * 128 + n)
            sr = s_v[0, c, :, at]
            si = s_v[1, c, :, at]
            img[0, :, at] += sr * re[:, 0:n] + si * im[:, 0:n]
            img[1, :, at] += sr * im[:, 0:n] - si * re[:, 0:n]

    spread_head(0, True)

    @pl.loop(0, LAG)
    def _(c):
        @pl.when(c == 0)
        def _():
            to_next.wait()
            to_prev.wait()
            hrt[...] = jnp.concatenate([hr[...], jnp.zeros((80, N_GRID), F32)], axis=0).T

        spread_tail(c)
        build_left_a(c + 1, 0)
        transform(c)
        spread_head(c + 1)
        send(c)

    image_first()

    @pl.loop(LAG, NC - 1)
    def _(c):
        image_wait(c - LAG)
        spread_tail(c)
        build_left_a(c + 1, 0)
        image_coil(c - LAG)
        transform(c)
        spread_head(c + 1)
        send(c)

    spread_tail(NC - 1)
    transform(NC - 1)
    send(NC - 1)

    @pl.loop(NC - 1 - LAG, NC)
    def _(c):
        image_wait(c)
        image_coil(c)

    halves = [jnp.where(cid == 0, img[e, :, BLK:N_IMG], img[e, :, 0:BLK]) for e in range(2)]
    ysend[...] = jnp.concatenate([x[r:r + COLS // 2] for x in halves for r in (0, COLS // 2)], axis=1)
    swap = pltpu.make_async_remote_copy(
        src_ref=ysend, dst_ref=yrecv, send_sem=ysend_sem, recv_sem=yrecv_sem,
        device_id={'coil': other}, device_id_type=MESH)
    swap.start()
    swap.wait()
    for e in range(2):
        lo = e * 2 * BLK
        theirs = jnp.concatenate([yrecv[:, lo:lo + BLK], yrecv[:, lo + BLK:lo + 2 * BLK]], axis=0)
        total = (jnp.where(cid == 0, img[e, :, 0:BLK], img[e, :, BLK:N_IMG]) + theirs) * dd[...]
        out_ref[e] = total.T
    for stage in [None] + list(range(NC)):
        for c in received(stage):
            c.wait_send()


def solution(mesh):
    t2c, t3ac, t3bc = constants()

    def local_part(kspace, weight_row, weight_col, grid_row, grid_col, valid_count, coil_maps, deapod):
        any_spec = pl.BlockSpec(memory_space=pl.ANY)
        dma = pltpu.SemaphoreType.DMA
        return pl.pallas_call(
            body,
            out_shape=pltpu.VMEM((2, BLK, COLS), F32),
            in_specs=[any_spec] * 5 + [pl.BlockSpec(memory_space=pltpu.SMEM)] + [any_spec] * 5,
            out_specs=pl.BlockSpec(memory_space=pltpu.VMEM),
            scratch_shapes=[
                pltpu.VMEM((2 * NC, SLOTS), F32),
                pltpu.VMEM((4, SLOTS), F32),
                pltpu.VMEM((4, SLOTS), F32),
                pltpu.VMEM((1, SLOTS), jnp.int32),
                pltpu.VMEM((1, SLOTS), jnp.int32),
                pltpu.VMEM((2, NC, COLS, N_IMG), F32),
                pltpu.VMEM((N_IMG,), F32),
                pltpu.VMEM((1, N_IMG), F32),
                pltpu.VMEM((N_IMG, 8), F32),
                pltpu.VMEM((COLS, BLK), F32),
                pltpu.VMEM((N_GRID, HALF), BF),
                pltpu.VMEM((N_GRID, HALF), BF),
                pltpu.VMEM((168, SLOTS), F32),
                pltpu.VMEM((512, KC), BF),
                pltpu.VMEM((512, KC), BF),
                pltpu.VMEM((256, HALF), BF),
                pltpu.VMEM((256, HALF), BF),
                pltpu.VMEM((48, SLOTS), BF),
                pltpu.VMEM((N_GRID, 512), F32),
                pltpu.VMEM((N_GRID, 256), F32),
                pltpu.VMEM((N_GRID, 512), BF),
                pltpu.VMEM((N_GRID, 256), BF),
                pltpu.VMEM((ROWS, 2 * COLS, 256), BF),
                pltpu.VMEM((ROWS, 2 * COLS, 256), BF),
                pltpu.VMEM((NC, ROWS, 2 * COLS, 128), BF),
                pltpu.VMEM((NC, ROWS, 2 * COLS, 128), BF),
                pltpu.VMEM((48, N_GRID), F32),
                pltpu.VMEM((48, N_GRID), F32),
                pltpu.VMEM((N_GRID, 128), F32),
                pltpu.VMEM((ROWS, 2, COLS, N_GRID), BF),
                pltpu.VMEM((ROWS, 128, 2 * LANES), BF),
                pltpu.VMEM((2, ROWS * B_ROWS, 2 * LANES), BF),
                pltpu.VMEM((NC, COLS, 2 * LANES), F32),
                pltpu.VMEM((2, COLS, N_IMG), F32),
                pltpu.VMEM((COLS // 2, 4 * BLK), F32),
                pltpu.VMEM((COLS // 2, 4 * BLK), F32),
                dma((6,)), dma((19,)), dma((9, 3)), dma((9, 3)), dma((2,)), dma((2,)), dma, dma,
            ],
            compiler_params=pltpu.CompilerParams(collective_id=0, has_side_effects=True, vmem_limit_bytes=60 * 1024 * 1024),
            name='nufft_adjoint',
        )(kspace, weight_row, weight_col, grid_row.reshape(1, SLOTS), grid_col.reshape(1, SLOTS), valid_count,
          jnp.swapaxes(coil_maps, 2, 3), deapod, jnp.asarray(t2c), jnp.asarray(t3ac), jnp.asarray(t3bc))

    spec_samples = P(None, 'coil', ('slab', 'rows'))
    spec_weights = P(None, ('slab', 'rows'))
    spec_index = P(('slab', 'rows'))
    return jax.shard_map(local_part, mesh=mesh, in_specs=(spec_samples, spec_weights, spec_weights, spec_index, spec_index, spec_index, P(None, 'coil', 'slab', 'rows'), P()), out_specs=P(None, ('slab', 'coil'), 'rows'), check_vma=False)
```

```python
import functools
import numpy as np
import jax
import jax.numpy as jnp
from jax import lax
from jax.experimental import pallas as pl
from jax.experimental.pallas import tpu as pltpu
from jax.sharding import PartitionSpec as P

MESH = pl.DeviceIdType.MESH
BF = jnp.bfloat16
F32 = jnp.float32

N_IMG = 320
N_GRID = 640
ROWS = 4
BLK = 160
COLS = 80
NC = 8
SLOTS = 5120
KC = 1280
NK = SLOTS // KC
LANES = 384
HALF = SLOTS // 2
LAG = 3
W = 256
B_FIRST = 64
B_ROWS = 32


def row_order():
    pos = np.arange(128)
    rows = pos + np.where(pos >= B_FIRST, B_ROWS, 0)
    rows[126], rows[16] = 16, 158
    rows[127], rows[32] = 32, 159
    return rows


def constants():
    k = np.arange(N_GRID)
    j = np.arange(N_IMG)
    ang = np.mod((k[:, None] - N_IMG) * (j[None, :] - N_IMG // 2), N_GRID) * (2.0 * np.pi / N_GRID)
    cos_t = np.cos(ang)
    sin_t = np.sin(ang)
    lanes = np.full((LANES,), -1)
    lanes[0:N_IMG] = np.arange(N_IMG)
    used = (lanes >= 0)[None, :]
    src = np.maximum(lanes, 0)
    pick = lambda t: np.where(used, t[:, src], 0.0)
    base = np.arange(ROWS)[:, None] * BLK
    ra = (base + row_order()[None, :]).reshape(-1)
    rb = (base + B_FIRST + np.arange(B_ROWS)[None, :]).reshape(-1)
    bf = jnp.bfloat16
    t3a = np.stack([pick(cos_t)[ra], pick(sin_t)[ra]]).reshape(2, ROWS, 128, LANES).astype(bf)
    t3b = np.stack([pick(cos_t)[rb], pick(sin_t)[rb]]).reshape(2, ROWS * B_ROWS, LANES).astype(bf)
    t2 = np.stack([cos_t.T, sin_t.T]).reshape(2, ROWS, COLS, N_GRID).astype(bf)
    return t2, t3a, t3b


def body(y_h, wr_h, wc_h, gr_h, gc_h, vc, s_h, d_h, t2_h, t3a_h, t3b_h, out_ref,
         y, wr, wc, gr, gc, s_v, din, drow, dcol, dd, rt0, rt1, wd, lb0, lb1, la0, la1, lh, accb, acc, gbb, gb,
         hbufb, recvb, hbuf, recv,
         hs, hr, hrt, t2, t3a, t3b, ib, img, ysend, yrecv,
         in_sem, tab_sem, send_sem, recv_sem, hsend_sem, hrecv_sem, ysend_sem, yrecv_sem):
    rts = (rt0, rt1)
    lefts_b = (lb0, lb1)
    lefts = (la0, la1)
    me = lax.axis_index('rows')
    cid = lax.axis_index('coil')
    nxt = lax.rem(me + 1, ROWS)
    prv = lax.rem(me + ROWS - 1, ROWS)
    other = 1 - cid

    ins = [pltpu.make_async_copy(a, b, in_sem.at[n]) for n, (a, b) in enumerate(
        ((gc_h, gc), (wc_h, wc), (gr_h, gr), (wr_h, wr), (y_h.at[0], y.at[0:8]), (y_h.at[1], y.at[8:16])))]
    for c in ins:
        c.start()
    tabs = [(t2_h.at[0], t2.at[:, 0]), (t2_h.at[1], t2.at[:, 1])]
    for g in range(3):
        src = slice(g * 128, g * 128 + 128)
        re = slice(g * 256, g * 256 + 128)
        im = slice(g * 256 + 128, g * 256 + 256)
        tabs += [
            (t3b_h.at[0, :, src], t3b.at[0, :, re]),
            (t3b_h.at[1, :, src], t3b.at[0, :, im]),
            (t3b_h.at[0, :, src], t3b.at[1, :, im]),
            (t3a_h.at[0, :, :, src], t3a.at[:, :, re]),
            (t3a_h.at[1, :, :, src], t3a.at[:, :, im]),
        ]
    tabs += [(s_h, s_v), (d_h, din)]
    tabs = [pltpu.make_async_copy(a, b, tab_sem.at[n]) for n, (a, b) in enumerate(tabs)]
    barrier = pltpu.get_barrier_semaphore()
    for d in range(1, ROWS):
        pl.semaphore_signal(barrier, inc=1, device_id={'rows': lax.rem(me + d, ROWS)}, device_id_type=MESH)
    pl.semaphore_signal(barrier, inc=1, device_id={'coil': other}, device_id_type=MESH)
    for c in ins:
        c.wait()
    for c in tabs:
        c.start()
    pl.semaphore_wait(barrier, 4)

    def build_wd(lo, groups):
        sl = pl.ds(lo, W)
        keep = (lax.broadcasted_iota(jnp.int32, (1, W), 1) + lo < vc[0]).astype(F32)
        first = gr[:, sl] - me * BLK
        taps = [(jnp.broadcast_to(first + (a - 2), (8, W)), jnp.broadcast_to(wr[a:a + 1, sl] * keep, (8, W)))
                for a in range(4)]
        ids = lax.broadcasted_iota(jnp.int32, (8, 1), 0)
        for n in groups:
            if n < 16:
                r = ids + (n * 8 + (B_ROWS if n * 8 >= B_FIRST else 0))
            elif n < 20:
                r = ids + (n * 8 - 128 + B_FIRST)
            else:
                r = jnp.where(ids == 0, BLK, ids - 3)
            for p, v in ((126, 16), (127, 32), (16, 158), (32, 159)):
                if p // 8 == n:
                    r = jnp.where(ids == p % 8, v, r)
            w = jnp.zeros((8, W), F32)
            for t, v in taps:
                w = jnp.where(r == t, v, w)
            wd[n * 8:n * 8 + 8, sl] = w

    def build_rt(lo):
        sl = pl.ds(lo, W)
        k, off = lo // HALF, lo % HALF
        col = gc[:, sl]
        taps = []
        for b in range(4):
            t = col + (b - 2)
            t = jnp.where(t < 0, t + N_GRID, jnp.where(t >= N_GRID, t - N_GRID, t))
            taps.append((jnp.broadcast_to(t, (16, W)).astype(jnp.int16),
                         jnp.broadcast_to(wc[b:b + 1, sl], (16, W)).astype(BF)))
        base = lax.broadcasted_iota(jnp.int16, (16, W), 0)
        for n in range(N_GRID // 16):
            ids = base + jnp.int16(n * 16)
            w = jnp.zeros((16, W), BF)
            for t, v in taps:
                w = jnp.where(ids == t, v, w)
            rts[k][n * 16:(n + 1) * 16, off:off + W] = w

    def build_left_b(k, off):
        sl = pl.ds(k * KC + off, W)
        w = wd[128:160, sl]
        for q in range(2):
            for c in range(NC):
                lo = q * 256 + c * 32
                lefts_b[k % 2][lo:lo + 32, off:off + W] = (y[q * 8 + c:q * 8 + c + 1, sl] * w).astype(BF)

    def build_halo(lo):
        sl = pl.ds(lo, W)
        for h in range(3):
            lh[h * 16:h * 16 + 16, sl] = (y[:, sl] * wd[160 + h:161 + h, sl]).astype(BF)

    def left_a_piece(c, lo):
        k, off = lo // HALF, lo % HALF
        sl = pl.ds(lo, W)
        rows = [jnp.broadcast_to(y[pl.ds(q * 8 + c, 1), sl], (16, W)) for q in range(2)]
        for n in range(8):
            w = wd[n * 16:n * 16 + 16, sl]
            for q, row in enumerate(rows):
                lefts[k][q * 128 + n * 16:q * 128 + n * 16 + 16, off:off + W] = (row * w).astype(BF)

    def build_left_a(c, k):
        for off in range(0, HALF, W):
            left_a_piece(c, k * HALF + off)

    def nt(a, b):
        return lax.dot_general(a, b, (((1,), (1,)), ((), ())), preferred_element_type=F32)

    def exchange(stage):
        if stage is None:
            src, dst, idx = hbufb, recvb, NC
        else:
            src, dst, idx = hbuf.at[stage], recv.at[stage], stage
        return [pltpu.make_async_remote_copy(
            src_ref=src.at[lax.rem(me + d, ROWS)], dst_ref=dst.at[me],
            send_sem=send_sem.at[idx, d - 1], recv_sem=recv_sem.at[idx, 3 - d],
            device_id={'rows': lax.rem(me + d, ROWS)}, device_id_type=MESH) for d in (1, 2, 3)]

    def received(stage):
        if stage is None:
            src, dst, idx = hbufb, recvb, NC
        else:
            src, dst, idx = hbuf.at[stage], recv.at[stage], stage
        return [pltpu.make_async_remote_copy(
            src_ref=src.at[0], dst_ref=dst.at[lax.rem(me + d, ROWS)],
            send_sem=send_sem.at[idx, d - 1], recv_sem=recv_sem.at[idx, d - 1],
            device_id={'rows': lax.rem(me + d, ROWS)}, device_id_type=MESH) for d in (1, 2, 3)]

    def transform(stage):
        g_ref, h_ref, r_ref = (gbb, hbufb, recvb) if stage is None else (gb, hbuf.at[stage], recv.at[stage])
        n = g_ref.shape[1] // 2
        for h in range(2):
            table = t2[2 * h:2 * h + 2].reshape(N_IMG, N_GRID)
            with_re = jnp.dot(table, g_ref[:, 0:n], preferred_element_type=F32) if n == 256 else None
            with_im = jnp.dot(table, g_ref[:, n:], preferred_element_type=F32) if n == 256 else None
            if n < 256:
                both = jnp.dot(table, g_ref[...], preferred_element_type=F32)
                with_re, with_im = both[:, 0:n], both[:, n:]
            for p in range(2):
                lo = p * 2 * COLS
                mid = lo + COLS
                end = mid + COLS
                h_ref[2 * h + p, 0:COLS] = (with_re[lo:mid] - with_im[mid:end]).astype(BF)
                h_ref[2 * h + p, COLS:] = (with_re[mid:end] + with_im[lo:mid]).astype(BF)

    def send(stage):
        h_ref, r_ref = (hbufb, recvb) if stage is None else (hbuf.at[stage], recv.at[stage])
        for c in exchange(stage):
            c.start()
        r_ref[me] = h_ref[me]

    parts = [(0, 0, 256), (0, 256, KC - 256)] + [(k, 0, KC) for k in range(1, NK)]

    def build_first(k, off, size):
        for o in range(off, off + size, W):
            build_rt(k * KC + o)
            build_wd(k * KC + o, (16, 17, 18, 19, 20))
            build_left_b(k, o)
            build_halo(k * KC + o)

    def first_stage(n):
        k, off, size = parts[n]
        lo = (k % 2) * KC + off
        for q in range(2):
            cs = slice(q * 256, q * 256 + 256)
            part = nt(rts[k // 2][:, lo:lo + size], lefts_b[k % 2][cs, off:off + size])
            if n == 0:
                accb[:, cs] = part
            elif n + 1 < len(parts):
                accb[:, cs] += part
            else:
                gbb[:, cs] = (accb[:, cs] + part).astype(BF)

    def halo(k):
        lo = (k % 2) * KC
        for h in range(2):
            rows = slice(h * 320, h * 320 + 320)
            part = nt(rts[k // 2][rows, lo:lo + KC], lh[:, k * KC:(k + 1) * KC])
            hrt[rows, 0:48] = part if k == 0 else hrt[rows, 0:48] + part

    build_first(*parts[0])
    for n in range(len(parts) - 1):
        first_stage(n)
        if n > 0:
            halo(parts[n][0])
        build_first(*parts[n + 1])
    halo(NK - 1)
    for lo in range(0, HALF, W):
        build_wd(lo, range(16))
        left_a_piece(0, lo)
    hs[...] = hrt[...].T[0:48]
    to_next = pltpu.make_async_remote_copy(
        src_ref=hs.at[0:16], dst_ref=hr.at[0:16], send_sem=hsend_sem.at[0], recv_sem=hrecv_sem.at[0],
        device_id={'rows': nxt}, device_id_type=MESH)
    to_prev = pltpu.make_async_remote_copy(
        src_ref=hs.at[16:48], dst_ref=hr.at[16:48], send_sem=hsend_sem.at[1], recv_sem=hrecv_sem.at[1],
        device_id={'rows': prv}, device_id_type=MESH)
    to_next.start()
    to_prev.start()
    for c in tabs:
        c.wait()

    first_stage(len(parts) - 1)
    for g in range(3):
        t3b[1, :, g * 256:g * 256 + 128] = -t3b[0, :, g * 256 + 128:g * 256 + 256]
    drow[...] = din[...].reshape(1, N_IMG)
    dcol[...] = jnp.broadcast_to(din[...].reshape(1, N_IMG), (8, N_IMG)).T
    mine = jnp.where(cid == 0, drow[:, 0:BLK], drow[:, BLK:])
    dd[...] = dcol[pl.ds(pl.multiple_of(me * COLS, COLS), COLS), 0:1] * mine
    img[...] = jnp.zeros_like(img)
    transform(None)
    send(None)

    def spread_head(c, first=False):
        for h in range(2):
            rows = slice(h * 320, h * 320 + 320)
            acc[rows, :] = nt(rts[0][rows, :], lefts[0][...])
        for lo in range(HALF, SLOTS, W):
            if first:
                build_wd(lo, range(16))
            left_a_piece(c, lo)

    lane = lax.broadcasted_iota(jnp.int32, (1, 128), 1)
    edge = (lane == 0) | (lane == 16) | (lane == 32)

    def spread_tail(c):
        for h in range(2):
            rows = slice(h * 320, h * 320 + 320)
            part = nt(rts[1][rows, :], lefts[1][...])
            for q in range(2):
                cs = slice(q * 128, q * 128 + 128)
                rolled = pltpu.roll(hrt[rows, :], 128 - (q * 8 + c), 1)
                gb[rows, cs] = (acc[rows, cs] + part[:, cs] + jnp.where(edge, rolled, 0.0)).astype(BF)

    def image_first():
        for c in received(None):
            c.wait_recv()
        for c in range(NC):
            blocks = [recvb[p, b * COLS:(b + 1) * COLS, c * 32:c * 32 + 32] for b in range(2) for p in range(ROWS)]
            lhs = jnp.concatenate(blocks, axis=1)
            ib[c] = jnp.dot(lhs, t3b[...].reshape(256, 2 * LANES), preferred_element_type=F32)

    def image_wait(c):
        for x in received(c):
            x.wait_recv()

    def image_coil(c):
        lhs = jnp.concatenate([recv[c, p] for p in range(ROWS)], axis=1)
        for g in range(3):
            lanes = slice(g * 256, g * 256 + 256)
            tot = jnp.dot(lhs, t3a[:, :, lanes].reshape(4 * 128, 256), preferred_element_type=F32)
            re = ib[c, :, g * 256:g * 256 + 128] + (tot[0:COLS, 0:128] - tot[COLS:, 128:])
            im = ib[c, :, g * 256 + 128:g * 256 + 256] + (tot[0:COLS, 128:] + tot[COLS:, 0:128])
            n = min(128, N_IMG - g * 128)
            at = slice(g * 128, g * 128 + n)
            sr = s_v[0, c, :, at]
            si = s_v[1, c, :, at]
            img[0, :, at] += sr * re[:, 0:n] + si * im[:, 0:n]
            img[1, :, at] += sr * im[:, 0:n] - si * re[:, 0:n]

    spread_head(0, True)

    @pl.loop(0, LAG)
    def _(c):
        @pl.when(c == 0)
        def _():
            to_next.wait()
            to_prev.wait()
            hrt[...] = jnp.concatenate([hr[...], jnp.zeros((80, N_GRID), F32)], axis=0).T

        spread_tail(c)
        build_left_a(c + 1, 0)
        transform(c)
        spread_head(c + 1)
        send(c)

    image_first()

    @pl.loop(LAG, NC - 2)
    def _(c):
        image_wait(c - LAG)
        spread_tail(c)
        build_left_a(c + 1, 0)
        image_coil(c - LAG)
        transform(c)
        spread_head(c + 1)
        send(c)

    c = NC - 2
    image_wait(c - LAG)
    spread_tail(c)
    build_left_a(c + 1, 0)
    image_coil(c - LAG)
    transform(c)
    send(c)
    spread_head(c + 1)
    spread_tail(c + 1)
    transform(c + 1)
    send(c + 1)

    @pl.loop(NC - 1 - LAG, NC)
    def _(c):
        image_wait(c)
        image_coil(c)

    halves = [jnp.where(cid == 0, img[e, :, BLK:N_IMG], img[e, :, 0:BLK]) for e in range(2)]
    ysend[...] = jnp.concatenate([x[r:r + COLS // 2] for x in halves for r in (0, COLS // 2)], axis=1)
    swap = pltpu.make_async_remote_copy(
        src_ref=ysend, dst_ref=yrecv, send_sem=ysend_sem, recv_sem=yrecv_sem,
        device_id={'coil': other}, device_id_type=MESH)
    swap.start()
    swap.wait()
    for e in range(2):
        lo = e * 2 * BLK
        theirs = jnp.concatenate([yrecv[:, lo:lo + BLK], yrecv[:, lo + BLK:lo + 2 * BLK]], axis=0)
        total = (jnp.where(cid == 0, img[e, :, 0:BLK], img[e, :, BLK:N_IMG]) + theirs) * dd[...]
        out_ref[e] = total.T
    for stage in [None] + list(range(NC)):
        for c in received(stage):
            c.wait_send()


def solution(mesh):
    t2c, t3ac, t3bc = constants()

    def local_part(kspace, weight_row, weight_col, grid_row, grid_col, valid_count, coil_maps, deapod):
        any_spec = pl.BlockSpec(memory_space=pl.ANY)
        dma = pltpu.SemaphoreType.DMA
        return pl.pallas_call(
            body,
            out_shape=pltpu.VMEM((2, BLK, COLS), F32),
            in_specs=[any_spec] * 5 + [pl.BlockSpec(memory_space=pltpu.SMEM)] + [any_spec] * 5,
            out_specs=pl.BlockSpec(memory_space=pltpu.VMEM),
            scratch_shapes=[
                pltpu.VMEM((2 * NC, SLOTS), F32),
                pltpu.VMEM((4, SLOTS), F32),
                pltpu.VMEM((4, SLOTS), F32),
                pltpu.VMEM((1, SLOTS), jnp.int32),
                pltpu.VMEM((1, SLOTS), jnp.int32),
                pltpu.VMEM((2, NC, COLS, N_IMG), F32),
                pltpu.VMEM((N_IMG,), F32),
                pltpu.VMEM((1, N_IMG), F32),
                pltpu.VMEM((N_IMG, 8), F32),
                pltpu.VMEM((COLS, BLK), F32),
                pltpu.VMEM((N_GRID, HALF), BF),
                pltpu.VMEM((N_GRID, HALF), BF),
                pltpu.VMEM((168, SLOTS), F32),
                pltpu.VMEM((512, KC), BF),
                pltpu.VMEM((512, KC), BF),
                pltpu.VMEM((256, HALF), BF),
                pltpu.VMEM((256, HALF), BF),
                pltpu.VMEM((48, SLOTS), BF),
                pltpu.VMEM((N_GRID, 512), F32),
                pltpu.VMEM((N_GRID, 256), F32),
                pltpu.VMEM((N_GRID, 512), BF),
                pltpu.VMEM((N_GRID, 256), BF),
                pltpu.VMEM((ROWS, 2 * COLS, 256), BF),
                pltpu.VMEM((ROWS, 2 * COLS, 256), BF),
                pltpu.VMEM((NC, ROWS, 2 * COLS, 128), BF),
                pltpu.VMEM((NC, ROWS, 2 * COLS, 128), BF),
                pltpu.VMEM((48, N_GRID), F32),
                pltpu.VMEM((48, N_GRID), F32),
                pltpu.VMEM((N_GRID, 128), F32),
                pltpu.VMEM((ROWS, 2, COLS, N_GRID), BF),
                pltpu.VMEM((ROWS, 128, 2 * LANES), BF),
                pltpu.VMEM((2, ROWS * B_ROWS, 2 * LANES), BF),
                pltpu.VMEM((NC, COLS, 2 * LANES), F32),
                pltpu.VMEM((2, COLS, N_IMG), F32),
                pltpu.VMEM((COLS // 2, 4 * BLK), F32),
                pltpu.VMEM((COLS // 2, 4 * BLK), F32),
                dma((6,)), dma((19,)), dma((9, 3)), dma((9, 3)), dma((2,)), dma((2,)), dma, dma,
            ],
            compiler_params=pltpu.CompilerParams(collective_id=0, has_side_effects=True, vmem_limit_bytes=60 * 1024 * 1024),
            name='nufft_adjoint',
        )(kspace, weight_row, weight_col, grid_row.reshape(1, SLOTS), grid_col.reshape(1, SLOTS), valid_count,
          jnp.swapaxes(coil_maps, 2, 3), deapod, jnp.asarray(t2c), jnp.asarray(t3ac), jnp.asarray(t3bc))

    spec_samples = P(None, 'coil', ('slab', 'rows'))
    spec_weights = P(None, ('slab', 'rows'))
    spec_index = P(('slab', 'rows'))
    return jax.shard_map(local_part, mesh=mesh, in_specs=(spec_samples, spec_weights, spec_weights, spec_index, spec_index, spec_index, P(None, 'coil', 'slab', 'rows'), P()), out_specs=P(None, ('slab', 'coil'), 'rows'), check_vma=False)
```

```python
import functools
import numpy as np
import jax
import jax.numpy as jnp
from jax import lax
from jax.experimental import pallas as pl
from jax.experimental.pallas import tpu as pltpu
from jax.sharding import PartitionSpec as P

MESH = pl.DeviceIdType.MESH
BF = jnp.bfloat16
F32 = jnp.float32

N_IMG = 320
N_GRID = 640
ROWS = 4
BLK = 160
COLS = 80
NC = 8
SLOTS = 5120
KC = 1280
NK = SLOTS // KC
LANES = 384
HALF = SLOTS // 2
LAG = 3
W = 256
B_FIRST = 64
B_ROWS = 32


def row_order():
    pos = np.arange(128)
    rows = pos + np.where(pos >= B_FIRST, B_ROWS, 0)
    rows[126], rows[16] = 16, 158
    rows[127], rows[32] = 32, 159
    return rows


def constants():
    k = np.arange(N_GRID)
    j = np.arange(N_IMG)
    ang = np.mod((k[:, None] - N_IMG) * (j[None, :] - N_IMG // 2), N_GRID) * (2.0 * np.pi / N_GRID)
    cos_t = np.cos(ang)
    sin_t = np.sin(ang)
    lanes = np.full((LANES,), -1)
    lanes[0:N_IMG] = np.arange(N_IMG)
    used = (lanes >= 0)[None, :]
    src = np.maximum(lanes, 0)
    pick = lambda t: np.where(used, t[:, src], 0.0)
    base = np.arange(ROWS)[:, None] * BLK
    ra = (base + row_order()[None, :]).reshape(-1)
    rb = (base + B_FIRST + np.arange(B_ROWS)[None, :]).reshape(-1)
    bf = jnp.bfloat16
    t3a = np.stack([pick(cos_t)[ra], pick(sin_t)[ra]]).reshape(2, ROWS, 128, LANES).astype(bf)
    t3b = np.stack([pick(cos_t)[rb], pick(sin_t)[rb]]).reshape(2, ROWS * B_ROWS, LANES).astype(bf)
    t2 = np.stack([cos_t.T, sin_t.T]).reshape(2, ROWS, COLS, N_GRID).astype(bf)
    return t2, t3a, t3b


def body(y_h, wr_h, wc_h, gr_h, gc_h, vc, s_h, d_h, t2_h, t3a_h, t3b_h, out_ref,
         y, wr, wc, gr, gc, s_v, din, drow, dcol, dd, rt0, rt1, wd, lb0, lb1, la0, la1, lh, accb, acc, gbb, gb,
         hbufb, recvb, hbuf, recv,
         hs, hr, hrt, t2, t3a, t3b, ib, img, ysend, yrecv,
         in_sem, tab_sem, send_sem, recv_sem, hsend_sem, hrecv_sem, ysend_sem, yrecv_sem):
    rts = (rt0, rt1)
    lefts_b = (lb0, lb1)
    lefts = (la0, la1)
    me = lax.axis_index('rows')
    cid = lax.axis_index('coil')
    nxt = lax.rem(me + 1, ROWS)
    prv = lax.rem(me + ROWS - 1, ROWS)
    other = 1 - cid

    ins = [pltpu.make_async_copy(a, b, in_sem.at[n]) for n, (a, b) in enumerate(
        ((gc_h, gc), (wc_h, wc), (gr_h, gr), (wr_h, wr), (y_h.at[0], y.at[0:8]), (y_h.at[1], y.at[8:16])))]
    for c in ins:
        c.start()
    tabs = [(t2_h.at[0], t2.at[:, 0]), (t2_h.at[1], t2.at[:, 1])]
    for g in range(3):
        src = slice(g * 128, g * 128 + 128)
        re = slice(g * 256, g * 256 + 128)
        im = slice(g * 256 + 128, g * 256 + 256)
        tabs += [
            (t3b_h.at[0, :, src], t3b.at[0, :, re]),
            (t3b_h.at[1, :, src], t3b.at[0, :, im]),
            (t3b_h.at[0, :, src], t3b.at[1, :, im]),
            (t3a_h.at[0, :, :, src], t3a.at[:, :, re]),
            (t3a_h.at[1, :, :, src], t3a.at[:, :, im]),
        ]
    tabs += [(s_h, s_v), (d_h, din)]
    tabs = [pltpu.make_async_copy(a, b, tab_sem.at[n]) for n, (a, b) in enumerate(tabs)]
    barrier = pltpu.get_barrier_semaphore()
    for d in range(1, ROWS):
        pl.semaphore_signal(barrier, inc=1, device_id={'rows': lax.rem(me + d, ROWS)}, device_id_type=MESH)
    pl.semaphore_signal(barrier, inc=1, device_id={'coil': other}, device_id_type=MESH)
    for c in ins:
        c.wait()
    for c in tabs:
        c.start()
    pl.semaphore_wait(barrier, 4)

    def build_wd(lo, groups):
        sl = pl.ds(lo, W)
        keep = (lax.broadcasted_iota(jnp.int32, (1, W), 1) + lo < vc[0]).astype(F32)
        start = gr[:, sl] - me * BLK - 2
        ids = lax.broadcasted_iota(jnp.int32, (8, W), 0)
        taps = [jnp.broadcast_to(wr[a:a + 1, sl] * keep, (8, W)) for a in range(4)]
        group = jnp.broadcast_to(lax.shift_right_arithmetic(start + 8, 3) - 1, (8, W))
        within = jnp.broadcast_to(start + 8 & 7, (8, W))
        head = jnp.zeros((8, W), F32)
        over = jnp.zeros((8, W), F32)
        for a in range(4):
            head = jnp.where(ids == within + a, taps[a], head)
            over = jnp.where(ids == within + (a - 8), taps[a], over)

        def rows_of(n):
            return jnp.where(group == n, head, jnp.where(group == n - 1, over, 0.0))

        for n in groups:
            if n < 16:
                w = rows_of(n + (B_ROWS // 8 if n * 8 >= B_FIRST else 0))
            elif n < 20:
                w = rows_of(n - 16 + B_FIRST // 8)
            else:
                w = jnp.where(ids == 0, rows_of(BLK // 8), pltpu.roll(rows_of(-1), 3, 0))
            wd[n * 8:n * 8 + 8, sl] = w
        if 15 in groups:
            for p, v in ((126, 16), (127, 32)):
                one, two = wd[p:p + 1, sl], wd[v:v + 1, sl]
                wd[p:p + 1, sl] = two
                wd[v:v + 1, sl] = one

    def build_rt(lo):
        sl = pl.ds(lo, W)
        k, off = lo // HALF, lo % HALF
        start = gc[:, sl] - 2
        start = jnp.where(start < 0, start + N_GRID, start)
        group = lax.shift_right_arithmetic(start, 4)
        after = jnp.where(group == N_GRID // 16 - 1, 0, group + 1)
        group = jnp.broadcast_to(group, (16, W)).astype(jnp.int16)
        after = jnp.broadcast_to(after, (16, W)).astype(jnp.int16)
        within = jnp.broadcast_to(start & 15, (16, W))
        ids = lax.broadcasted_iota(jnp.int16, (16, W), 0)
        head = jnp.zeros((16, W), BF)
        over = jnp.zeros((16, W), BF)
        for b in range(4):
            v = jnp.broadcast_to(wc[b:b + 1, sl], (16, W)).astype(BF)
            head = jnp.where(ids == (within + b).astype(jnp.int16), v, head)
            over = jnp.where(ids == (within + (b - 16)).astype(jnp.int16), v, over)
        zero = jnp.zeros((16, W), BF)
        for n in range(N_GRID // 16):
            w = jnp.where(group == jnp.int16(n), head, jnp.where(after == jnp.int16(n), over, zero))
            rts[k][n * 16:(n + 1) * 16, off:off + W] = w

    def build_left_b(k, off):
        sl = pl.ds(k * KC + off, W)
        w = wd[128:160, sl]
        for q in range(2):
            for c in range(NC):
                lo = q * 256 + c * 32
                lefts_b[k % 2][lo:lo + 32, off:off + W] = (y[q * 8 + c:q * 8 + c + 1, sl] * w).astype(BF)

    def build_halo(lo):
        sl = pl.ds(lo, W)
        for h in range(3):
            lh[h * 16:h * 16 + 16, sl] = (y[:, sl] * wd[160 + h:161 + h, sl]).astype(BF)

    def left_a_piece(c, lo):
        k, off = lo // HALF, lo % HALF
        sl = pl.ds(lo, W)
        rows = [jnp.broadcast_to(y[pl.ds(q * 8 + c, 1), sl], (16, W)) for q in range(2)]
        for n in range(8):
            w = wd[n * 16:n * 16 + 16, sl]
            for q, row in enumerate(rows):
                lefts[k][q * 128 + n * 16:q * 128 + n * 16 + 16, off:off + W] = (row * w).astype(BF)

    def build_left_a(c, k):
        for off in range(0, HALF, W):
            left_a_piece(c, k * HALF + off)

    def nt(a, b):
        return lax.dot_general(a, b, (((1,), (1,)), ((), ())), preferred_element_type=F32)

    def exchange(stage):
        if stage is None:
            src, dst, idx = hbufb, recvb, NC
        else:
            src, dst, idx = hbuf.at[stage], recv.at[stage], stage
        return [pltpu.make_async_remote_copy(
            src_ref=src.at[lax.rem(me + d, ROWS)], dst_ref=dst.at[me],
            send_sem=send_sem.at[idx, d - 1], recv_sem=recv_sem.at[idx, 3 - d],
            device_id={'rows': lax.rem(me + d, ROWS)}, device_id_type=MESH) for d in (1, 2, 3)]

    def received(stage):
        if stage is None:
            src, dst, idx = hbufb, recvb, NC
        else:
            src, dst, idx = hbuf.at[stage], recv.at[stage], stage
        return [pltpu.make_async_remote_copy(
            src_ref=src.at[0], dst_ref=dst.at[lax.rem(me + d, ROWS)],
            send_sem=send_sem.at[idx, d - 1], recv_sem=recv_sem.at[idx, d - 1],
            device_id={'rows': lax.rem(me + d, ROWS)}, device_id_type=MESH) for d in (1, 2, 3)]

    def transform(stage):
        g_ref, h_ref, r_ref = (gbb, hbufb, recvb) if stage is None else (gb, hbuf.at[stage], recv.at[stage])
        n = g_ref.shape[1] // 2
        for h in range(2):
            table = t2[2 * h:2 * h + 2].reshape(N_IMG, N_GRID)
            with_re = jnp.dot(table, g_ref[:, 0:n], preferred_element_type=F32) if n == 256 else None
            with_im = jnp.dot(table, g_ref[:, n:], preferred_element_type=F32) if n == 256 else None
            if n < 256:
                both = jnp.dot(table, g_ref[...], preferred_element_type=F32)
                with_re, with_im = both[:, 0:n], both[:, n:]
            for p in range(2):
                lo = p * 2 * COLS
                mid = lo + COLS
                end = mid + COLS
                h_ref[2 * h + p, 0:COLS] = (with_re[lo:mid] - with_im[mid:end]).astype(BF)
                h_ref[2 * h + p, COLS:] = (with_re[mid:end] + with_im[lo:mid]).astype(BF)

    def send(stage):
        h_ref, r_ref = (hbufb, recvb) if stage is None else (hbuf.at[stage], recv.at[stage])
        for c in exchange(stage):
            c.start()
        r_ref[me] = h_ref[me]

    parts = [(0, 0, 256), (0, 256, KC - 256)] + [(k, 0, KC) for k in range(1, NK)]

    def build_first(k, off, size):
        for o in range(off, off + size, W):
            build_rt(k * KC + o)
            build_wd(k * KC + o, (16, 17, 18, 19, 20))
            build_left_b(k, o)
            build_halo(k * KC + o)

    def first_stage(n):
        k, off, size = parts[n]
        lo = (k % 2) * KC + off
        for q in range(2):
            cs = slice(q * 256, q * 256 + 256)
            part = nt(rts[k // 2][:, lo:lo + size], lefts_b[k % 2][cs, off:off + size])
            if n == 0:
                accb[:, cs] = part
            elif n + 1 < len(parts):
                accb[:, cs] += part
            else:
                gbb[:, cs] = (accb[:, cs] + part).astype(BF)

    def halo(k):
        lo = (k % 2) * KC
        for h in range(2):
            rows = slice(h * 320, h * 320 + 320)
            part = nt(rts[k // 2][rows, lo:lo + KC], lh[:, k * KC:(k + 1) * KC])
            hrt[rows, 0:48] = part if k == 0 else hrt[rows, 0:48] + part

    build_first(*parts[0])
    for n in range(len(parts) - 1):
        first_stage(n)
        if n > 0:
            halo(parts[n][0])
        build_first(*parts[n + 1])
    halo(NK - 1)
    for lo in range(0, HALF, W):
        build_wd(lo, range(16))
        left_a_piece(0, lo)
    hs[...] = hrt[...].T[0:48]
    to_next = pltpu.make_async_remote_copy(
        src_ref=hs.at[0:16], dst_ref=hr.at[0:16], send_sem=hsend_sem.at[0], recv_sem=hrecv_sem.at[0],
        device_id={'rows': nxt}, device_id_type=MESH)
    to_prev = pltpu.make_async_remote_copy(
        src_ref=hs.at[16:48], dst_ref=hr.at[16:48], send_sem=hsend_sem.at[1], recv_sem=hrecv_sem.at[1],
        device_id={'rows': prv}, device_id_type=MESH)
    to_next.start()
    to_prev.start()
    for c in tabs:
        c.wait()

    first_stage(len(parts) - 1)
    for g in range(3):
        t3b[1, :, g * 256:g * 256 + 128] = -t3b[0, :, g * 256 + 128:g * 256 + 256]
    drow[...] = din[...].reshape(1, N_IMG)
    dcol[...] = jnp.broadcast_to(din[...].reshape(1, N_IMG), (8, N_IMG)).T
    mine = jnp.where(cid == 0, drow[:, 0:BLK], drow[:, BLK:])
    dd[...] = dcol[pl.ds(pl.multiple_of(me * COLS, COLS), COLS), 0:1] * mine
    img[...] = jnp.zeros_like(img)
    transform(None)
    send(None)

    def spread_head(c, first=False):
        for h in range(2):
            rows = slice(h * 320, h * 320 + 320)
            acc[rows, :] = nt(rts[0][rows, :], lefts[0][...])
        for lo in range(HALF, SLOTS, W):
            if first:
                build_wd(lo, range(16))
            left_a_piece(c, lo)

    lane = lax.broadcasted_iota(jnp.int32, (1, 128), 1)
    edge = (lane == 0) | (lane == 16) | (lane == 32)

    def spread_tail(c):
        for h in range(2):
            rows = slice(h * 320, h * 320 + 320)
            part = nt(rts[1][rows, :], lefts[1][...])
            for q in range(2):
                cs = slice(q * 128, q * 128 + 128)
                rolled = pltpu.roll(hrt[rows, :], 128 - (q * 8 + c), 1)
                gb[rows, cs] = (acc[rows, cs] + part[:, cs] + jnp.where(edge, rolled, 0.0)).astype(BF)

    def image_first():
        for c in range(NC):
            blocks = [recvb[p, b * COLS:(b + 1) * COLS, c * 32:c * 32 + 32] for b in range(2) for p in range(ROWS)]
            lhs = jnp.concatenate(blocks, axis=1)
            ib[c] = jnp.dot(lhs, t3b[...].reshape(256, 2 * LANES), preferred_element_type=F32)

    def image_wait(c):
        for x in received(c):
            x.wait_recv()

    def image_coil(c):
        lhs = jnp.concatenate([recv[c, p] for p in range(ROWS)], axis=1)
        for g in range(3):
            lanes = slice(g * 256, g * 256 + 256)
            tot = jnp.dot(lhs, t3a[:, :, lanes].reshape(4 * 128, 256), preferred_element_type=F32)
            re = ib[c, :, g * 256:g * 256 + 128] + (tot[0:COLS, 0:128] - tot[COLS:, 128:])
            im = ib[c, :, g * 256 + 128:g * 256 + 256] + (tot[0:COLS, 128:] + tot[COLS:, 0:128])
            n = min(128, N_IMG - g * 128)
            at = slice(g * 128, g * 128 + n)
            sr = s_v[0, c, :, at]
            si = s_v[1, c, :, at]
            img[0, :, at] += sr * re[:, 0:n] + si * im[:, 0:n]
            img[1, :, at] += sr * im[:, 0:n] - si * re[:, 0:n]

    spread_head(0, True)

    @pl.loop(0, LAG - 1)
    def _(c):
        @pl.when(c == 0)
        def _():
            to_next.wait()
            to_prev.wait()
            hrt[...] = jnp.concatenate([hr[...], jnp.zeros((80, N_GRID), F32)], axis=0).T

        spread_tail(c)
        build_left_a(c + 1, 0)
        transform(c)
        spread_head(c + 1)
        send(c)

    for c in received(None):
        c.wait_recv()
    c = LAG - 1
    spread_tail(c)
    build_left_a(c + 1, 0)
    image_first()
    transform(c)
    spread_head(c + 1)
    send(c)

    @pl.loop(LAG, NC - 2)
    def _(c):
        image_wait(c - LAG)
        spread_tail(c)
        build_left_a(c + 1, 0)
        image_coil(c - LAG)
        transform(c)
        spread_head(c + 1)
        send(c)

    c = NC - 2
    image_wait(c - LAG)
    spread_tail(c)
    build_left_a(c + 1, 0)
    image_coil(c - LAG)
    transform(c)
    send(c)
    spread_head(c + 1)
    spread_tail(c + 1)
    transform(c + 1)
    send(c + 1)

    @pl.loop(NC - 1 - LAG, NC)
    def _(c):
        image_wait(c)
        image_coil(c)

    halves = [jnp.where(cid == 0, img[e, :, BLK:N_IMG], img[e, :, 0:BLK]) for e in range(2)]
    ysend[...] = jnp.concatenate([x[r:r + COLS // 2] for x in halves for r in (0, COLS // 2)], axis=1)
    swap = pltpu.make_async_remote_copy(
        src_ref=ysend, dst_ref=yrecv, send_sem=ysend_sem, recv_sem=yrecv_sem,
        device_id={'coil': other}, device_id_type=MESH)
    swap.start()
    swap.wait()
    for e in range(2):
        lo = e * 2 * BLK
        theirs = jnp.concatenate([yrecv[:, lo:lo + BLK], yrecv[:, lo + BLK:lo + 2 * BLK]], axis=0)
        total = (jnp.where(cid == 0, img[e, :, 0:BLK], img[e, :, BLK:N_IMG]) + theirs) * dd[...]
        out_ref[e] = total.T
    for stage in [None] + list(range(NC)):
        for c in received(stage):
            c.wait_send()


def solution(mesh):
    t2c, t3ac, t3bc = constants()

    def local_part(kspace, weight_row, weight_col, grid_row, grid_col, valid_count, coil_maps, deapod):
        any_spec = pl.BlockSpec(memory_space=pl.ANY)
        dma = pltpu.SemaphoreType.DMA
        return pl.pallas_call(
            body,
            out_shape=pltpu.VMEM((2, BLK, COLS), F32),
            in_specs=[any_spec] * 5 + [pl.BlockSpec(memory_space=pltpu.SMEM)] + [any_spec] * 5,
            out_specs=pl.BlockSpec(memory_space=pltpu.VMEM),
            scratch_shapes=[
                pltpu.VMEM((2 * NC, SLOTS), F32),
                pltpu.VMEM((4, SLOTS), F32),
                pltpu.VMEM((4, SLOTS), F32),
                pltpu.VMEM((1, SLOTS), jnp.int32),
                pltpu.VMEM((1, SLOTS), jnp.int32),
                pltpu.VMEM((2, NC, COLS, N_IMG), F32),
                pltpu.VMEM((N_IMG,), F32),
                pltpu.VMEM((1, N_IMG), F32),
                pltpu.VMEM((N_IMG, 8), F32),
                pltpu.VMEM((COLS, BLK), F32),
                pltpu.VMEM((N_GRID, HALF), BF),
                pltpu.VMEM((N_GRID, HALF), BF),
                pltpu.VMEM((168, SLOTS), F32),
                pltpu.VMEM((512, KC), BF),
                pltpu.VMEM((512, KC), BF),
                pltpu.VMEM((256, HALF), BF),
                pltpu.VMEM((256, HALF), BF),
                pltpu.VMEM((48, SLOTS), BF),
                pltpu.VMEM((N_GRID, 512), F32),
                pltpu.VMEM((N_GRID, 256), F32),
                pltpu.VMEM((N_GRID, 512), BF),
                pltpu.VMEM((N_GRID, 256), BF),
                pltpu.VMEM((ROWS, 2 * COLS, 256), BF),
                pltpu.VMEM((ROWS, 2 * COLS, 256), BF),
                pltpu.VMEM((NC, ROWS, 2 * COLS, 128), BF),
                pltpu.VMEM((NC, ROWS, 2 * COLS, 128), BF),
                pltpu.VMEM((48, N_GRID), F32),
                pltpu.VMEM((48, N_GRID), F32),
                pltpu.VMEM((N_GRID, 128), F32),
                pltpu.VMEM((ROWS, 2, COLS, N_GRID), BF),
                pltpu.VMEM((ROWS, 128, 2 * LANES), BF),
                pltpu.VMEM((2, ROWS * B_ROWS, 2 * LANES), BF),
                pltpu.VMEM((NC, COLS, 2 * LANES), F32),
                pltpu.VMEM((2, COLS, N_IMG), F32),
                pltpu.VMEM((COLS // 2, 4 * BLK), F32),
                pltpu.VMEM((COLS // 2, 4 * BLK), F32),
                dma((6,)), dma((19,)), dma((9, 3)), dma((9, 3)), dma((2,)), dma((2,)), dma, dma,
            ],
            compiler_params=pltpu.CompilerParams(collective_id=0, has_side_effects=True, vmem_limit_bytes=60 * 1024 * 1024),
            name='nufft_adjoint',
        )(kspace, weight_row, weight_col, grid_row.reshape(1, SLOTS), grid_col.reshape(1, SLOTS), valid_count,
          jnp.swapaxes(coil_maps, 2, 3), deapod, jnp.asarray(t2c), jnp.asarray(t3ac), jnp.asarray(t3bc))

    spec_samples = P(None, 'coil', ('slab', 'rows'))
    spec_weights = P(None, ('slab', 'rows'))
    spec_index = P(('slab', 'rows'))
    return jax.shard_map(local_part, mesh=mesh, in_specs=(spec_samples, spec_weights, spec_weights, spec_index, spec_index, spec_index, P(None, 'coil', 'slab', 'rows'), P()), out_specs=P(None, ('slab', 'coil'), 'rows'), check_vma=False)
```

```python
import functools
import numpy as np
import jax
import jax.numpy as jnp
from jax import lax
from jax.experimental import pallas as pl
from jax.experimental.pallas import tpu as pltpu
from jax.sharding import PartitionSpec as P

MESH = pl.DeviceIdType.MESH
BF = jnp.bfloat16
F32 = jnp.float32

N_IMG = 320
N_GRID = 640
ROWS = 4
BLK = 160
COLS = 80
NC = 8
SLOTS = 5120
KC = 1280
NK = SLOTS // KC
LANES = 384
HALF = SLOTS // 2
LAG = 3
LATE = 2
W = 256
B_FIRST = 64
B_ROWS = 32


def row_order():
    pos = np.arange(128)
    rows = pos + np.where(pos >= B_FIRST, B_ROWS, 0)
    rows[126], rows[16] = 16, 158
    rows[127], rows[32] = 32, 159
    return rows


def constants():
    k = np.arange(N_GRID)
    j = np.arange(N_IMG)
    ang = np.mod((k[:, None] - N_IMG) * (j[None, :] - N_IMG // 2), N_GRID) * (2.0 * np.pi / N_GRID)
    cos_t = np.cos(ang)
    sin_t = np.sin(ang)
    lanes = np.full((LANES,), -1)
    lanes[0:N_IMG] = np.arange(N_IMG)
    used = (lanes >= 0)[None, :]
    src = np.maximum(lanes, 0)
    pick = lambda t: np.where(used, t[:, src], 0.0)
    base = np.arange(ROWS)[:, None] * BLK
    ra = (base + row_order()[None, :]).reshape(-1)
    rb = (base + B_FIRST + np.arange(B_ROWS)[None, :]).reshape(-1)
    bf = jnp.bfloat16
    t3a = np.stack([pick(cos_t)[ra], pick(sin_t)[ra]]).reshape(2, ROWS, 128, LANES).astype(bf)
    t3b = np.stack([pick(cos_t)[rb], pick(sin_t)[rb]]).reshape(2, ROWS * B_ROWS, LANES).astype(bf)
    t2 = np.stack([cos_t.T, sin_t.T]).reshape(2, ROWS, COLS, N_GRID).astype(bf)
    return t2, t3a, t3b


def body(y_h, wr_h, wc_h, gr_h, gc_h, vc, s_h, d_h, t2_h, t3a_h, t3b_h, out_ref,
         y, wr, wc, gr, gc, s_v, din, drow, dcol, dd, rt0, rt1, wd, lb0, lb1, la0, la1, lh, accb, acc, gbb, gb,
         hbufb, recvb, hbuf, recv,
         hs, hr, hrt, t2, t3a, t3b, ib, img, own, ysend, yrecv,
         in_sem, tab_sem, send_sem, recv_sem, hsend_sem, hrecv_sem, ysend_sem, yrecv_sem):
    rts = (rt0, rt1)
    lefts_b = (lb0, lb1)
    lefts = (la0, la1)
    me = lax.axis_index('rows')
    cid = lax.axis_index('coil')
    nxt = lax.rem(me + 1, ROWS)
    prv = lax.rem(me + ROWS - 1, ROWS)
    other = 1 - cid

    ins = [pltpu.make_async_copy(a, b, in_sem.at[n]) for n, (a, b) in enumerate(
        ((gc_h, gc), (wc_h, wc), (gr_h, gr), (wr_h, wr), (y_h.at[0], y.at[0:8]), (y_h.at[1], y.at[8:16])))]
    for c in ins:
        c.start()
    tabs = [(t2_h.at[0], t2.at[:, 0]), (t2_h.at[1], t2.at[:, 1])]
    for g in range(3):
        src = slice(g * 128, g * 128 + 128)
        re = slice(g * 256, g * 256 + 128)
        im = slice(g * 256 + 128, g * 256 + 256)
        tabs += [
            (t3b_h.at[0, :, src], t3b.at[0, :, re]),
            (t3b_h.at[1, :, src], t3b.at[0, :, im]),
            (t3b_h.at[0, :, src], t3b.at[1, :, im]),
            (t3a_h.at[0, :, :, src], t3a.at[:, :, re]),
            (t3a_h.at[1, :, :, src], t3a.at[:, :, im]),
        ]
    tabs += [(s_h, s_v), (d_h, din)]
    tabs = [pltpu.make_async_copy(a, b, tab_sem.at[n]) for n, (a, b) in enumerate(tabs)]
    barrier = pltpu.get_barrier_semaphore()
    for d in range(1, ROWS):
        pl.semaphore_signal(barrier, inc=1, device_id={'rows': lax.rem(me + d, ROWS)}, device_id_type=MESH)
    pl.semaphore_signal(barrier, inc=1, device_id={'coil': other}, device_id_type=MESH)
    for c in ins:
        c.wait()
    for c in tabs:
        c.start()
    pl.semaphore_wait(barrier, 4)

    def build_wd(lo, groups):
        sl = pl.ds(lo, W)
        keep = (lax.broadcasted_iota(jnp.int32, (1, W), 1) + lo < vc[0]).astype(F32)
        start = gr[:, sl] - me * BLK - 2
        ids = lax.broadcasted_iota(jnp.int32, (8, W), 0)
        taps = [jnp.broadcast_to(wr[a:a + 1, sl] * keep, (8, W)) for a in range(4)]
        group = jnp.broadcast_to(lax.shift_right_arithmetic(start + 8, 3) - 1, (8, W))
        within = jnp.broadcast_to(start + 8 & 7, (8, W))
        head = jnp.zeros((8, W), F32)
        over = jnp.zeros((8, W), F32)
        for a in range(4):
            head = jnp.where(ids == within + a, taps[a], head)
            over = jnp.where(ids == within + (a - 8), taps[a], over)

        def rows_of(n):
            return jnp.where(group == n, head, jnp.where(group == n - 1, over, 0.0))

        for n in groups:
            if n < 16:
                w = rows_of(n + (B_ROWS // 8 if n * 8 >= B_FIRST else 0))
            elif n < 20:
                w = rows_of(n - 16 + B_FIRST // 8)
            else:
                w = jnp.where(ids == 0, rows_of(BLK // 8), pltpu.roll(rows_of(-1), 3, 0))
            wd[n * 8:n * 8 + 8, sl] = w
        if 15 in groups:
            for p, v in ((126, 16), (127, 32)):
                one, two = wd[p:p + 1, sl], wd[v:v + 1, sl]
                wd[p:p + 1, sl] = two
                wd[v:v + 1, sl] = one

    def build_rt(lo):
        sl = pl.ds(lo, W)
        k, off = lo // HALF, lo % HALF
        start = gc[:, sl] - 2
        start = jnp.where(start < 0, start + N_GRID, start)
        group = lax.shift_right_arithmetic(start, 4)
        after = jnp.where(group == N_GRID // 16 - 1, 0, group + 1)
        group = jnp.broadcast_to(group, (16, W)).astype(jnp.int16)
        after = jnp.broadcast_to(after, (16, W)).astype(jnp.int16)
        within = jnp.broadcast_to(start & 15, (16, W))
        ids = lax.broadcasted_iota(jnp.int16, (16, W), 0)
        head = jnp.zeros((16, W), BF)
        over = jnp.zeros((16, W), BF)
        for b in range(4):
            v = jnp.broadcast_to(wc[b:b + 1, sl], (16, W)).astype(BF)
            head = jnp.where(ids == (within + b).astype(jnp.int16), v, head)
            over = jnp.where(ids == (within + (b - 16)).astype(jnp.int16), v, over)
        zero = jnp.zeros((16, W), BF)
        for n in range(N_GRID // 16):
            w = jnp.where(group == jnp.int16(n), head, jnp.where(after == jnp.int16(n), over, zero))
            rts[k][n * 16:(n + 1) * 16, off:off + W] = w

    def build_left_b(k, off):
        sl = pl.ds(k * KC + off, W)
        w = wd[128:160, sl]
        for q in range(2):
            for c in range(NC):
                lo = q * 256 + c * 32
                lefts_b[k % 2][lo:lo + 32, off:off + W] = (y[q * 8 + c:q * 8 + c + 1, sl] * w).astype(BF)

    def build_halo(lo):
        sl = pl.ds(lo, W)
        for h in range(3):
            lh[h * 16:h * 16 + 16, sl] = (y[:, sl] * wd[160 + h:161 + h, sl]).astype(BF)

    def left_a_piece(c, lo):
        k, off = lo // HALF, lo % HALF
        sl = pl.ds(lo, W)
        rows = [jnp.broadcast_to(y[pl.ds(q * 8 + c, 1), sl], (16, W)) for q in range(2)]
        for n in range(8):
            w = wd[n * 16:n * 16 + 16, sl]
            for q, row in enumerate(rows):
                lefts[k][q * 128 + n * 16:q * 128 + n * 16 + 16, off:off + W] = (row * w).astype(BF)

    def build_left_a(c, k):
        for off in range(0, HALF, W):
            left_a_piece(c, k * HALF + off)

    def nt(a, b):
        return lax.dot_general(a, b, (((1,), (1,)), ((), ())), preferred_element_type=F32)

    def exchange(stage):
        if stage is None:
            src, dst, idx = hbufb, recvb, NC
        else:
            src, dst, idx = hbuf.at[stage], recv.at[stage], stage
        return [pltpu.make_async_remote_copy(
            src_ref=src.at[lax.rem(me + d, ROWS)], dst_ref=dst.at[me],
            send_sem=send_sem.at[idx, d - 1], recv_sem=recv_sem.at[idx, 3 - d],
            device_id={'rows': lax.rem(me + d, ROWS)}, device_id_type=MESH) for d in (1, 2, 3)]

    def received(stage):
        if stage is None:
            src, dst, idx = hbufb, recvb, NC
        else:
            src, dst, idx = hbuf.at[stage], recv.at[stage], stage
        return [pltpu.make_async_remote_copy(
            src_ref=src.at[0], dst_ref=dst.at[lax.rem(me + d, ROWS)],
            send_sem=send_sem.at[idx, d - 1], recv_sem=recv_sem.at[idx, d - 1],
            device_id={'rows': lax.rem(me + d, ROWS)}, device_id_type=MESH) for d in (1, 2, 3)]

    def transform(stage):
        g_ref, h_ref, r_ref = (gbb, hbufb, recvb) if stage is None else (gb, hbuf.at[stage], recv.at[stage])
        n = g_ref.shape[1] // 2
        for h in range(2):
            table = t2[2 * h:2 * h + 2].reshape(N_IMG, N_GRID)
            with_re = jnp.dot(table, g_ref[:, 0:n], preferred_element_type=F32) if n == 256 else None
            with_im = jnp.dot(table, g_ref[:, n:], preferred_element_type=F32) if n == 256 else None
            if n < 256:
                both = jnp.dot(table, g_ref[...], preferred_element_type=F32)
                with_re, with_im = both[:, 0:n], both[:, n:]
            for p in range(2):
                lo = p * 2 * COLS
                mid = lo + COLS
                end = mid + COLS
                h_ref[2 * h + p, 0:COLS] = (with_re[lo:mid] - with_im[mid:end]).astype(BF)
                h_ref[2 * h + p, COLS:] = (with_re[mid:end] + with_im[lo:mid]).astype(BF)

    def send(stage):
        h_ref, r_ref = (hbufb, recvb) if stage is None else (hbuf.at[stage], recv.at[stage])
        for c in exchange(stage):
            c.start()
        r_ref[me] = h_ref[me]

    parts = [(0, 0, 256), (0, 256, KC - 256)] + [(k, 0, KC) for k in range(1, NK)]

    def build_first(k, off, size):
        for o in range(off, off + size, W):
            build_rt(k * KC + o)
            build_wd(k * KC + o, (16, 17, 18, 19, 20))
            build_left_b(k, o)
            build_halo(k * KC + o)

    def first_stage(n):
        k, off, size = parts[n]
        lo = (k % 2) * KC + off
        for q in range(2):
            cs = slice(q * 256, q * 256 + 256)
            part = nt(rts[k // 2][:, lo:lo + size], lefts_b[k % 2][cs, off:off + size])
            if n == 0:
                accb[:, cs] = part
            elif n + 1 < len(parts):
                accb[:, cs] += part
            else:
                gbb[:, cs] = (accb[:, cs] + part).astype(BF)

    def halo(k):
        lo = (k % 2) * KC
        for h in range(2):
            rows = slice(h * 320, h * 320 + 320)
            part = nt(rts[k // 2][rows, lo:lo + KC], lh[:, k * KC:(k + 1) * KC])
            hrt[rows, 0:48] = part if k == 0 else hrt[rows, 0:48] + part

    build_first(*parts[0])
    for n in range(len(parts) - 1):
        if n + LATE < len(parts):
            first_stage(n)
        if n > 0:
            halo(parts[n][0])
        build_first(*parts[n + 1])
    halo(NK - 1)
    for lo in range(0, HALF, W):
        build_wd(lo, range(16))
        left_a_piece(0, lo)
    hs[...] = hrt[...].T[0:48]
    to_next = pltpu.make_async_remote_copy(
        src_ref=hs.at[0:16], dst_ref=hr.at[0:16], send_sem=hsend_sem.at[0], recv_sem=hrecv_sem.at[0],
        device_id={'rows': nxt}, device_id_type=MESH)
    to_prev = pltpu.make_async_remote_copy(
        src_ref=hs.at[16:48], dst_ref=hr.at[16:48], send_sem=hsend_sem.at[1], recv_sem=hrecv_sem.at[1],
        device_id={'rows': prv}, device_id_type=MESH)
    to_next.start()
    to_prev.start()
    for c in tabs:
        c.wait()

    for n in range(len(parts) - LATE, len(parts)):
        first_stage(n)
    for g in range(3):
        t3b[1, :, g * 256:g * 256 + 128] = -t3b[0, :, g * 256 + 128:g * 256 + 256]
    drow[...] = din[...].reshape(1, N_IMG)
    dcol[...] = jnp.broadcast_to(din[...].reshape(1, N_IMG), (8, N_IMG)).T
    mine = jnp.where(cid == 0, drow[:, 0:BLK], drow[:, BLK:])
    dd[...] = dcol[pl.ds(pl.multiple_of(me * COLS, COLS), COLS), 0:1] * mine
    img[...] = jnp.zeros_like(img)
    transform(None)
    send(None)

    def spread_head(c, first=False):
        for h in range(2):
            rows = slice(h * 320, h * 320 + 320)
            acc[rows, :] = nt(rts[0][rows, :], lefts[0][...])
        for lo in range(HALF, SLOTS, W):
            if first:
                build_wd(lo, range(16))
            left_a_piece(c, lo)

    lane = lax.broadcasted_iota(jnp.int32, (1, 128), 1)
    edge = (lane == 0) | (lane == 16) | (lane == 32)

    def spread_tail(c):
        for h in range(2):
            rows = slice(h * 320, h * 320 + 320)
            part = nt(rts[1][rows, :], lefts[1][...])
            for q in range(2):
                cs = slice(q * 128, q * 128 + 128)
                rolled = pltpu.roll(hrt[rows, :], 128 - (q * 8 + c), 1)
                gb[rows, cs] = (acc[rows, cs] + part[:, cs] + jnp.where(edge, rolled, 0.0)).astype(BF)

    def image_first():
        for c in range(NC):
            blocks = [recvb[p, b * COLS:(b + 1) * COLS, c * 32:c * 32 + 32] for b in range(2) for p in range(ROWS)]
            lhs = jnp.concatenate(blocks, axis=1)
            ib[c] = jnp.dot(lhs, t3b[...].reshape(256, 2 * LANES), preferred_element_type=F32)

    def image_wait(c):
        for x in received(c):
            x.wait_recv()

    def image_coil(c):
        lhs = jnp.concatenate([recv[c, p] for p in range(ROWS)], axis=1)
        for g in range(3):
            lanes = slice(g * 256, g * 256 + 256)
            tot = jnp.dot(lhs, t3a[:, :, lanes].reshape(4 * 128, 256), preferred_element_type=F32)
            re = ib[c, :, g * 256:g * 256 + 128] + (tot[0:COLS, 0:128] - tot[COLS:, 128:])
            im = ib[c, :, g * 256 + 128:g * 256 + 256] + (tot[0:COLS, 128:] + tot[COLS:, 0:128])
            n = min(128, N_IMG - g * 128)
            at = slice(g * 128, g * 128 + n)
            sr = s_v[0, c, :, at]
            si = s_v[1, c, :, at]
            img[0, :, at] += sr * re[:, 0:n] + si * im[:, 0:n]
            img[1, :, at] += sr * im[:, 0:n] - si * re[:, 0:n]

    spread_head(0, True)

    @pl.loop(0, LAG)
    def _(c):
        @pl.when(c == 0)
        def _():
            to_next.wait()
            to_prev.wait()
            hrt[...] = jnp.concatenate([hr[...], jnp.zeros((80, N_GRID), F32)], axis=0).T

        spread_tail(c)
        build_left_a(c + 1, 0)
        transform(c)
        spread_head(c + 1)
        send(c)

    for c in received(None):
        c.wait_recv()
    c = LAG
    image_wait(c - LAG)
    spread_tail(c)
    build_left_a(c + 1, 0)
    image_first()
    image_coil(c - LAG)
    transform(c)
    spread_head(c + 1)
    send(c)

    @pl.loop(LAG + 1, NC - 2)
    def _(c):
        image_wait(c - LAG)
        spread_tail(c)
        build_left_a(c + 1, 0)
        image_coil(c - LAG)
        transform(c)
        spread_head(c + 1)
        send(c)

    c = NC - 2
    image_wait(c - LAG)
    spread_tail(c)
    build_left_a(c + 1, 0)
    image_coil(c - LAG)
    transform(c)
    send(c)
    spread_head(c + 1)
    spread_tail(c + 1)
    transform(c + 1)
    send(c + 1)

    @pl.loop(NC - 1 - LAG, NC)
    def _(c):
        image_wait(c)
        image_coil(c)

    halves = [jnp.where(cid == 0, img[e, :, BLK:N_IMG], img[e, :, 0:BLK]) for e in range(2)]
    ysend[...] = jnp.concatenate([x[r:r + COLS // 2] for x in halves for r in (0, COLS // 2)], axis=1)
    swap = pltpu.make_async_remote_copy(
        src_ref=ysend, dst_ref=yrecv, send_sem=ysend_sem, recv_sem=yrecv_sem,
        device_id={'coil': other}, device_id_type=MESH)
    swap.start()
    for e in range(2):
        own[e] = jnp.where(cid == 0, img[e, :, 0:BLK], img[e, :, BLK:N_IMG])
    for stage in [None] + list(range(NC)):
        for c in received(stage):
            c.wait_send()
    swap.wait()
    for e in range(2):
        lo = e * 2 * BLK
        theirs = jnp.concatenate([yrecv[:, lo:lo + BLK], yrecv[:, lo + BLK:lo + 2 * BLK]], axis=0)
        out_ref[e] = ((own[e] + theirs) * dd[...]).T


def solution(mesh):
    t2c, t3ac, t3bc = constants()

    def local_part(kspace, weight_row, weight_col, grid_row, grid_col, valid_count, coil_maps, deapod):
        any_spec = pl.BlockSpec(memory_space=pl.ANY)
        dma = pltpu.SemaphoreType.DMA
        return pl.pallas_call(
            body,
            out_shape=pltpu.VMEM((2, BLK, COLS), F32),
            in_specs=[any_spec] * 5 + [pl.BlockSpec(memory_space=pltpu.SMEM)] + [any_spec] * 5,
            out_specs=pl.BlockSpec(memory_space=pltpu.VMEM),
            scratch_shapes=[
                pltpu.VMEM((2 * NC, SLOTS), F32),
                pltpu.VMEM((4, SLOTS), F32),
                pltpu.VMEM((4, SLOTS), F32),
                pltpu.VMEM((1, SLOTS), jnp.int32),
                pltpu.VMEM((1, SLOTS), jnp.int32),
                pltpu.VMEM((2, NC, COLS, N_IMG), F32),
                pltpu.VMEM((N_IMG,), F32),
                pltpu.VMEM((1, N_IMG), F32),
                pltpu.VMEM((N_IMG, 8), F32),
                pltpu.VMEM((COLS, BLK), F32),
                pltpu.VMEM((N_GRID, HALF), BF),
                pltpu.VMEM((N_GRID, HALF), BF),
                pltpu.VMEM((168, SLOTS), F32),
                pltpu.VMEM((512, KC), BF),
                pltpu.VMEM((512, KC), BF),
                pltpu.VMEM((256, HALF), BF),
                pltpu.VMEM((256, HALF), BF),
                pltpu.VMEM((48, SLOTS), BF),
                pltpu.VMEM((N_GRID, 512), F32),
                pltpu.VMEM((N_GRID, 256), F32),
                pltpu.VMEM((N_GRID, 512), BF),
                pltpu.VMEM((N_GRID, 256), BF),
                pltpu.VMEM((ROWS, 2 * COLS, 256), BF),
                pltpu.VMEM((ROWS, 2 * COLS, 256), BF),
                pltpu.VMEM((NC, ROWS, 2 * COLS, 128), BF),
                pltpu.VMEM((NC, ROWS, 2 * COLS, 128), BF),
                pltpu.VMEM((48, N_GRID), F32),
                pltpu.VMEM((48, N_GRID), F32),
                pltpu.VMEM((N_GRID, 128), F32),
                pltpu.VMEM((ROWS, 2, COLS, N_GRID), BF),
                pltpu.VMEM((ROWS, 128, 2 * LANES), BF),
                pltpu.VMEM((2, ROWS * B_ROWS, 2 * LANES), BF),
                pltpu.VMEM((NC, COLS, 2 * LANES), F32),
                pltpu.VMEM((2, COLS, N_IMG), F32),
                pltpu.VMEM((2, COLS, BLK), F32),
                pltpu.VMEM((COLS // 2, 4 * BLK), F32),
                pltpu.VMEM((COLS // 2, 4 * BLK), F32),
                dma((6,)), dma((19,)), dma((9, 3)), dma((9, 3)), dma((2,)), dma((2,)), dma, dma,
            ],
            compiler_params=pltpu.CompilerParams(collective_id=0, has_side_effects=True, vmem_limit_bytes=60 * 1024 * 1024),
            name='nufft_adjoint',
        )(kspace, weight_row, weight_col, grid_row.reshape(1, SLOTS), grid_col.reshape(1, SLOTS), valid_count,
          jnp.swapaxes(coil_maps, 2, 3), deapod, jnp.asarray(t2c), jnp.asarray(t3ac), jnp.asarray(t3bc))

    spec_samples = P(None, 'coil', ('slab', 'rows'))
    spec_weights = P(None, ('slab', 'rows'))
    spec_index = P(('slab', 'rows'))
    return jax.shard_map(local_part, mesh=mesh, in_specs=(spec_samples, spec_weights, spec_weights, spec_index, spec_index, spec_index, P(None, 'coil', 'slab', 'rows'), P()), out_specs=P(None, ('slab', 'coil'), 'rows'), check_vma=False)
```

```python
import functools
import numpy as np
import jax
import jax.numpy as jnp
from jax import lax
from jax.experimental import pallas as pl
from jax.experimental.pallas import tpu as pltpu
from jax.sharding import PartitionSpec as P

MESH = pl.DeviceIdType.MESH
BF = jnp.bfloat16
F32 = jnp.float32

N_IMG = 320
N_GRID = 640
ROWS = 4
BLK = 160
COLS = 80
NC = 8
SLOTS = 5120
KC = 1280
NK = SLOTS // KC
LANES = 384
HALF = SLOTS // 2
LATE = 1
W = 256
B_FIRST = 64
B_ROWS = 32


def row_order():
    pos = np.arange(128)
    rows = pos + np.where(pos >= B_FIRST, B_ROWS, 0)
    rows[126], rows[16] = 16, 158
    rows[127], rows[32] = 32, 159
    return rows


def constants():
    k = np.arange(N_GRID)
    j = np.arange(N_IMG)
    ang = np.mod((k[:, None] - N_IMG) * (j[None, :] - N_IMG // 2), N_GRID) * (2.0 * np.pi / N_GRID)
    cos_t = np.cos(ang)
    sin_t = np.sin(ang)
    lanes = np.full((LANES,), -1)
    lanes[0:N_IMG] = np.arange(N_IMG)
    used = (lanes >= 0)[None, :]
    src = np.maximum(lanes, 0)
    pick = lambda t: np.where(used, t[:, src], 0.0)
    base = np.arange(ROWS)[:, None] * BLK
    ra = (base + row_order()[None, :]).reshape(-1)
    rb = (base + B_FIRST + np.arange(B_ROWS)[None, :]).reshape(-1)
    bf = jnp.bfloat16
    t3a = np.stack([pick(cos_t)[ra], pick(sin_t)[ra]]).reshape(2, ROWS, 128, LANES).astype(bf)
    t3b = np.stack([pick(cos_t)[rb], pick(sin_t)[rb]]).reshape(2, ROWS * B_ROWS, LANES).astype(bf)
    t2 = np.stack([cos_t.T, sin_t.T]).reshape(2, ROWS, COLS, N_GRID).astype(bf)
    return t2, t3a, t3b


def body(y_h, wr_h, wc_h, gr_h, gc_h, vc, s_h, d_h, t2_h, t3a_h, t3b_h, out_ref,
         y, wr, wc, gr, gc, s_v, din, drow, dcol, dd, rt0, rt1, wd, lb0, lb1, la0, la1, lh, accb, acc, gbb, gb,
         hbufb, recvb, hbuf, recv,
         hs, hr, hrt, t2, t3a, t3b, ib, img, own, ysend, yrecv,
         in_sem, tab_sem, send_sem, recv_sem, hsend_sem, hrecv_sem, ysend_sem, yrecv_sem):
    rts = (rt0, rt1)
    lefts_b = (lb0, lb1)
    lefts = (la0, la1)
    me = lax.axis_index('rows')
    cid = lax.axis_index('coil')
    nxt = lax.rem(me + 1, ROWS)
    prv = lax.rem(me + ROWS - 1, ROWS)
    other = 1 - cid

    ins = [pltpu.make_async_copy(a, b, in_sem.at[n]) for n, (a, b) in enumerate(
        ((gc_h, gc), (wc_h, wc), (gr_h, gr), (wr_h, wr), (y_h.at[0], y.at[0:8]), (y_h.at[1], y.at[8:16])))]
    for c in ins:
        c.start()
    tabs = [(t2_h.at[0], t2.at[:, 0]), (t2_h.at[1], t2.at[:, 1])]
    for g in range(3):
        src = slice(g * 128, g * 128 + 128)
        re = slice(g * 256, g * 256 + 128)
        im = slice(g * 256 + 128, g * 256 + 256)
        tabs += [
            (t3b_h.at[0, :, src], t3b.at[0, :, re]),
            (t3b_h.at[1, :, src], t3b.at[0, :, im]),
            (t3b_h.at[0, :, src], t3b.at[1, :, im]),
            (t3a_h.at[0, :, :, src], t3a.at[:, :, re]),
            (t3a_h.at[1, :, :, src], t3a.at[:, :, im]),
        ]
    tabs += [(s_h, s_v), (d_h, din)]
    tabs = [pltpu.make_async_copy(a, b, tab_sem.at[n]) for n, (a, b) in enumerate(tabs)]
    barrier = pltpu.get_barrier_semaphore()
    for d in range(1, ROWS):
        pl.semaphore_signal(barrier, inc=1, device_id={'rows': lax.rem(me + d, ROWS)}, device_id_type=MESH)
    pl.semaphore_signal(barrier, inc=1, device_id={'coil': other}, device_id_type=MESH)
    for c in ins:
        c.wait()
    for c in tabs:
        c.start()
    pl.semaphore_wait(barrier, 4)

    def build_wd(lo, groups):
        sl = pl.ds(lo, W)
        keep = (lax.broadcasted_iota(jnp.int32, (1, W), 1) + lo < vc[0]).astype(F32)
        start = gr[:, sl] - me * BLK - 2
        ids = lax.broadcasted_iota(jnp.int32, (8, W), 0)
        taps = [jnp.broadcast_to(wr[a:a + 1, sl] * keep, (8, W)) for a in range(4)]
        group = jnp.broadcast_to(lax.shift_right_arithmetic(start + 8, 3) - 1, (8, W))
        within = jnp.broadcast_to(start + 8 & 7, (8, W))
        head = jnp.zeros((8, W), F32)
        over = jnp.zeros((8, W), F32)
        for a in range(4):
            head = jnp.where(ids == within + a, taps[a], head)
            over = jnp.where(ids == within + (a - 8), taps[a], over)

        def rows_of(n):
            return jnp.where(group == n, head, jnp.where(group == n - 1, over, 0.0))

        for n in groups:
            if n < 16:
                w = rows_of(n + (B_ROWS // 8 if n * 8 >= B_FIRST else 0))
            elif n < 20:
                w = rows_of(n - 16 + B_FIRST // 8)
            else:
                w = jnp.where(ids == 0, rows_of(BLK // 8), pltpu.roll(rows_of(-1), 3, 0))
            wd[n * 8:n * 8 + 8, sl] = w
        if 15 in groups:
            for p, v in ((126, 16), (127, 32)):
                one, two = wd[p:p + 1, sl], wd[v:v + 1, sl]
                wd[p:p + 1, sl] = two
                wd[v:v + 1, sl] = one

    def build_rt(lo):
        sl = pl.ds(lo, W)
        k, off = lo // HALF, lo % HALF
        start = gc[:, sl] - 2
        start = jnp.where(start < 0, start + N_GRID, start)
        group = lax.shift_right_arithmetic(start, 4)
        after = jnp.where(group == N_GRID // 16 - 1, 0, group + 1)
        group = jnp.broadcast_to(group, (16, W)).astype(jnp.int16)
        after = jnp.broadcast_to(after, (16, W)).astype(jnp.int16)
        within = jnp.broadcast_to(start & 15, (16, W))
        ids = lax.broadcasted_iota(jnp.int16, (16, W), 0)
        head = jnp.zeros((16, W), BF)
        over = jnp.zeros((16, W), BF)
        for b in range(4):
            v = jnp.broadcast_to(wc[b:b + 1, sl], (16, W)).astype(BF)
            head = jnp.where(ids == (within + b).astype(jnp.int16), v, head)
            over = jnp.where(ids == (within + (b - 16)).astype(jnp.int16), v, over)
        zero = jnp.zeros((16, W), BF)
        for n in range(N_GRID // 16):
            w = jnp.where(group == jnp.int16(n), head, jnp.where(after == jnp.int16(n), over, zero))
            rts[k][n * 16:(n + 1) * 16, off:off + W] = w

    def build_left_b(k, off):
        sl = pl.ds(k * KC + off, W)
        w = wd[128:160, sl]
        for q in range(2):
            for c in range(NC):
                lo = q * 256 + c * 32
                lefts_b[k % 2][lo:lo + 32, off:off + W] = (y[q * 8 + c:q * 8 + c + 1, sl] * w).astype(BF)

    def build_halo(lo):
        sl = pl.ds(lo, W)
        for h in range(3):
            lh[h * 16:h * 16 + 16, sl] = (y[:, sl] * wd[160 + h:161 + h, sl]).astype(BF)

    def left_a_piece(c, lo):
        k, off = lo // HALF, lo % HALF
        sl = pl.ds(lo, W)
        rows = [jnp.broadcast_to(y[pl.ds(q * 8 + c, 1), sl], (16, W)) for q in range(2)]
        for n in range(8):
            w = wd[n * 16:n * 16 + 16, sl]
            for q, row in enumerate(rows):
                lefts[k][q * 128 + n * 16:q * 128 + n * 16 + 16, off:off + W] = (row * w).astype(BF)

    def build_left_a(c, k):
        for off in range(0, HALF, W):
            left_a_piece(c, k * HALF + off)

    def nt(a, b):
        return lax.dot_general(a, b, (((1,), (1,)), ((), ())), preferred_element_type=F32)

    def exchange(stage):
        if stage is None:
            src, dst, idx = hbufb, recvb, NC
        else:
            src, dst, idx = hbuf.at[stage], recv.at[stage], stage
        return [pltpu.make_async_remote_copy(
            src_ref=src.at[lax.rem(me + d, ROWS)], dst_ref=dst.at[me],
            send_sem=send_sem.at[idx, d - 1], recv_sem=recv_sem.at[idx, 3 - d],
            device_id={'rows': lax.rem(me + d, ROWS)}, device_id_type=MESH) for d in (1, 2, 3)]

    def received(stage):
        if stage is None:
            src, dst, idx = hbufb, recvb, NC
        else:
            src, dst, idx = hbuf.at[stage], recv.at[stage], stage
        return [pltpu.make_async_remote_copy(
            src_ref=src.at[0], dst_ref=dst.at[lax.rem(me + d, ROWS)],
            send_sem=send_sem.at[idx, d - 1], recv_sem=recv_sem.at[idx, d - 1],
            device_id={'rows': lax.rem(me + d, ROWS)}, device_id_type=MESH) for d in (1, 2, 3)]

    def transform(stage):
        g_ref, h_ref, r_ref = (gbb, hbufb, recvb) if stage is None else (gb, hbuf.at[stage], recv.at[stage])
        n = g_ref.shape[1] // 2
        for h in range(2):
            table = t2[2 * h:2 * h + 2].reshape(N_IMG, N_GRID)
            with_re = jnp.dot(table, g_ref[:, 0:n], preferred_element_type=F32) if n == 256 else None
            with_im = jnp.dot(table, g_ref[:, n:], preferred_element_type=F32) if n == 256 else None
            if n < 256:
                both = jnp.dot(table, g_ref[...], preferred_element_type=F32)
                with_re, with_im = both[:, 0:n], both[:, n:]
            for p in range(2):
                lo = p * 2 * COLS
                mid = lo + COLS
                end = mid + COLS
                h_ref[2 * h + p, 0:COLS] = (with_re[lo:mid] - with_im[mid:end]).astype(BF)
                h_ref[2 * h + p, COLS:] = (with_re[mid:end] + with_im[lo:mid]).astype(BF)

    def send(stage):
        h_ref, r_ref = (hbufb, recvb) if stage is None else (hbuf.at[stage], recv.at[stage])
        for c in exchange(stage):
            c.start()
        r_ref[me] = h_ref[me]

    parts = [(0, 0, 256), (0, 256, KC - 256)] + [(k, 0, KC) for k in range(1, NK)]

    def build_first(k, off, size):
        for o in range(off, off + size, W):
            build_rt(k * KC + o)
            build_wd(k * KC + o, (16, 17, 18, 19, 20))
            build_left_b(k, o)
            build_halo(k * KC + o)

    def first_stage(n):
        k, off, size = parts[n]
        lo = (k % 2) * KC + off
        for q in range(2):
            cs = slice(q * 256, q * 256 + 256)
            part = nt(rts[k // 2][:, lo:lo + size], lefts_b[k % 2][cs, off:off + size])
            if n == 0:
                accb[:, cs] = part
            elif n + 1 < len(parts):
                accb[:, cs] += part
            else:
                gbb[:, cs] = (accb[:, cs] + part).astype(BF)

    def halo(k):
        lo = (k % 2) * KC
        for h in range(2):
            rows = slice(h * 320, h * 320 + 320)
            part = nt(rts[k // 2][rows, lo:lo + KC], lh[:, k * KC:(k + 1) * KC])
            hrt[rows, 0:48] = part if k == 0 else hrt[rows, 0:48] + part

    build_first(*parts[0])
    for n in range(len(parts) - 1):
        if n + LATE < len(parts):
            first_stage(n)
        if n > 0:
            halo(parts[n][0])
        build_first(*parts[n + 1])
    halo(NK - 1)
    for lo in range(0, HALF, W):
        build_wd(lo, range(16))
        left_a_piece(0, lo)
    hs[...] = hrt[...].T[0:48]
    to_next = pltpu.make_async_remote_copy(
        src_ref=hs.at[0:16], dst_ref=hr.at[0:16], send_sem=hsend_sem.at[0], recv_sem=hrecv_sem.at[0],
        device_id={'rows': nxt}, device_id_type=MESH)
    to_prev = pltpu.make_async_remote_copy(
        src_ref=hs.at[16:48], dst_ref=hr.at[16:48], send_sem=hsend_sem.at[1], recv_sem=hrecv_sem.at[1],
        device_id={'rows': prv}, device_id_type=MESH)
    to_next.start()
    to_prev.start()
    for c in tabs:
        c.wait()

    for n in range(len(parts) - LATE, len(parts)):
        first_stage(n)
    for g in range(3):
        t3b[1, :, g * 256:g * 256 + 128] = -t3b[0, :, g * 256 + 128:g * 256 + 256]
    drow[...] = din[...].reshape(1, N_IMG)
    dcol[...] = jnp.broadcast_to(din[...].reshape(1, N_IMG), (8, N_IMG)).T
    mine = jnp.where(cid == 0, drow[:, 0:BLK], drow[:, BLK:])
    dd[...] = dcol[pl.ds(pl.multiple_of(me * COLS, COLS), COLS), 0:1] * mine
    img[...] = jnp.zeros_like(img)
    transform(None)
    send(None)

    def spread_head(c, first=False):
        for h in range(2):
            rows = slice(h * 320, h * 320 + 320)
            acc[rows, :] = nt(rts[0][rows, :], lefts[0][...])
        for lo in range(HALF, SLOTS, W):
            if first:
                build_wd(lo, range(16))
            left_a_piece(c, lo)

    lane = lax.broadcasted_iota(jnp.int32, (1, 128), 1)
    edge = (lane == 0) | (lane == 16) | (lane == 32)

    def spread_tail(c):
        for h in range(2):
            rows = slice(h * 320, h * 320 + 320)
            part = nt(rts[1][rows, :], lefts[1][...])
            for q in range(2):
                cs = slice(q * 128, q * 128 + 128)
                rolled = pltpu.roll(hrt[rows, :], 128 - (q * 8 + c), 1)
                gb[rows, cs] = (acc[rows, cs] + part[:, cs] + jnp.where(edge, rolled, 0.0)).astype(BF)

    def image_first():
        for c in range(NC):
            blocks = [recvb[p, b * COLS:(b + 1) * COLS, c * 32:c * 32 + 32] for b in range(2) for p in range(ROWS)]
            lhs = jnp.concatenate(blocks, axis=1)
            ib[c] = jnp.dot(lhs, t3b[...].reshape(256, 2 * LANES), preferred_element_type=F32)

    def image_coil(c):
        lhs = jnp.concatenate([recv[c, p] for p in range(ROWS)], axis=1)
        for g in range(3):
            lanes = slice(g * 256, g * 256 + 256)
            tot = jnp.dot(lhs, t3a[:, :, lanes].reshape(4 * 128, 256), preferred_element_type=F32)
            re = ib[c, :, g * 256:g * 256 + 128] + (tot[0:COLS, 0:128] - tot[COLS:, 128:])
            im = ib[c, :, g * 256 + 128:g * 256 + 256] + (tot[0:COLS, 128:] + tot[COLS:, 0:128])
            n = min(128, N_IMG - g * 128)
            at = slice(g * 128, g * 128 + n)
            sr = s_v[0, c, :, at]
            si = s_v[1, c, :, at]
            img[0, :, at] += sr * re[:, 0:n] + si * im[:, 0:n]
            img[1, :, at] += sr * im[:, 0:n] - si * re[:, 0:n]

    spread_head(0, True)

    @pl.loop(0, NC - 2)
    def _(c):
        @pl.when(c == 0)
        def _():
            to_next.wait()
            to_prev.wait()
            hrt[...] = jnp.concatenate([hr[...], jnp.zeros((80, N_GRID), F32)], axis=0).T

        spread_tail(c)
        build_left_a(c + 1, 0)
        transform(c)
        spread_head(c + 1)
        send(c)

    c = NC - 2
    spread_tail(c)
    build_left_a(c + 1, 0)
    transform(c)
    send(c)
    spread_head(c + 1)
    spread_tail(c + 1)
    transform(c + 1)
    send(c + 1)

    for c in received(None):
        c.wait_recv()
    image_first()

    @pl.loop(0, NC)
    def _(c):
        for x in received(c):
            x.wait_recv()
        image_coil(c)

    halves = [jnp.where(cid == 0, img[e, :, BLK:N_IMG], img[e, :, 0:BLK]) for e in range(2)]
    ysend[...] = jnp.concatenate([x[r:r + COLS // 2] for x in halves for r in (0, COLS // 2)], axis=1)
    swap = pltpu.make_async_remote_copy(
        src_ref=ysend, dst_ref=yrecv, send_sem=ysend_sem, recv_sem=yrecv_sem,
        device_id={'coil': other}, device_id_type=MESH)
    swap.start()
    for e in range(2):
        own[e] = jnp.where(cid == 0, img[e, :, 0:BLK], img[e, :, BLK:N_IMG])
    for stage in [None] + list(range(NC)):
        for c in received(stage):
            c.wait_send()
    swap.wait()
    for e in range(2):
        lo = e * 2 * BLK
        theirs = jnp.concatenate([yrecv[:, lo:lo + BLK], yrecv[:, lo + BLK:lo + 2 * BLK]], axis=0)
        out_ref[e] = ((own[e] + theirs) * dd[...]).T


def solution(mesh):
    t2c, t3ac, t3bc = constants()

    def local_part(kspace, weight_row, weight_col, grid_row, grid_col, valid_count, coil_maps, deapod):
        any_spec = pl.BlockSpec(memory_space=pl.ANY)
        dma = pltpu.SemaphoreType.DMA
        return pl.pallas_call(
            body,
            out_shape=pltpu.VMEM((2, BLK, COLS), F32),
            in_specs=[any_spec] * 5 + [pl.BlockSpec(memory_space=pltpu.SMEM)] + [any_spec] * 5,
            out_specs=pl.BlockSpec(memory_space=pltpu.VMEM),
            scratch_shapes=[
                pltpu.VMEM((2 * NC, SLOTS), F32),
                pltpu.VMEM((4, SLOTS), F32),
                pltpu.VMEM((4, SLOTS), F32),
                pltpu.VMEM((1, SLOTS), jnp.int32),
                pltpu.VMEM((1, SLOTS), jnp.int32),
                pltpu.VMEM((2, NC, COLS, N_IMG), F32),
                pltpu.VMEM((N_IMG,), F32),
                pltpu.VMEM((1, N_IMG), F32),
                pltpu.VMEM((N_IMG, 8), F32),
                pltpu.VMEM((COLS, BLK), F32),
                pltpu.VMEM((N_GRID, HALF), BF),
                pltpu.VMEM((N_GRID, HALF), BF),
                pltpu.VMEM((168, SLOTS), F32),
                pltpu.VMEM((512, KC), BF),
                pltpu.VMEM((512, KC), BF),
                pltpu.VMEM((256, HALF), BF),
                pltpu.VMEM((256, HALF), BF),
                pltpu.VMEM((48, SLOTS), BF),
                pltpu.VMEM((N_GRID, 512), F32),
                pltpu.VMEM((N_GRID, 256), F32),
                pltpu.VMEM((N_GRID, 512), BF),
                pltpu.VMEM((N_GRID, 256), BF),
                pltpu.VMEM((ROWS, 2 * COLS, 256), BF),
                pltpu.VMEM((ROWS, 2 * COLS, 256), BF),
                pltpu.VMEM((NC, ROWS, 2 * COLS, 128), BF),
                pltpu.VMEM((NC, ROWS, 2 * COLS, 128), BF),
                pltpu.VMEM((48, N_GRID), F32),
                pltpu.VMEM((48, N_GRID), F32),
                pltpu.VMEM((N_GRID, 128), F32),
                pltpu.VMEM((ROWS, 2, COLS, N_GRID), BF),
                pltpu.VMEM((ROWS, 128, 2 * LANES), BF),
                pltpu.VMEM((2, ROWS * B_ROWS, 2 * LANES), BF),
                pltpu.VMEM((NC, COLS, 2 * LANES), F32),
                pltpu.VMEM((2, COLS, N_IMG), F32),
                pltpu.VMEM((2, COLS, BLK), F32),
                pltpu.VMEM((COLS // 2, 4 * BLK), F32),
                pltpu.VMEM((COLS // 2, 4 * BLK), F32),
                dma((6,)), dma((19,)), dma((9, 3)), dma((9, 3)), dma((2,)), dma((2,)), dma, dma,
            ],
            compiler_params=pltpu.CompilerParams(collective_id=0, has_side_effects=True, vmem_limit_bytes=60 * 1024 * 1024),
            name='nufft_adjoint',
        )(kspace, weight_row, weight_col, grid_row.reshape(1, SLOTS), grid_col.reshape(1, SLOTS), valid_count,
          jnp.swapaxes(coil_maps, 2, 3), deapod, jnp.asarray(t2c), jnp.asarray(t3ac), jnp.asarray(t3bc))

    spec_samples = P(None, 'coil', ('slab', 'rows'))
    spec_weights = P(None, ('slab', 'rows'))
    spec_index = P(('slab', 'rows'))
    return jax.shard_map(local_part, mesh=mesh, in_specs=(spec_samples, spec_weights, spec_weights, spec_index, spec_index, spec_index, P(None, 'coil', 'slab', 'rows'), P()), out_specs=P(None, ('slab', 'coil'), 'rows'), check_vma=False)
```

```python
import functools
import numpy as np
import jax
import jax.numpy as jnp
from jax import lax
from jax.experimental import pallas as pl
from jax.experimental.pallas import tpu as pltpu
from jax.sharding import PartitionSpec as P

MESH = pl.DeviceIdType.MESH
BF = jnp.bfloat16
F32 = jnp.float32

N_IMG = 320
N_GRID = 640
ROWS = 4
BLK = 160
COLS = 80
NC = 8
SLOTS = 5120
KC = 1280
NK = SLOTS // KC
LANES = 384
HALF = SLOTS // 2
LATE = 1
W = 256
B_FIRST = 64
B_ROWS = 32


def row_order():
    pos = np.arange(128)
    rows = pos + np.where(pos >= B_FIRST, B_ROWS, 0)
    rows[126], rows[16] = 16, 158
    rows[127], rows[32] = 32, 159
    return rows


def constants():
    k = np.arange(N_GRID)
    j = np.arange(N_IMG)
    ang = np.mod((k[:, None] - N_IMG) * (j[None, :] - N_IMG // 2), N_GRID) * (2.0 * np.pi / N_GRID)
    cos_t = np.cos(ang)
    sin_t = np.sin(ang)
    lanes = np.full((LANES,), -1)
    lanes[0:N_IMG] = np.arange(N_IMG)
    used = (lanes >= 0)[None, :]
    src = np.maximum(lanes, 0)
    pick = lambda t: np.where(used, t[:, src], 0.0)
    base = np.arange(ROWS)[:, None] * BLK
    ra = (base + row_order()[None, :]).reshape(-1)
    rb = (base + B_FIRST + np.arange(B_ROWS)[None, :]).reshape(-1)
    bf = jnp.bfloat16
    t3a = np.stack([pick(cos_t)[ra], pick(sin_t)[ra]]).reshape(2, ROWS, 128, LANES).astype(bf)
    t3b = np.stack([pick(cos_t)[rb], pick(sin_t)[rb]]).reshape(2, ROWS * B_ROWS, LANES).astype(bf)
    t2 = np.stack([cos_t.T, sin_t.T]).reshape(2, ROWS, COLS, N_GRID).astype(bf)
    return t2, t3a, t3b


def body(y_h, wr_h, wc_h, gr_h, gc_h, vc_h, s_h, d_h, t2_h, t3a_h, t3b_h, out_ref,
         y, wr, wc, gr, gc, vc, s_v, din, drow, dcol, dd, rt0, rt1, wd, lb0, lb1, la0, la1, lh, accb, acc, gbb, gb,
         hbufb, recvb, hbuf, recv,
         hs, hr, hrt, t2, t3a, t3b, ib, img, own, ysend, yrecv,
         in_sem, tab_sem, send_sem, recv_sem, hsend_sem, hrecv_sem, ysend_sem, yrecv_sem):
    rts = (rt0, rt1)
    lefts_b = (lb0, lb1)
    lefts = (la0, la1)
    me = lax.axis_index('rows')
    cid = lax.axis_index('coil')
    nxt = lax.rem(me + 1, ROWS)
    prv = lax.rem(me + ROWS - 1, ROWS)
    other = 1 - cid

    ins = [pltpu.make_async_copy(a, b, in_sem.at[n]) for n, (a, b) in enumerate(
        ((gc_h, gc), (wc_h, wc), (vc_h, vc), (gr_h, gr), (wr_h, wr), (y_h.at[0], y.at[0:8]), (y_h.at[1], y.at[8:16])))]
    for c in ins:
        c.start()
    tabs = [(t2_h.at[0], t2.at[:, 0]), (t2_h.at[1], t2.at[:, 1])]
    for g in range(3):
        src = slice(g * 128, g * 128 + 128)
        re = slice(g * 256, g * 256 + 128)
        im = slice(g * 256 + 128, g * 256 + 256)
        tabs += [
            (t3b_h.at[0, :, src], t3b.at[0, :, re]),
            (t3b_h.at[1, :, src], t3b.at[0, :, im]),
            (t3b_h.at[0, :, src], t3b.at[1, :, im]),
            (t3a_h.at[0, :, :, src], t3a.at[:, :, re]),
            (t3a_h.at[1, :, :, src], t3a.at[:, :, im]),
        ]
    tabs += [(s_h, s_v), (d_h, din)]
    tabs = [pltpu.make_async_copy(a, b, tab_sem.at[n]) for n, (a, b) in enumerate(tabs)]
    barrier = pltpu.get_barrier_semaphore()
    for d in range(1, ROWS):
        pl.semaphore_signal(barrier, inc=1, device_id={'rows': lax.rem(me + d, ROWS)}, device_id_type=MESH)
    pl.semaphore_signal(barrier, inc=1, device_id={'coil': other}, device_id_type=MESH)
    for c in ins:
        c.wait()
    for c in tabs:
        c.start()
    pl.semaphore_wait(barrier, 4)

    def build_wd(lo, groups):
        sl = pl.ds(lo, W)
        keep = (lax.broadcasted_iota(jnp.int32, (1, W), 1) + lo < vc[0, 0]).astype(F32)
        start = gr[:, sl] - me * BLK - 2
        ids = lax.broadcasted_iota(jnp.int32, (8, W), 0)
        taps = [jnp.broadcast_to(wr[a:a + 1, sl] * keep, (8, W)) for a in range(4)]
        group = jnp.broadcast_to(lax.shift_right_arithmetic(start + 8, 3) - 1, (8, W))
        within = jnp.broadcast_to(start + 8 & 7, (8, W))
        head = jnp.zeros((8, W), F32)
        over = jnp.zeros((8, W), F32)
        for a in range(4):
            head = jnp.where(ids == within + a, taps[a], head)
            over = jnp.where(ids == within + (a - 8), taps[a], over)

        def rows_of(n):
            return jnp.where(group == n, head, jnp.where(group == n - 1, over, 0.0))

        for n in groups:
            if n < 16:
                w = rows_of(n + (B_ROWS // 8 if n * 8 >= B_FIRST else 0))
            elif n < 20:
                w = rows_of(n - 16 + B_FIRST // 8)
            else:
                w = jnp.where(ids == 0, rows_of(BLK // 8), pltpu.roll(rows_of(-1), 3, 0))
            wd[n * 8:n * 8 + 8, sl] = w
        if 15 in groups:
            for p, v in ((126, 16), (127, 32)):
                one, two = wd[p:p + 1, sl], wd[v:v + 1, sl]
                wd[p:p + 1, sl] = two
                wd[v:v + 1, sl] = one

    def build_rt(lo):
        sl = pl.ds(lo, W)
        k, off = lo // HALF, lo % HALF
        start = gc[:, sl] - 2
        start = jnp.where(start < 0, start + N_GRID, start)
        group = lax.shift_right_arithmetic(start, 4)
        after = jnp.where(group == N_GRID // 16 - 1, 0, group + 1)
        group = jnp.broadcast_to(group, (16, W)).astype(jnp.int16)
        after = jnp.broadcast_to(after, (16, W)).astype(jnp.int16)
        within = jnp.broadcast_to(start & 15, (16, W))
        ids = lax.broadcasted_iota(jnp.int16, (16, W), 0)
        head = jnp.zeros((16, W), BF)
        over = jnp.zeros((16, W), BF)
        for b in range(4):
            v = jnp.broadcast_to(wc[b:b + 1, sl], (16, W)).astype(BF)
            head = jnp.where(ids == (within + b).astype(jnp.int16), v, head)
            over = jnp.where(ids == (within + (b - 16)).astype(jnp.int16), v, over)
        zero = jnp.zeros((16, W), BF)
        for n in range(N_GRID // 16):
            w = jnp.where(group == jnp.int16(n), head, jnp.where(after == jnp.int16(n), over, zero))
            rts[k][n * 16:(n + 1) * 16, off:off + W] = w

    def build_left_b(k, off):
        sl = pl.ds(k * KC + off, W)
        w = wd[128:160, sl]
        for q in range(2):
            for c in range(NC):
                lo = q * 256 + c * 32
                lefts_b[k % 2][lo:lo + 32, off:off + W] = (y[q * 8 + c:q * 8 + c + 1, sl] * w).astype(BF)

    def build_halo(lo):
        sl = pl.ds(lo, W)
        for h in range(3):
            lh[h * 16:h * 16 + 16, sl] = (y[:, sl] * wd[160 + h:161 + h, sl]).astype(BF)

    def left_a_piece(c, lo):
        k, off = lo // HALF, lo % HALF
        sl = pl.ds(lo, W)
        rows = [jnp.broadcast_to(y[pl.ds(q * 8 + c, 1), sl], (16, W)) for q in range(2)]
        for n in range(8):
            w = wd[n * 16:n * 16 + 16, sl]
            for q, row in enumerate(rows):
                lefts[k][q * 128 + n * 16:q * 128 + n * 16 + 16, off:off + W] = (row * w).astype(BF)

    def build_left_a(c, k):
        for off in range(0, HALF, W):
            left_a_piece(c, k * HALF + off)

    def nt(a, b):
        return lax.dot_general(a, b, (((1,), (1,)), ((), ())), preferred_element_type=F32)

    def exchange(stage):
        if stage is None:
            src, dst, idx = hbufb, recvb, NC
        else:
            src, dst, idx = hbuf.at[stage], recv.at[stage], stage
        return [pltpu.make_async_remote_copy(
            src_ref=src.at[lax.rem(me + d, ROWS)], dst_ref=dst.at[me],
            send_sem=send_sem.at[idx, d - 1], recv_sem=recv_sem.at[idx, 3 - d],
            device_id={'rows': lax.rem(me + d, ROWS)}, device_id_type=MESH) for d in (1, 2, 3)]

    def received(stage):
        if stage is None:
            src, dst, idx = hbufb, recvb, NC
        else:
            src, dst, idx = hbuf.at[stage], recv.at[stage], stage
        return [pltpu.make_async_remote_copy(
            src_ref=src.at[0], dst_ref=dst.at[lax.rem(me + d, ROWS)],
            send_sem=send_sem.at[idx, d - 1], recv_sem=recv_sem.at[idx, d - 1],
            device_id={'rows': lax.rem(me + d, ROWS)}, device_id_type=MESH) for d in (1, 2, 3)]

    def transform(stage):
        g_ref, h_ref, r_ref = (gbb, hbufb, recvb) if stage is None else (gb, hbuf.at[stage], recv.at[stage])
        n = g_ref.shape[1] // 2
        for h in range(2):
            table = t2[2 * h:2 * h + 2].reshape(N_IMG, N_GRID)
            with_re = jnp.dot(table, g_ref[:, 0:n], preferred_element_type=F32) if n == 256 else None
            with_im = jnp.dot(table, g_ref[:, n:], preferred_element_type=F32) if n == 256 else None
            if n < 256:
                both = jnp.dot(table, g_ref[...], preferred_element_type=F32)
                with_re, with_im = both[:, 0:n], both[:, n:]
            for p in range(2):
                lo = p * 2 * COLS
                mid = lo + COLS
                end = mid + COLS
                h_ref[2 * h + p, 0:COLS] = (with_re[lo:mid] - with_im[mid:end]).astype(BF)
                h_ref[2 * h + p, COLS:] = (with_re[mid:end] + with_im[lo:mid]).astype(BF)

    def send(stage):
        h_ref, r_ref = (hbufb, recvb) if stage is None else (hbuf.at[stage], recv.at[stage])
        for c in exchange(stage):
            c.start()
        r_ref[me] = h_ref[me]

    parts = [(0, 0, 256), (0, 256, KC - 256)] + [(k, 0, KC) for k in range(1, NK)]

    def build_first(k, off, size):
        for o in range(off, off + size, W):
            build_rt(k * KC + o)
            build_wd(k * KC + o, (16, 17, 18, 19, 20))
            build_left_b(k, o)
            build_halo(k * KC + o)

    def first_stage(n):
        k, off, size = parts[n]
        lo = (k % 2) * KC + off
        for q in range(2):
            cs = slice(q * 256, q * 256 + 256)
            part = nt(rts[k // 2][:, lo:lo + size], lefts_b[k % 2][cs, off:off + size])
            if n == 0:
                accb[:, cs] = part
            elif n + 1 < len(parts):
                accb[:, cs] += part
            else:
                gbb[:, cs] = (accb[:, cs] + part).astype(BF)

    def halo(k):
        lo = (k % 2) * KC
        for h in range(2):
            rows = slice(h * 320, h * 320 + 320)
            part = nt(rts[k // 2][rows, lo:lo + KC], lh[:, k * KC:(k + 1) * KC])
            hrt[rows, 0:48] = part if k == 0 else hrt[rows, 0:48] + part

    build_first(*parts[0])
    for n in range(len(parts) - 1):
        if n + LATE < len(parts):
            first_stage(n)
        if n > 0:
            halo(parts[n][0])
        build_first(*parts[n + 1])
    halo(NK - 1)
    for lo in range(0, HALF, W):
        build_wd(lo, range(16))
        left_a_piece(0, lo)
    hs[...] = hrt[...].T[0:48]
    to_next = pltpu.make_async_remote_copy(
        src_ref=hs.at[0:16], dst_ref=hr.at[0:16], send_sem=hsend_sem.at[0], recv_sem=hrecv_sem.at[0],
        device_id={'rows': nxt}, device_id_type=MESH)
    to_prev = pltpu.make_async_remote_copy(
        src_ref=hs.at[16:48], dst_ref=hr.at[16:48], send_sem=hsend_sem.at[1], recv_sem=hrecv_sem.at[1],
        device_id={'rows': prv}, device_id_type=MESH)
    to_next.start()
    to_prev.start()
    for c in tabs[:2]:
        c.wait()

    for n in range(len(parts) - LATE, len(parts)):
        first_stage(n)
    transform(None)
    send(None)

    def spread_head(c, first=False):
        for h in range(2):
            rows = slice(h * 320, h * 320 + 320)
            acc[rows, :] = nt(rts[0][rows, :], lefts[0][...])
        for lo in range(HALF, SLOTS, W):
            if first:
                build_wd(lo, range(16))
            left_a_piece(c, lo)

    lane = lax.broadcasted_iota(jnp.int32, (1, 128), 1)
    edge = (lane == 0) | (lane == 16) | (lane == 32)

    def spread_tail(c):
        for h in range(2):
            rows = slice(h * 320, h * 320 + 320)
            part = nt(rts[1][rows, :], lefts[1][...])
            for q in range(2):
                cs = slice(q * 128, q * 128 + 128)
                rolled = pltpu.roll(hrt[rows, :], 128 - (q * 8 + c), 1)
                gb[rows, cs] = (acc[rows, cs] + part[:, cs] + jnp.where(edge, rolled, 0.0)).astype(BF)

    def image_first():
        for c in range(NC):
            blocks = [recvb[p, b * COLS:(b + 1) * COLS, c * 32:c * 32 + 32] for b in range(2) for p in range(ROWS)]
            lhs = jnp.concatenate(blocks, axis=1)
            ib[c] = jnp.dot(lhs, t3b[...].reshape(256, 2 * LANES), preferred_element_type=F32)

    def image_coil(c):
        lhs = jnp.concatenate([recv[c, p] for p in range(ROWS)], axis=1)
        for g in range(3):
            lanes = slice(g * 256, g * 256 + 256)
            tot = jnp.dot(lhs, t3a[:, :, lanes].reshape(4 * 128, 256), preferred_element_type=F32)
            re = ib[c, :, g * 256:g * 256 + 128] + (tot[0:COLS, 0:128] - tot[COLS:, 128:])
            im = ib[c, :, g * 256 + 128:g * 256 + 256] + (tot[0:COLS, 128:] + tot[COLS:, 0:128])
            n = min(128, N_IMG - g * 128)
            at = slice(g * 128, g * 128 + n)
            sr = s_v[0, c, :, at]
            si = s_v[1, c, :, at]
            img[0, :, at] += sr * re[:, 0:n] + si * im[:, 0:n]
            img[1, :, at] += sr * im[:, 0:n] - si * re[:, 0:n]

    spread_head(0, True)

    @pl.loop(0, NC - 2)
    def _(c):
        @pl.when(c == 0)
        def _():
            to_next.wait()
            to_prev.wait()
            hrt[...] = jnp.concatenate([hr[...], jnp.zeros((80, N_GRID), F32)], axis=0).T

        spread_tail(c)
        build_left_a(c + 1, 0)
        transform(c)
        spread_head(c + 1)
        send(c)

    c = NC - 2
    spread_tail(c)
    build_left_a(c + 1, 0)
    transform(c)
    send(c)
    spread_head(c + 1)
    spread_tail(c + 1)
    transform(c + 1)
    send(c + 1)

    for c in tabs[2:]:
        c.wait()
    for g in range(3):
        t3b[1, :, g * 256:g * 256 + 128] = -t3b[0, :, g * 256 + 128:g * 256 + 256]
    drow[...] = din[...].reshape(1, N_IMG)
    dcol[...] = jnp.broadcast_to(din[...].reshape(1, N_IMG), (8, N_IMG)).T
    mine = jnp.where(cid == 0, drow[:, 0:BLK], drow[:, BLK:])
    dd[...] = dcol[pl.ds(pl.multiple_of(me * COLS, COLS), COLS), 0:1] * mine
    img[...] = jnp.zeros_like(img)
    for c in received(None):
        c.wait_recv()
    image_first()

    @pl.loop(0, NC)
    def _(c):
        for x in received(c):
            x.wait_recv()
        image_coil(c)

    halves = [jnp.where(cid == 0, img[e, :, BLK:N_IMG], img[e, :, 0:BLK]) for e in range(2)]
    ysend[...] = jnp.concatenate([x[r:r + COLS // 2] for x in halves for r in (0, COLS // 2)], axis=1)
    swap = pltpu.make_async_remote_copy(
        src_ref=ysend, dst_ref=yrecv, send_sem=ysend_sem, recv_sem=yrecv_sem,
        device_id={'coil': other}, device_id_type=MESH)
    swap.start()
    for e in range(2):
        own[e] = jnp.where(cid == 0, img[e, :, 0:BLK], img[e, :, BLK:N_IMG])
    for stage in [None] + list(range(NC)):
        for c in received(stage):
            c.wait_send()
    swap.wait()
    for e in range(2):
        lo = e * 2 * BLK
        theirs = jnp.concatenate([yrecv[:, lo:lo + BLK], yrecv[:, lo + BLK:lo + 2 * BLK]], axis=0)
        out_ref[e] = ((own[e] + theirs) * dd[...]).T


def solution(mesh):
    t2c, t3ac, t3bc = constants()

    def local_part(kspace, weight_row, weight_col, grid_row, grid_col, valid_count, coil_maps, deapod):
        any_spec = pl.BlockSpec(memory_space=pl.ANY)
        dma = pltpu.SemaphoreType.DMA
        return pl.pallas_call(
            body,
            out_shape=pltpu.VMEM((2, BLK, COLS), F32),
            in_specs=[any_spec] * 5 + [pl.BlockSpec(memory_space=pltpu.HBM)] + [any_spec] * 5,
            out_specs=pl.BlockSpec(memory_space=pltpu.VMEM),
            scratch_shapes=[
                pltpu.VMEM((2 * NC, SLOTS), F32),
                pltpu.VMEM((4, SLOTS), F32),
                pltpu.VMEM((4, SLOTS), F32),
                pltpu.VMEM((1, SLOTS), jnp.int32),
                pltpu.VMEM((1, SLOTS), jnp.int32),
                pltpu.SMEM((1, 1), jnp.int32),
                pltpu.VMEM((2, NC, COLS, N_IMG), F32),
                pltpu.VMEM((N_IMG,), F32),
                pltpu.VMEM((1, N_IMG), F32),
                pltpu.VMEM((N_IMG, 8), F32),
                pltpu.VMEM((COLS, BLK), F32),
                pltpu.VMEM((N_GRID, HALF), BF),
                pltpu.VMEM((N_GRID, HALF), BF),
                pltpu.VMEM((168, SLOTS), F32),
                pltpu.VMEM((512, KC), BF),
                pltpu.VMEM((512, KC), BF),
                pltpu.VMEM((256, HALF), BF),
                pltpu.VMEM((256, HALF), BF),
                pltpu.VMEM((48, SLOTS), BF),
                pltpu.VMEM((N_GRID, 512), F32),
                pltpu.VMEM((N_GRID, 256), F32),
                pltpu.VMEM((N_GRID, 512), BF),
                pltpu.VMEM((N_GRID, 256), BF),
                pltpu.VMEM((ROWS, 2 * COLS, 256), BF),
                pltpu.VMEM((ROWS, 2 * COLS, 256), BF),
                pltpu.VMEM((NC, ROWS, 2 * COLS, 128), BF),
                pltpu.VMEM((NC, ROWS, 2 * COLS, 128), BF),
                pltpu.VMEM((48, N_GRID), F32),
                pltpu.VMEM((48, N_GRID), F32),
                pltpu.VMEM((N_GRID, 128), F32),
                pltpu.VMEM((ROWS, 2, COLS, N_GRID), BF),
                pltpu.VMEM((ROWS, 128, 2 * LANES), BF),
                pltpu.VMEM((2, ROWS * B_ROWS, 2 * LANES), BF),
                pltpu.VMEM((NC, COLS, 2 * LANES), F32),
                pltpu.VMEM((2, COLS, N_IMG), F32),
                pltpu.VMEM((2, COLS, BLK), F32),
                pltpu.VMEM((COLS // 2, 4 * BLK), F32),
                pltpu.VMEM((COLS // 2, 4 * BLK), F32),
                dma((7,)), dma((19,)), dma((9, 3)), dma((9, 3)), dma((2,)), dma((2,)), dma, dma,
            ],
            compiler_params=pltpu.CompilerParams(collective_id=0, has_side_effects=True, vmem_limit_bytes=60 * 1024 * 1024),
            name='nufft_adjoint',
        )(kspace, weight_row, weight_col, grid_row.reshape(1, SLOTS), grid_col.reshape(1, SLOTS), valid_count.reshape(1, 1),
          jnp.swapaxes(coil_maps, 2, 3), deapod, jnp.asarray(t2c), jnp.asarray(t3ac), jnp.asarray(t3bc))

    spec_samples = P(None, 'coil', ('slab', 'rows'))
    spec_weights = P(None, ('slab', 'rows'))
    spec_index = P(('slab', 'rows'))
    return jax.shard_map(local_part, mesh=mesh, in_specs=(spec_samples, spec_weights, spec_weights, spec_index, spec_index, spec_index, P(None, 'coil', 'slab', 'rows'), P()), out_specs=P(None, ('slab', 'coil'), 'rows'), check_vma=False)
```

```python
import functools
import numpy as np
import jax
import jax.numpy as jnp
from jax import lax
from jax.experimental import pallas as pl
from jax.experimental.pallas import tpu as pltpu
from jax.sharding import PartitionSpec as P

MESH = pl.DeviceIdType.MESH
BF = jnp.bfloat16
F32 = jnp.float32

N_IMG = 320
N_GRID = 640
ROWS = 4
BLK = 160
COLS = 80
NC = 8
SLOTS = 5120
KC = 1280
NK = SLOTS // KC
LANES = 384
HALF = SLOTS // 2
LATE = 1
W = 256
B_FIRST = 64
B_ROWS = 32


def row_order():
    pos = np.arange(128)
    rows = pos + np.where(pos >= B_FIRST, B_ROWS, 0)
    rows[126], rows[16] = 16, 158
    rows[127], rows[32] = 32, 159
    return rows


def constants():
    k = np.arange(N_GRID)
    j = np.arange(N_IMG)
    ang = np.mod((k[:, None] - N_IMG) * (j[None, :] - N_IMG // 2), N_GRID) * (2.0 * np.pi / N_GRID)
    cos_t = np.cos(ang)
    sin_t = np.sin(ang)
    lanes = np.full((LANES,), -1)
    lanes[0:N_IMG] = np.arange(N_IMG)
    used = (lanes >= 0)[None, :]
    src = np.maximum(lanes, 0)
    pick = lambda t: np.where(used, t[:, src], 0.0)
    base = np.arange(ROWS)[:, None] * BLK
    ra = (base + row_order()[None, :]).reshape(-1)
    rb = (base + B_FIRST + np.arange(B_ROWS)[None, :]).reshape(-1)
    bf = jnp.bfloat16
    t3a = np.stack([pick(cos_t)[ra], pick(sin_t)[ra]]).reshape(2, ROWS, 128, LANES).astype(bf)
    t3b = np.stack([pick(cos_t)[rb], pick(sin_t)[rb]]).reshape(2, ROWS * B_ROWS, LANES).astype(bf)
    t2 = np.stack([cos_t.T, sin_t.T]).reshape(2, ROWS, COLS, N_GRID).astype(bf)
    return t2, t3a, t3b


def body(y_h, wr_h, wc_h, gr_h, gc_h, vc, s_h, d_h, t2_h, t3a_h, t3b_h, out_ref,
         y, wr, wc, gr, gc, s_v, din, drow, dcol, dd, rt0, rt1, wd, lb0, lb1, la0, la1, lh, accb, acc, gbb, gb,
         hbufb, recvb, hbuf, recv,
         hs, hr, hrt, t2, t3a, t3b, ib, img, own, ysend, yrecv,
         in_sem, tab_sem, send_sem, recv_sem, hsend_sem, hrecv_sem, ysend_sem, yrecv_sem):
    rts = (rt0, rt1)
    lefts_b = (lb0, lb1)
    lefts = (la0, la1)
    me = lax.axis_index('rows')
    cid = lax.axis_index('coil')
    nxt = lax.rem(me + 1, ROWS)
    prv = lax.rem(me + ROWS - 1, ROWS)
    other = 1 - cid

    ins = [pltpu.make_async_copy(a, b, in_sem.at[n]) for n, (a, b) in enumerate(
        ((gc_h, gc), (wc_h, wc), (gr_h, gr), (wr_h, wr), (y_h.at[0], y.at[0:8]), (y_h.at[1], y.at[8:16])))]
    for c in ins:
        c.start()
    tabs = [(t2_h.at[0], t2.at[:, 0]), (t2_h.at[1], t2.at[:, 1])]
    for g in range(3):
        src = slice(g * 128, g * 128 + 128)
        re = slice(g * 256, g * 256 + 128)
        im = slice(g * 256 + 128, g * 256 + 256)
        tabs += [
            (t3b_h.at[0, :, src], t3b.at[0, :, re]),
            (t3b_h.at[1, :, src], t3b.at[0, :, im]),
            (t3b_h.at[0, :, src], t3b.at[1, :, im]),
            (t3a_h.at[0, :, :, src], t3a.at[:, :, re]),
            (t3a_h.at[1, :, :, src], t3a.at[:, :, im]),
        ]
    tabs += [(s_h, s_v), (d_h, din)]
    tabs = [pltpu.make_async_copy(a, b, tab_sem.at[n]) for n, (a, b) in enumerate(tabs)]
    barrier = pltpu.get_barrier_semaphore()
    for d in range(1, ROWS):
        pl.semaphore_signal(barrier, inc=1, device_id={'rows': lax.rem(me + d, ROWS)}, device_id_type=MESH)
    pl.semaphore_signal(barrier, inc=1, device_id={'coil': other}, device_id_type=MESH)
    for c in ins:
        c.wait()
    for c in tabs:
        c.start()
    pl.semaphore_wait(barrier, 4)

    def build_wd(lo, groups):
        sl = pl.ds(lo, W)
        keep = (lax.broadcasted_iota(jnp.int32, (1, W), 1) + lo < vc[0]).astype(F32)
        start = gr[:, sl] - me * BLK - 2
        ids = lax.broadcasted_iota(jnp.int32, (8, W), 0)
        taps = [jnp.broadcast_to(wr[a:a + 1, sl] * keep, (8, W)) for a in range(4)]
        group = jnp.broadcast_to(lax.shift_right_arithmetic(start + 8, 3) - 1, (8, W))
        within = jnp.broadcast_to(start + 8 & 7, (8, W))
        head = jnp.zeros((8, W), F32)
        over = jnp.zeros((8, W), F32)
        for a in range(4):
            head = jnp.where(ids == within + a, taps[a], head)
            over = jnp.where(ids == within + (a - 8), taps[a], over)

        def rows_of(n):
            return jnp.where(group == n, head, jnp.where(group == n - 1, over, 0.0))

        for n in groups:
            if n < 16:
                w = rows_of(n + (B_ROWS // 8 if n * 8 >= B_FIRST else 0))
            elif n < 20:
                w = rows_of(n - 16 + B_FIRST // 8)
            else:
                w = jnp.where(ids == 0, rows_of(BLK // 8), pltpu.roll(rows_of(-1), 3, 0))
            wd[n * 8:n * 8 + 8, sl] = w
        if 15 in groups:
            for p, v in ((126, 16), (127, 32)):
                one, two = wd[p:p + 1, sl], wd[v:v + 1, sl]
                wd[p:p + 1, sl] = two
                wd[v:v + 1, sl] = one

    def build_rt(lo):
        sl = pl.ds(lo, W)
        k, off = lo // HALF, lo % HALF
        start = gc[:, sl] - 2
        start = jnp.where(start < 0, start + N_GRID, start)
        group = lax.shift_right_arithmetic(start, 4)
        after = jnp.where(group == N_GRID // 16 - 1, 0, group + 1)
        group = jnp.broadcast_to(group, (16, W)).astype(jnp.int16)
        after = jnp.broadcast_to(after, (16, W)).astype(jnp.int16)
        within = jnp.broadcast_to(start & 15, (16, W))
        ids = lax.broadcasted_iota(jnp.int16, (16, W), 0)
        head = jnp.zeros((16, W), BF)
        over = jnp.zeros((16, W), BF)
        for b in range(4):
            v = jnp.broadcast_to(wc[b:b + 1, sl], (16, W)).astype(BF)
            head = jnp.where(ids == (within + b).astype(jnp.int16), v, head)
            over = jnp.where(ids == (within + (b - 16)).astype(jnp.int16), v, over)
        zero = jnp.zeros((16, W), BF)
        for n in range(N_GRID // 16):
            w = jnp.where(group == jnp.int16(n), head, jnp.where(after == jnp.int16(n), over, zero))
            rts[k][n * 16:(n + 1) * 16, off:off + W] = w

    def build_left_b(k, off):
        sl = pl.ds(k * KC + off, W)
        w = wd[128:160, sl]
        for q in range(2):
            for c in range(NC):
                lo = q * 256 + c * 32
                lefts_b[k % 2][lo:lo + 32, off:off + W] = (y[q * 8 + c:q * 8 + c + 1, sl] * w).astype(BF)

    def build_halo(lo):
        sl = pl.ds(lo, W)
        for h in range(3):
            lh[h * 16:h * 16 + 16, sl] = (y[:, sl] * wd[160 + h:161 + h, sl]).astype(BF)

    def left_a_piece(c, lo):
        k, off = lo // HALF, lo % HALF
        sl = pl.ds(lo, W)
        rows = [jnp.broadcast_to(y[pl.ds(q * 8 + c, 1), sl], (16, W)) for q in range(2)]
        for n in range(8):
            w = wd[n * 16:n * 16 + 16, sl]
            for q, row in enumerate(rows):
                lefts[k][q * 128 + n * 16:q * 128 + n * 16 + 16, off:off + W] = (row * w).astype(BF)

    def build_left_a(c, k):
        for off in range(0, HALF, W):
            left_a_piece(c, k * HALF + off)

    def nt(a, b):
        return lax.dot_general(a, b, (((1,), (1,)), ((), ())), preferred_element_type=F32)

    def exchange(stage):
        if stage is None:
            src, dst, idx = hbufb, recvb, NC
        else:
            src, dst, idx = hbuf.at[stage], recv.at[stage], stage
        return [pltpu.make_async_remote_copy(
            src_ref=src.at[lax.rem(me + d, ROWS)], dst_ref=dst.at[me],
            send_sem=send_sem.at[idx, d - 1], recv_sem=recv_sem.at[idx, 3 - d],
            device_id={'rows': lax.rem(me + d, ROWS)}, device_id_type=MESH) for d in (1, 2, 3)]

    def received(stage):
        if stage is None:
            src, dst, idx = hbufb, recvb, NC
        else:
            src, dst, idx = hbuf.at[stage], recv.at[stage], stage
        return [pltpu.make_async_remote_copy(
            src_ref=src.at[0], dst_ref=dst.at[lax.rem(me + d, ROWS)],
            send_sem=send_sem.at[idx, d - 1], recv_sem=recv_sem.at[idx, d - 1],
            device_id={'rows': lax.rem(me + d, ROWS)}, device_id_type=MESH) for d in (1, 2, 3)]

    def transform(stage):
        g_ref, h_ref, r_ref = (gbb, hbufb, recvb) if stage is None else (gb, hbuf.at[stage], recv.at[stage])
        n = g_ref.shape[1] // 2
        for h in range(2):
            table = t2[2 * h:2 * h + 2].reshape(N_IMG, N_GRID)
            with_re = jnp.dot(table, g_ref[:, 0:n], preferred_element_type=F32) if n == 256 else None
            with_im = jnp.dot(table, g_ref[:, n:], preferred_element_type=F32) if n == 256 else None
            if n < 256:
                both = jnp.dot(table, g_ref[...], preferred_element_type=F32)
                with_re, with_im = both[:, 0:n], both[:, n:]
            for p in range(2):
                lo = p * 2 * COLS
                mid = lo + COLS
                end = mid + COLS
                h_ref[2 * h + p, 0:COLS] = (with_re[lo:mid] - with_im[mid:end]).astype(BF)
                h_ref[2 * h + p, COLS:] = (with_re[mid:end] + with_im[lo:mid]).astype(BF)

    def send(stage):
        h_ref, r_ref = (hbufb, recvb) if stage is None else (hbuf.at[stage], recv.at[stage])
        for c in exchange(stage):
            c.start()
        r_ref[me] = h_ref[me]

    parts = [(0, 0, 256), (0, 256, KC - 256)] + [(k, 0, KC) for k in range(1, NK)]

    def build_first(k, off, size):
        for o in range(off, off + size, W):
            build_rt(k * KC + o)
            build_wd(k * KC + o, (16, 17, 18, 19, 20))
            build_left_b(k, o)
            build_halo(k * KC + o)

    def first_stage(n):
        k, off, size = parts[n]
        lo = (k % 2) * KC + off
        for q in range(2):
            cs = slice(q * 256, q * 256 + 256)
            part = nt(rts[k // 2][:, lo:lo + size], lefts_b[k % 2][cs, off:off + size])
            if n == 0:
                accb[:, cs] = part
            elif n + 1 < len(parts):
                accb[:, cs] += part
            else:
                gbb[:, cs] = (accb[:, cs] + part).astype(BF)

    def halo(k):
        lo = (k % 2) * KC
        for h in range(2):
            rows = slice(h * 320, h * 320 + 320)
            part = nt(rts[k // 2][rows, lo:lo + KC], lh[:, k * KC:(k + 1) * KC])
            hrt[rows, 0:48] = part if k == 0 else hrt[rows, 0:48] + part

    build_first(*parts[0])
    for n in range(len(parts) - 1):
        if n + LATE < len(parts):
            first_stage(n)
        if n > 0:
            halo(parts[n][0])
        build_first(*parts[n + 1])
    halo(NK - 1)
    for lo in range(0, HALF, W):
        build_wd(lo, range(16))
        left_a_piece(0, lo)
    hs[...] = hrt[...].T[0:48]
    to_next = pltpu.make_async_remote_copy(
        src_ref=hs.at[0:16], dst_ref=hr.at[0:16], send_sem=hsend_sem.at[0], recv_sem=hrecv_sem.at[0],
        device_id={'rows': nxt}, device_id_type=MESH)
    to_prev = pltpu.make_async_remote_copy(
        src_ref=hs.at[16:48], dst_ref=hr.at[16:48], send_sem=hsend_sem.at[1], recv_sem=hrecv_sem.at[1],
        device_id={'rows': prv}, device_id_type=MESH)
    to_next.start()
    to_prev.start()
    for c in tabs:
        c.wait()

    for n in range(len(parts) - LATE, len(parts)):
        first_stage(n)
    for g in range(3):
        t3b[1, :, g * 256:g * 256 + 128] = -t3b[0, :, g * 256 + 128:g * 256 + 256]
    drow[...] = din[...].reshape(1, N_IMG)
    dcol[...] = jnp.broadcast_to(din[...].reshape(1, N_IMG), (8, N_IMG)).T
    mine = jnp.where(cid == 0, drow[:, 0:BLK], drow[:, BLK:])
    dd[...] = dcol[pl.ds(pl.multiple_of(me * COLS, COLS), COLS), 0:1] * mine
    img[...] = jnp.zeros_like(img)
    transform(None)
    send(None)

    def spread_head(c, first=False):
        for h in range(2):
            rows = slice(h * 320, h * 320 + 320)
            acc[rows, :] = nt(rts[0][rows, :], lefts[0][...])
        for lo in range(HALF, SLOTS, W):
            if first:
                build_wd(lo, range(16))
            left_a_piece(c, lo)

    lane = lax.broadcasted_iota(jnp.int32, (1, 128), 1)
    edge = (lane == 0) | (lane == 16) | (lane == 32)

    def spread_tail(c):
        for h in range(2):
            rows = slice(h * 320, h * 320 + 320)
            part = nt(rts[1][rows, :], lefts[1][...])
            for q in range(2):
                cs = slice(q * 128, q * 128 + 128)
                rolled = pltpu.roll(hrt[rows, :], 128 - (q * 8 + c), 1)
                gb[rows, cs] = (acc[rows, cs] + part[:, cs] + jnp.where(edge, rolled, 0.0)).astype(BF)

    def image_first():
        for c in range(NC):
            blocks = [recvb[p, b * COLS:(b + 1) * COLS, c * 32:c * 32 + 32] for b in range(2) for p in range(ROWS)]
            lhs = jnp.concatenate(blocks, axis=1)
            ib[c] = jnp.dot(lhs, t3b[...].reshape(256, 2 * LANES), preferred_element_type=F32)

    def image_coil(c):
        lhs = jnp.concatenate([recv[c, p] for p in range(ROWS)], axis=1)
        for g in range(3):
            lanes = slice(g * 256, g * 256 + 256)
            tot = jnp.dot(lhs, t3a[:, :, lanes].reshape(4 * 128, 256), preferred_element_type=F32)
            re = ib[c, :, g * 256:g * 256 + 128] + (tot[0:COLS, 0:128] - tot[COLS:, 128:])
            im = ib[c, :, g * 256 + 128:g * 256 + 256] + (tot[0:COLS, 128:] + tot[COLS:, 0:128])
            n = min(128, N_IMG - g * 128)
            at = slice(g * 128, g * 128 + n)
            sr = s_v[0, c, :, at]
            si = s_v[1, c, :, at]
            img[0, :, at] += sr * re[:, 0:n] + si * im[:, 0:n]
            img[1, :, at] += sr * im[:, 0:n] - si * re[:, 0:n]

    spread_head(0, True)

    def advance(c):
        spread_tail(c)
        build_left_a(c + 1, 0)
        transform(c)
        spread_head(c + 1)
        send(c)

    to_next.wait()
    to_prev.wait()
    hrt[...] = jnp.concatenate([hr[...], jnp.zeros((80, N_GRID), F32)], axis=0).T
    advance(0)

    @pl.loop(1, NC - 2)
    def _(c):
        advance(c)

    c = NC - 2
    spread_tail(c)
    build_left_a(c + 1, 0)
    transform(c)
    send(c)
    spread_head(c + 1)
    spread_tail(c + 1)
    last = NC - 1
    here = me // 2

    def start(to):
        d = lax.rem(to - me + ROWS, ROWS)
        pltpu.make_async_remote_copy(
            src_ref=hbuf.at[last, to], dst_ref=recv.at[last, me],
            send_sem=send_sem.at[last, d - 1], recv_sem=recv_sem.at[last, 3 - d],
            device_id={'rows': to}, device_id_type=MESH).start()

    for chip in (1 - here, here):
        for q in range(2):
            to = 2 * chip + q
            both = jnp.dot(t2[to].reshape(2 * COLS, N_GRID), gb[...], preferred_element_type=F32)
            hbuf[last, to, 0:COLS] = (both[0:COLS, 0:128] - both[COLS:, 128:]).astype(BF)
            hbuf[last, to, COLS:] = (both[COLS:, 0:128] + both[0:COLS, 128:]).astype(BF)
        if chip is not here:
            start(2 * chip)
            start(2 * chip + 1)
    start(2 * here + 1 - lax.rem(me, 2))
    recv[last, me] = hbuf[last, me]

    for c in received(None):
        c.wait_recv()
    image_first()

    @pl.loop(0, NC)
    def _(c):
        for x in received(c):
            x.wait_recv()
        image_coil(c)

    halves = [jnp.where(cid == 0, img[e, :, BLK:N_IMG], img[e, :, 0:BLK]) for e in range(2)]
    ysend[...] = jnp.concatenate([x[r:r + COLS // 2] for x in halves for r in (0, COLS // 2)], axis=1)
    swap = pltpu.make_async_remote_copy(
        src_ref=ysend, dst_ref=yrecv, send_sem=ysend_sem, recv_sem=yrecv_sem,
        device_id={'coil': other}, device_id_type=MESH)
    swap.start()
    for e in range(2):
        own[e] = jnp.where(cid == 0, img[e, :, 0:BLK], img[e, :, BLK:N_IMG])
    for stage in [None] + list(range(NC)):
        for c in received(stage):
            c.wait_send()
    swap.wait()
    for e in range(2):
        lo = e * 2 * BLK
        theirs = jnp.concatenate([yrecv[:, lo:lo + BLK], yrecv[:, lo + BLK:lo + 2 * BLK]], axis=0)
        out_ref[e] = ((own[e] + theirs) * dd[...]).T


def solution(mesh):
    t2c, t3ac, t3bc = constants()

    def local_part(kspace, weight_row, weight_col, grid_row, grid_col, valid_count, coil_maps, deapod):
        any_spec = pl.BlockSpec(memory_space=pl.ANY)
        dma = pltpu.SemaphoreType.DMA
        return pl.pallas_call(
            body,
            out_shape=pltpu.VMEM((2, BLK, COLS), F32),
            in_specs=[any_spec] * 5 + [pl.BlockSpec(memory_space=pltpu.SMEM)] + [any_spec] * 5,
            out_specs=pl.BlockSpec(memory_space=pltpu.VMEM),
            scratch_shapes=[
                pltpu.VMEM((2 * NC, SLOTS), F32),
                pltpu.VMEM((4, SLOTS), F32),
                pltpu.VMEM((4, SLOTS), F32),
                pltpu.VMEM((1, SLOTS), jnp.int32),
                pltpu.VMEM((1, SLOTS), jnp.int32),
                pltpu.VMEM((2, NC, COLS, N_IMG), F32),
                pltpu.VMEM((N_IMG,), F32),
                pltpu.VMEM((1, N_IMG), F32),
                pltpu.VMEM((N_IMG, 8), F32),
                pltpu.VMEM((COLS, BLK), F32),
                pltpu.VMEM((N_GRID, HALF), BF),
                pltpu.VMEM((N_GRID, HALF), BF),
                pltpu.VMEM((168, SLOTS), F32),
                pltpu.VMEM((512, KC), BF),
                pltpu.VMEM((512, KC), BF),
                pltpu.VMEM((256, HALF), BF),
                pltpu.VMEM((256, HALF), BF),
                pltpu.VMEM((48, SLOTS), BF),
                pltpu.VMEM((N_GRID, 512), F32),
                pltpu.VMEM((N_GRID, 256), F32),
                pltpu.VMEM((N_GRID, 512), BF),
                pltpu.VMEM((N_GRID, 256), BF),
                pltpu.VMEM((ROWS, 2 * COLS, 256), BF),
                pltpu.VMEM((ROWS, 2 * COLS, 256), BF),
                pltpu.VMEM((NC, ROWS, 2 * COLS, 128), BF),
                pltpu.VMEM((NC, ROWS, 2 * COLS, 128), BF),
                pltpu.VMEM((48, N_GRID), F32),
                pltpu.VMEM((48, N_GRID), F32),
                pltpu.VMEM((N_GRID, 128), F32),
                pltpu.VMEM((ROWS, 2, COLS, N_GRID), BF),
                pltpu.VMEM((ROWS, 128, 2 * LANES), BF),
                pltpu.VMEM((2, ROWS * B_ROWS, 2 * LANES), BF),
                pltpu.VMEM((NC, COLS, 2 * LANES), F32),
                pltpu.VMEM((2, COLS, N_IMG), F32),
                pltpu.VMEM((2, COLS, BLK), F32),
                pltpu.VMEM((COLS // 2, 4 * BLK), F32),
                pltpu.VMEM((COLS // 2, 4 * BLK), F32),
                dma((6,)), dma((19,)), dma((9, 3)), dma((9, 3)), dma((2,)), dma((2,)), dma, dma,
            ],
            compiler_params=pltpu.CompilerParams(collective_id=0, has_side_effects=True, vmem_limit_bytes=60 * 1024 * 1024),
            name='nufft_adjoint',
        )(kspace, weight_row, weight_col, grid_row.reshape(1, SLOTS), grid_col.reshape(1, SLOTS), valid_count,
          jnp.swapaxes(coil_maps, 2, 3), deapod, jnp.asarray(t2c), jnp.asarray(t3ac), jnp.asarray(t3bc))

    spec_samples = P(None, 'coil', ('slab', 'rows'))
    spec_weights = P(None, ('slab', 'rows'))
    spec_index = P(('slab', 'rows'))
    return jax.shard_map(local_part, mesh=mesh, in_specs=(spec_samples, spec_weights, spec_weights, spec_index, spec_index, spec_index, P(None, 'coil', 'slab', 'rows'), P()), out_specs=P(None, ('slab', 'coil'), 'rows'), check_vma=False)
```

```python
import functools
import numpy as np
import jax
import jax.numpy as jnp
from jax import lax
from jax.experimental import pallas as pl
from jax.experimental.pallas import tpu as pltpu
from jax.sharding import PartitionSpec as P

MESH = pl.DeviceIdType.MESH
BF = jnp.bfloat16
F32 = jnp.float32

N_IMG = 320
N_GRID = 640
ROWS = 4
BLK = 160
COLS = 80
NC = 8
SLOTS = 5120
KC = 1280
NK = SLOTS // KC
LANES = 384
HALF = SLOTS // 2
W = 256
B_FIRST = 64
B_ROWS = 32


def row_order():
    pos = np.arange(128)
    rows = pos + np.where(pos >= B_FIRST, B_ROWS, 0)
    rows[126], rows[16] = 16, 158
    rows[127], rows[32] = 32, 159
    return rows


def constants():
    k = np.arange(N_GRID)
    j = np.arange(N_IMG)
    ang = np.mod((k[:, None] - N_IMG) * (j[None, :] - N_IMG // 2), N_GRID) * (2.0 * np.pi / N_GRID)
    cos_t = np.cos(ang)
    sin_t = np.sin(ang)
    lanes = np.full((LANES,), -1)
    lanes[0:N_IMG] = np.arange(N_IMG)
    used = (lanes >= 0)[None, :]
    src = np.maximum(lanes, 0)
    pick = lambda t: np.where(used, t[:, src], 0.0)
    base = np.arange(ROWS)[:, None] * BLK
    ra = (base + row_order()[None, :]).reshape(-1)
    rb = (base + B_FIRST + np.arange(B_ROWS)[None, :]).reshape(-1)
    bf = jnp.bfloat16
    t3a = np.stack([pick(cos_t)[ra], pick(sin_t)[ra]]).reshape(2, ROWS, 128, LANES).astype(bf)
    t3b = np.stack([pick(cos_t)[rb], pick(sin_t)[rb]]).reshape(2, ROWS * B_ROWS, LANES).astype(bf)
    t2 = np.stack([cos_t.T, sin_t.T]).reshape(2, ROWS, COLS, N_GRID).astype(bf)
    return t2, t3a, t3b


def body(y_h, wr_h, wc_h, gr_h, gc_h, vc, s_h, d_h, t2_h, t3a_h, t3b_h, out_ref,
         y, wr, wc, gr, gc, s_v, din, drow, dcol, dd, rt0, rt1, wd, lb0, lb1, la0, la1, lh, acc, gb, hbuf, recv,
         hs, hr, hrt, t2, t3a, t3b, ib, img, own, ysend, yrecv,
         in_sem, tab_sem, send_sem, recv_sem, hsend_sem, hrecv_sem, ysend_sem, yrecv_sem):
    rts = (rt0, rt1)
    lefts_b = (lb0, lb1)
    lefts = (la0, la1)
    me = lax.axis_index('rows')
    cid = lax.axis_index('coil')
    nxt = lax.rem(me + 1, ROWS)
    prv = lax.rem(me + ROWS - 1, ROWS)
    other = 1 - cid

    ins = [pltpu.make_async_copy(a, b, in_sem.at[n]) for n, (a, b) in enumerate(
        ((gc_h, gc), (wc_h, wc), (gr_h, gr), (wr_h, wr), (y_h.at[0], y.at[0:8]), (y_h.at[1], y.at[8:16])))]
    for c in ins:
        c.start()
    tabs = [(t2_h.at[0], t2.at[:, 0]), (t2_h.at[1], t2.at[:, 1])]
    for g in range(3):
        src = slice(g * 128, g * 128 + 128)
        re = slice(g * 256, g * 256 + 128)
        im = slice(g * 256 + 128, g * 256 + 256)
        tabs += [
            (t3b_h.at[0, :, src], t3b.at[0, :, re]),
            (t3b_h.at[1, :, src], t3b.at[0, :, im]),
            (t3b_h.at[0, :, src], t3b.at[1, :, im]),
            (t3a_h.at[0, :, :, src], t3a.at[:, :, re]),
            (t3a_h.at[1, :, :, src], t3a.at[:, :, im]),
        ]
    tabs += [(s_h, s_v), (d_h, din)]
    tabs = [pltpu.make_async_copy(a, b, tab_sem.at[n]) for n, (a, b) in enumerate(tabs)]
    barrier = pltpu.get_barrier_semaphore()
    for d in range(1, ROWS):
        pl.semaphore_signal(barrier, inc=1, device_id={'rows': lax.rem(me + d, ROWS)}, device_id_type=MESH)
    pl.semaphore_signal(barrier, inc=1, device_id={'coil': other}, device_id_type=MESH)
    for c in ins:
        c.wait()
    for c in tabs:
        c.start()
    pl.semaphore_wait(barrier, 4)

    def build_wd(lo, groups):
        sl = pl.ds(lo, W)
        keep = (lax.broadcasted_iota(jnp.int32, (1, W), 1) + lo < vc[0]).astype(F32)
        start = gr[:, sl] - me * BLK - 2
        ids = lax.broadcasted_iota(jnp.int32, (8, W), 0)
        taps = [jnp.broadcast_to(wr[a:a + 1, sl] * keep, (8, W)) for a in range(4)]
        group = jnp.broadcast_to(lax.shift_right_arithmetic(start + 8, 3) - 1, (8, W))
        within = jnp.broadcast_to(start + 8 & 7, (8, W))
        head = jnp.zeros((8, W), F32)
        over = jnp.zeros((8, W), F32)
        for a in range(4):
            head = jnp.where(ids == within + a, taps[a], head)
            over = jnp.where(ids == within + (a - 8), taps[a], over)

        def rows_of(n):
            return jnp.where(group == n, head, jnp.where(group == n - 1, over, 0.0))

        for n in groups:
            if n < 16:
                w = rows_of(n + (B_ROWS // 8 if n * 8 >= B_FIRST else 0))
            elif n < 20:
                w = rows_of(n - 16 + B_FIRST // 8)
            else:
                w = jnp.where(ids == 0, rows_of(BLK // 8), pltpu.roll(rows_of(-1), 3, 0))
            wd[n * 8:n * 8 + 8, sl] = w
        if 15 in groups:
            for p, v in ((126, 16), (127, 32)):
                one, two = wd[p:p + 1, sl], wd[v:v + 1, sl]
                wd[p:p + 1, sl] = two
                wd[v:v + 1, sl] = one

    def build_rt(lo):
        sl = pl.ds(lo, W)
        k, off = lo // HALF, lo % HALF
        start = gc[:, sl] - 2
        start = jnp.where(start < 0, start + N_GRID, start)
        group = lax.shift_right_arithmetic(start, 4)
        after = jnp.where(group == N_GRID // 16 - 1, 0, group + 1)
        group = jnp.broadcast_to(group, (16, W)).astype(jnp.int16)
        after = jnp.broadcast_to(after, (16, W)).astype(jnp.int16)
        within = jnp.broadcast_to(start & 15, (16, W))
        ids = lax.broadcasted_iota(jnp.int16, (16, W), 0)
        head = jnp.zeros((16, W), BF)
        over = jnp.zeros((16, W), BF)
        for b in range(4):
            v = jnp.broadcast_to(wc[b:b + 1, sl], (16, W)).astype(BF)
            head = jnp.where(ids == (within + b).astype(jnp.int16), v, head)
            over = jnp.where(ids == (within + (b - 16)).astype(jnp.int16), v, over)
        zero = jnp.zeros((16, W), BF)
        for n in range(N_GRID // 16):
            w = jnp.where(group == jnp.int16(n), head, jnp.where(after == jnp.int16(n), over, zero))
            rts[k][n * 16:(n + 1) * 16, off:off + W] = w

    def build_left_b(k, off, half):
        sl = pl.ds(k * KC + off, W)
        w = wd[128:160, sl]
        for q in range(2):
            for n in range(4):
                c = half * 4 + n
                lo = half * 256 + q * 128 + n * 32
                lefts_b[k % 2][lo:lo + 32, off:off + W] = (y[q * 8 + c:q * 8 + c + 1, sl] * w).astype(BF)

    def build_halo(lo):
        sl = pl.ds(lo, W)
        for h in range(3):
            lh[h * 16:h * 16 + 16, sl] = (y[:, sl] * wd[160 + h:161 + h, sl]).astype(BF)

    def left_a_piece(c, lo):
        k, off = lo // HALF, lo % HALF
        sl = pl.ds(lo, W)
        rows = [jnp.broadcast_to(y[pl.ds(q * 8 + c, 1), sl], (16, W)) for q in range(2)]
        for n in range(8):
            w = wd[n * 16:n * 16 + 16, sl]
            for q, row in enumerate(rows):
                lefts[k][q * 128 + n * 16:q * 128 + n * 16 + 16, off:off + W] = (row * w).astype(BF)

    def build_left_a(c, k):
        for off in range(0, HALF, W):
            left_a_piece(c, k * HALF + off)

    def nt(a, b):
        return lax.dot_general(a, b, (((1,), (1,)), ((), ())), preferred_element_type=F32)

    def exchange(stage):
        src, dst, idx = hbuf.at[stage], recv.at[stage], stage
        return [pltpu.make_async_remote_copy(
            src_ref=src.at[lax.rem(me + d, ROWS)], dst_ref=dst.at[me],
            send_sem=send_sem.at[idx, d - 1], recv_sem=recv_sem.at[idx, 3 - d],
            device_id={'rows': lax.rem(me + d, ROWS)}, device_id_type=MESH) for d in (1, 2, 3)]

    def received(stage):
        src, dst, idx = hbuf.at[stage], recv.at[stage], stage
        return [pltpu.make_async_remote_copy(
            src_ref=src.at[0], dst_ref=dst.at[lax.rem(me + d, ROWS)],
            send_sem=send_sem.at[idx, d - 1], recv_sem=recv_sem.at[idx, d - 1],
            device_id={'rows': lax.rem(me + d, ROWS)}, device_id_type=MESH) for d in (1, 2, 3)]

    def transform(stage):
        for h in range(2):
            both = jnp.dot(t2[2 * h:2 * h + 2].reshape(N_IMG, N_GRID), gb[...], preferred_element_type=F32)
            for p in range(2):
                lo = p * 2 * COLS
                mid = lo + COLS
                end = mid + COLS
                hbuf[stage, 2 * h + p, 0:COLS] = (both[lo:mid, 0:128] - both[mid:end, 128:]).astype(BF)
                hbuf[stage, 2 * h + p, COLS:] = (both[mid:end, 0:128] + both[lo:mid, 128:]).astype(BF)

    def send(stage):
        for c in exchange(stage):
            c.start()
        recv[stage, me] = hbuf[stage, me]

    parts = [(0, 0, 256), (0, 256, KC - 256)] + [(k, 0, KC) for k in range(1, NK)]

    def build_first(k, off, size):
        for o in range(off, off + size, W):
            build_rt(k * KC + o)
            build_wd(k * KC + o, (16, 17, 18, 19, 20))
            build_left_b(k, o, 0)
            build_halo(k * KC + o)

    def inner(k, off, size, half, begin, end):
        lo = (k % 2) * KC + off
        for h in range(2):
            rows = slice(h * 320, h * 320 + 320)
            part = nt(rts[k // 2][rows, lo:lo + size], lefts_b[k % 2][half * 256:half * 256 + 256, off:off + size])
            if begin:
                acc[rows, :] = part
            elif not end:
                acc[rows, :] += part
            else:
                gb[rows, :] = (acc[rows, :] + part).astype(BF)

    build_first(*parts[0])
    for n, part in enumerate(parts):
        inner(*part, 0, n == 0, n + 1 == len(parts))
        if n + 1 < len(parts):
            build_first(*parts[n + 1])
    for c in tabs:
        c.wait()
    transform(NC)
    send(NC)

    for lo in range(0, HALF, W):
        build_wd(lo, range(16))
        left_a_piece(0, lo)
    for k in range(2):
        for o in range(0, KC, W):
            build_left_b(k, o, 1)
    for h in range(2):
        rows = slice(h * 320, h * 320 + 320)
        hrt[rows, 0:48] = nt(rts[0][rows, :], lh[:, 0:HALF]) + nt(rts[1][rows, :], lh[:, HALF:])
    hs[...] = hrt[...].T[0:48]
    to_next = pltpu.make_async_remote_copy(
        src_ref=hs.at[0:16], dst_ref=hr.at[0:16], send_sem=hsend_sem.at[0], recv_sem=hrecv_sem.at[0],
        device_id={'rows': nxt}, device_id_type=MESH)
    to_prev = pltpu.make_async_remote_copy(
        src_ref=hs.at[16:48], dst_ref=hr.at[16:48], send_sem=hsend_sem.at[1], recv_sem=hrecv_sem.at[1],
        device_id={'rows': prv}, device_id_type=MESH)
    to_next.start()
    to_prev.start()
    for k in range(NK):
        inner(k, 0, KC, 1, k == 0, k + 1 == NK)
        if k + 2 < NK:
            for o in range(0, KC, W):
                build_left_b(k + 2, o, 1)
    for g in range(3):
        t3b[1, :, g * 256:g * 256 + 128] = -t3b[0, :, g * 256 + 128:g * 256 + 256]
    drow[...] = din[...].reshape(1, N_IMG)
    dcol[...] = jnp.broadcast_to(din[...].reshape(1, N_IMG), (8, N_IMG)).T
    mine = jnp.where(cid == 0, drow[:, 0:BLK], drow[:, BLK:])
    dd[...] = dcol[pl.ds(pl.multiple_of(me * COLS, COLS), COLS), 0:1] * mine
    img[...] = jnp.zeros_like(img)
    transform(NC + 1)
    send(NC + 1)

    def spread_head(c, first=False):
        for h in range(2):
            rows = slice(h * 320, h * 320 + 320)
            acc[rows, :] = nt(rts[0][rows, :], lefts[0][...])
        for lo in range(HALF, SLOTS, W):
            if first:
                build_wd(lo, range(16))
            left_a_piece(c, lo)

    lane = lax.broadcasted_iota(jnp.int32, (1, 128), 1)
    edge = (lane == 0) | (lane == 16) | (lane == 32)

    def spread_tail(c):
        for h in range(2):
            rows = slice(h * 320, h * 320 + 320)
            part = nt(rts[1][rows, :], lefts[1][...])
            for q in range(2):
                cs = slice(q * 128, q * 128 + 128)
                rolled = pltpu.roll(hrt[rows, :], 128 - (q * 8 + c), 1)
                gb[rows, cs] = (acc[rows, cs] + part[:, cs] + jnp.where(edge, rolled, 0.0)).astype(BF)

    def image_first():
        for c in range(NC):
            blocks = [recv[NC + c // 4, p, b * COLS:(b + 1) * COLS, c % 4 * 32:c % 4 * 32 + 32] for b in range(2) for p in range(ROWS)]
            lhs = jnp.concatenate(blocks, axis=1)
            ib[c] = jnp.dot(lhs, t3b[...].reshape(256, 2 * LANES), preferred_element_type=F32)

    def image_coil(c):
        lhs = jnp.concatenate([recv[c, p] for p in range(ROWS)], axis=1)
        for g in range(3):
            lanes = slice(g * 256, g * 256 + 256)
            tot = jnp.dot(lhs, t3a[:, :, lanes].reshape(4 * 128, 256), preferred_element_type=F32)
            re = ib[c, :, g * 256:g * 256 + 128] + (tot[0:COLS, 0:128] - tot[COLS:, 128:])
            im = ib[c, :, g * 256 + 128:g * 256 + 256] + (tot[0:COLS, 128:] + tot[COLS:, 0:128])
            n = min(128, N_IMG - g * 128)
            at = slice(g * 128, g * 128 + n)
            sr = s_v[0, c, :, at]
            si = s_v[1, c, :, at]
            img[0, :, at] += sr * re[:, 0:n] + si * im[:, 0:n]
            img[1, :, at] += sr * im[:, 0:n] - si * re[:, 0:n]

    spread_head(0, True)

    def advance(c):
        spread_tail(c)
        build_left_a(c + 1, 0)
        transform(c)
        spread_head(c + 1)
        send(c)

    to_next.wait()
    to_prev.wait()
    hrt[...] = jnp.concatenate([hr[...], jnp.zeros((80, N_GRID), F32)], axis=0).T
    advance(0)

    @pl.loop(1, NC - 2)
    def _(c):
        advance(c)

    c = NC - 2
    spread_tail(c)
    build_left_a(c + 1, 0)
    transform(c)
    send(c)
    spread_head(c + 1)
    spread_tail(c + 1)
    last = NC - 1
    here = me // 2

    def start(to):
        d = lax.rem(to - me + ROWS, ROWS)
        pltpu.make_async_remote_copy(
            src_ref=hbuf.at[last, to], dst_ref=recv.at[last, me],
            send_sem=send_sem.at[last, d - 1], recv_sem=recv_sem.at[last, 3 - d],
            device_id={'rows': to}, device_id_type=MESH).start()

    for chip in (1 - here, here):
        for q in range(2):
            to = 2 * chip + q
            both = jnp.dot(t2[to].reshape(2 * COLS, N_GRID), gb[...], preferred_element_type=F32)
            hbuf[last, to, 0:COLS] = (both[0:COLS, 0:128] - both[COLS:, 128:]).astype(BF)
            hbuf[last, to, COLS:] = (both[COLS:, 0:128] + both[0:COLS, 128:]).astype(BF)
        if chip is not here:
            start(2 * chip)
            start(2 * chip + 1)
    start(2 * here + 1 - lax.rem(me, 2))
    recv[last, me] = hbuf[last, me]

    for stage in (NC, NC + 1):
        for c in received(stage):
            c.wait_recv()
    image_first()

    @pl.loop(0, NC)
    def _(c):
        for x in received(c):
            x.wait_recv()
        image_coil(c)

    halves = [jnp.where(cid == 0, img[e, :, BLK:N_IMG], img[e, :, 0:BLK]) for e in range(2)]
    ysend[...] = jnp.concatenate([x[r:r + COLS // 2] for x in halves for r in (0, COLS // 2)], axis=1)
    swap = pltpu.make_async_remote_copy(
        src_ref=ysend, dst_ref=yrecv, send_sem=ysend_sem, recv_sem=yrecv_sem,
        device_id={'coil': other}, device_id_type=MESH)
    swap.start()
    for e in range(2):
        own[e] = jnp.where(cid == 0, img[e, :, 0:BLK], img[e, :, BLK:N_IMG])
    for stage in range(NC + 2):
        for c in received(stage):
            c.wait_send()
    swap.wait()
    for e in range(2):
        lo = e * 2 * BLK
        theirs = jnp.concatenate([yrecv[:, lo:lo + BLK], yrecv[:, lo + BLK:lo + 2 * BLK]], axis=0)
        out_ref[e] = ((own[e] + theirs) * dd[...]).T


def solution(mesh):
    t2c, t3ac, t3bc = constants()

    def local_part(kspace, weight_row, weight_col, grid_row, grid_col, valid_count, coil_maps, deapod):
        any_spec = pl.BlockSpec(memory_space=pl.ANY)
        dma = pltpu.SemaphoreType.DMA
        return pl.pallas_call(
            body,
            out_shape=pltpu.VMEM((2, BLK, COLS), F32),
            in_specs=[any_spec] * 5 + [pl.BlockSpec(memory_space=pltpu.SMEM)] + [any_spec] * 5,
            out_specs=pl.BlockSpec(memory_space=pltpu.VMEM),
            scratch_shapes=[
                pltpu.VMEM((2 * NC, SLOTS), F32),
                pltpu.VMEM((4, SLOTS), F32),
                pltpu.VMEM((4, SLOTS), F32),
                pltpu.VMEM((1, SLOTS), jnp.int32),
                pltpu.VMEM((1, SLOTS), jnp.int32),
                pltpu.VMEM((2, NC, COLS, N_IMG), F32),
                pltpu.VMEM((N_IMG,), F32),
                pltpu.VMEM((1, N_IMG), F32),
                pltpu.VMEM((N_IMG, 8), F32),
                pltpu.VMEM((COLS, BLK), F32),
                pltpu.VMEM((N_GRID, HALF), BF),
                pltpu.VMEM((N_GRID, HALF), BF),
                pltpu.VMEM((168, SLOTS), F32),
                pltpu.VMEM((512, KC), BF),
                pltpu.VMEM((512, KC), BF),
                pltpu.VMEM((256, HALF), BF),
                pltpu.VMEM((256, HALF), BF),
                pltpu.VMEM((48, SLOTS), BF),
                pltpu.VMEM((N_GRID, 256), F32),
                pltpu.VMEM((N_GRID, 256), BF),
                pltpu.VMEM((NC + 2, ROWS, 2 * COLS, 128), BF),
                pltpu.VMEM((NC + 2, ROWS, 2 * COLS, 128), BF),
                pltpu.VMEM((48, N_GRID), F32),
                pltpu.VMEM((48, N_GRID), F32),
                pltpu.VMEM((N_GRID, 128), F32),
                pltpu.VMEM((ROWS, 2, COLS, N_GRID), BF),
                pltpu.VMEM((ROWS, 128, 2 * LANES), BF),
                pltpu.VMEM((2, ROWS * B_ROWS, 2 * LANES), BF),
                pltpu.VMEM((NC, COLS, 2 * LANES), F32),
                pltpu.VMEM((2, COLS, N_IMG), F32),
                pltpu.VMEM((2, COLS, BLK), F32),
                pltpu.VMEM((COLS // 2, 4 * BLK), F32),
                pltpu.VMEM((COLS // 2, 4 * BLK), F32),
                dma((6,)), dma((19,)), dma((NC + 2, 3)), dma((NC + 2, 3)), dma((2,)), dma((2,)), dma, dma,
            ],
            compiler_params=pltpu.CompilerParams(collective_id=0, has_side_effects=True, vmem_limit_bytes=60 * 1024 * 1024),
            name='nufft_adjoint',
        )(kspace, weight_row, weight_col, grid_row.reshape(1, SLOTS), grid_col.reshape(1, SLOTS), valid_count,
          jnp.swapaxes(coil_maps, 2, 3), deapod, jnp.asarray(t2c), jnp.asarray(t3ac), jnp.asarray(t3bc))

    spec_samples = P(None, 'coil', ('slab', 'rows'))
    spec_weights = P(None, ('slab', 'rows'))
    spec_index = P(('slab', 'rows'))
    return jax.shard_map(local_part, mesh=mesh, in_specs=(spec_samples, spec_weights, spec_weights, spec_index, spec_index, spec_index, P(None, 'coil', 'slab', 'rows'), P()), out_specs=P(None, ('slab', 'coil'), 'rows'), check_vma=False)
```

```python
import functools
import numpy as np
import jax
import jax.numpy as jnp
from jax import lax
from jax.experimental import pallas as pl
from jax.experimental.pallas import tpu as pltpu
from jax.sharding import PartitionSpec as P

MESH = pl.DeviceIdType.MESH
BF = jnp.bfloat16
F32 = jnp.float32

N_IMG = 320
N_GRID = 640
ROWS = 4
BLK = 160
COLS = 80
NC = 8
SLOTS = 5120
KC = 1280
NK = SLOTS // KC
LANES = 384
HALF = SLOTS // 2
LATE = 1
W = 256
B_FIRST = 64
B_ROWS = 32


def row_order():
    pos = np.arange(128)
    rows = pos + np.where(pos >= B_FIRST, B_ROWS, 0)
    rows[126], rows[16] = 16, 158
    rows[127], rows[32] = 32, 159
    return rows


def constants():
    k = np.arange(N_GRID)
    j = np.arange(N_IMG)
    ang = np.mod((k[:, None] - N_IMG) * (j[None, :] - N_IMG // 2), N_GRID) * (2.0 * np.pi / N_GRID)
    cos_t = np.cos(ang)
    sin_t = np.sin(ang)
    lanes = np.full((LANES,), -1)
    lanes[0:N_IMG] = np.arange(N_IMG)
    used = (lanes >= 0)[None, :]
    src = np.maximum(lanes, 0)
    pick = lambda t: np.where(used, t[:, src], 0.0)
    base = np.arange(ROWS)[:, None] * BLK
    ra = (base + row_order()[None, :]).reshape(-1)
    rb = (base + B_FIRST + np.arange(B_ROWS)[None, :]).reshape(-1)
    bf = jnp.bfloat16
    t3a = np.stack([pick(cos_t)[ra], pick(sin_t)[ra]]).reshape(2, ROWS, 128, LANES).astype(bf)
    t3b = np.stack([pick(cos_t)[rb], pick(sin_t)[rb]]).reshape(2, ROWS * B_ROWS, LANES).astype(bf)
    t2 = np.stack([cos_t.T, sin_t.T]).reshape(2, ROWS, COLS, N_GRID).astype(bf)
    return t2, t3a, t3b


def body(y_h, wr_h, wc_h, gr_h, gc_h, vc, s_h, d_h, t2_h, t3a_h, t3b_h, out_ref,
         y, wr, wc, gr, gc, s_v, din, drow, dcol, dd, rt0, rt1, wd, lb0, lb1, la0, la1, lh, accb, acc, gbb, gb,
         hbufb, recvb, hbuf, recv,
         hs, hr, hrt, t2, t3a, t3b, ib, img, own, ysend, yrecv,
         in_sem, tab_sem, send_sem, recv_sem, hsend_sem, hrecv_sem, ysend_sem, yrecv_sem):
    rts = (rt0, rt1)
    lefts_b = (lb0, lb1)
    lefts = (la0, la1)
    me = lax.axis_index('rows')
    cid = lax.axis_index('coil')
    nxt = lax.rem(me + 1, ROWS)
    prv = lax.rem(me + ROWS - 1, ROWS)
    other = 1 - cid

    ins = [pltpu.make_async_copy(a, b, in_sem.at[n]) for n, (a, b) in enumerate(
        ((gc_h, gc), (wc_h, wc), (gr_h, gr), (wr_h, wr), (y_h.at[0], y.at[0:8]), (y_h.at[1], y.at[8:16])))]
    for c in ins:
        c.start()
    tabs = [(t2_h.at[0], t2.at[:, 0]), (t2_h.at[1], t2.at[:, 1])]
    for g in range(3):
        src = slice(g * 128, g * 128 + 128)
        re = slice(g * 256, g * 256 + 128)
        im = slice(g * 256 + 128, g * 256 + 256)
        tabs += [
            (t3b_h.at[0, :, src], t3b.at[0, :, re]),
            (t3b_h.at[1, :, src], t3b.at[0, :, im]),
            (t3b_h.at[0, :, src], t3b.at[1, :, im]),
            (t3a_h.at[0, :, :, src], t3a.at[:, :, re]),
            (t3a_h.at[1, :, :, src], t3a.at[:, :, im]),
        ]
    tabs += [(s_h, s_v), (d_h, din)]
    tabs = [pltpu.make_async_copy(a, b, tab_sem.at[n]) for n, (a, b) in enumerate(tabs)]
    barrier = pltpu.get_barrier_semaphore()
    for d in range(1, ROWS):
        pl.semaphore_signal(barrier, inc=1, device_id={'rows': lax.rem(me + d, ROWS)}, device_id_type=MESH)
    pl.semaphore_signal(barrier, inc=1, device_id={'coil': other}, device_id_type=MESH)
    for c in ins:
        c.wait()
    for c in tabs:
        c.start()
    pl.semaphore_wait(barrier, 4)

    def build_wd(lo, groups):
        sl = pl.ds(lo, W)
        keep = (lax.broadcasted_iota(jnp.int32, (1, W), 1) + lo < vc[0]).astype(F32)
        start = gr[:, sl] - me * BLK - 2
        ids = lax.broadcasted_iota(jnp.int32, (8, W), 0)
        taps = [jnp.broadcast_to(wr[a:a + 1, sl] * keep, (8, W)) for a in range(4)]
        group = jnp.broadcast_to(lax.shift_right_arithmetic(start + 8, 3) - 1, (8, W))
        within = jnp.broadcast_to(start + 8 & 7, (8, W))
        head = jnp.zeros((8, W), F32)
        over = jnp.zeros((8, W), F32)
        for a in range(4):
            head = jnp.where(ids == within + a, taps[a], head)
            over = jnp.where(ids == within + (a - 8), taps[a], over)

        def rows_of(n):
            return jnp.where(group == n, head, jnp.where(group == n - 1, over, 0.0))

        for n in groups:
            if n < 16:
                w = rows_of(n + (B_ROWS // 8 if n * 8 >= B_FIRST else 0))
            elif n < 20:
                w = rows_of(n - 16 + B_FIRST // 8)
            else:
                w = jnp.where(ids == 0, rows_of(BLK // 8), pltpu.roll(rows_of(-1), 3, 0))
            wd[n * 8:n * 8 + 8, sl] = w
        if 15 in groups:
            for p, v in ((126, 16), (127, 32)):
                one, two = wd[p:p + 1, sl], wd[v:v + 1, sl]
                wd[p:p + 1, sl] = two
                wd[v:v + 1, sl] = one

    def build_rt(lo):
        sl = pl.ds(lo, W)
        k, off = lo // HALF, lo % HALF
        start = gc[:, sl] - 2
        start = jnp.where(start < 0, start + N_GRID, start)
        group = lax.shift_right_arithmetic(start, 4)
        after = jnp.where(group == N_GRID // 16 - 1, 0, group + 1)
        group = jnp.broadcast_to(group, (16, W)).astype(jnp.int16)
        after = jnp.broadcast_to(after, (16, W)).astype(jnp.int16)
        within = jnp.broadcast_to(start & 15, (16, W))
        ids = lax.broadcasted_iota(jnp.int16, (16, W), 0)
        head = jnp.zeros((16, W), BF)
        over = jnp.zeros((16, W), BF)
        for b in range(4):
            v = jnp.broadcast_to(wc[b:b + 1, sl], (16, W)).astype(BF)
            head = jnp.where(ids == (within + b).astype(jnp.int16), v, head)
            over = jnp.where(ids == (within + (b - 16)).astype(jnp.int16), v, over)
        zero = jnp.zeros((16, W), BF)
        for n in range(N_GRID // 16):
            w = jnp.where(group == jnp.int16(n), head, jnp.where(after == jnp.int16(n), over, zero))
            rts[k][n * 16:(n + 1) * 16, off:off + W] = w

    def build_left_b(k, off):
        sl = pl.ds(k * KC + off, W)
        w = wd[128:160, sl]
        for q in range(2):
            for c in range(NC):
                lo = q * 256 + c * 32
                lefts_b[k % 2][lo:lo + 32, off:off + W] = (y[q * 8 + c:q * 8 + c + 1, sl] * w).astype(BF)

    def build_halo(lo):
        sl = pl.ds(lo, W)
        for h in range(3):
            lh[h * 16:h * 16 + 16, sl] = (y[:, sl] * wd[160 + h:161 + h, sl]).astype(BF)

    def left_a_piece(c, lo):
        k, off = lo // HALF, lo % HALF
        sl = pl.ds(lo, W)
        rows = [jnp.broadcast_to(y[pl.ds(q * 8 + c, 1), sl], (16, W)) for q in range(2)]
        for n in range(8):
            w = wd[n * 16:n * 16 + 16, sl]
            for q, row in enumerate(rows):
                lefts[k][q * 128 + n * 16:q * 128 + n * 16 + 16, off:off + W] = (row * w).astype(BF)

    def build_left_a(c, k):
        for off in range(0, HALF, W):
            left_a_piece(c, k * HALF + off)

    def nt(a, b):
        return lax.dot_general(a, b, (((1,), (1,)), ((), ())), preferred_element_type=F32)

    def exchange(stage):
        if stage is None:
            src, dst, idx = hbufb, recvb, NC
        else:
            src, dst, idx = hbuf.at[stage], recv.at[stage], stage
        return [pltpu.make_async_remote_copy(
            src_ref=src.at[lax.rem(me + d, ROWS)], dst_ref=dst.at[me],
            send_sem=send_sem.at[idx, d - 1], recv_sem=recv_sem.at[idx, 3 - d],
            device_id={'rows': lax.rem(me + d, ROWS)}, device_id_type=MESH) for d in (2, 1, 3)]

    def received(stage):
        if stage is None:
            src, dst, idx = hbufb, recvb, NC
        else:
            src, dst, idx = hbuf.at[stage], recv.at[stage], stage
        return [pltpu.make_async_remote_copy(
            src_ref=src.at[0], dst_ref=dst.at[lax.rem(me + d, ROWS)],
            send_sem=send_sem.at[idx, d - 1], recv_sem=recv_sem.at[idx, d - 1],
            device_id={'rows': lax.rem(me + d, ROWS)}, device_id_type=MESH) for d in (1, 2, 3)]

    def transform(stage):
        g_ref, h_ref, r_ref = (gbb, hbufb, recvb) if stage is None else (gb, hbuf.at[stage], recv.at[stage])
        n = g_ref.shape[1] // 2
        for h in range(2):
            table = t2[2 * h:2 * h + 2].reshape(N_IMG, N_GRID)
            with_re = jnp.dot(table, g_ref[:, 0:n], preferred_element_type=F32) if n == 256 else None
            with_im = jnp.dot(table, g_ref[:, n:], preferred_element_type=F32) if n == 256 else None
            if n < 256:
                both = jnp.dot(table, g_ref[...], preferred_element_type=F32)
                with_re, with_im = both[:, 0:n], both[:, n:]
            for p in range(2):
                lo = p * 2 * COLS
                mid = lo + COLS
                end = mid + COLS
                h_ref[2 * h + p, 0:COLS] = (with_re[lo:mid] - with_im[mid:end]).astype(BF)
                h_ref[2 * h + p, COLS:] = (with_re[mid:end] + with_im[lo:mid]).astype(BF)

    def send(stage):
        h_ref, r_ref = (hbufb, recvb) if stage is None else (hbuf.at[stage], recv.at[stage])
        for c in exchange(stage):
            c.start()
        r_ref[me] = h_ref[me]

    parts = [(0, 0, 256), (0, 256, KC - 256)] + [(k, 0, KC) for k in range(1, NK)]

    def build_first(k, off, size):
        for o in range(off, off + size, W):
            build_rt(k * KC + o)
            build_wd(k * KC + o, (16, 17, 18, 19, 20))
            build_left_b(k, o)
            build_halo(k * KC + o)

    def first_stage(n):
        k, off, size = parts[n]
        lo = (k % 2) * KC + off
        for q in range(2):
            cs = slice(q * 256, q * 256 + 256)
            part = nt(rts[k // 2][:, lo:lo + size], lefts_b[k % 2][cs, off:off + size])
            if n == 0:
                accb[:, cs] = part
            elif n + 1 < len(parts):
                accb[:, cs] += part
            else:
                gbb[:, cs] = (accb[:, cs] + part).astype(BF)

    def halo(k):
        lo = (k % 2) * KC
        for h in range(2):
            rows = slice(h * 320, h * 320 + 320)
            part = nt(rts[k // 2][rows, lo:lo + KC], lh[:, k * KC:(k + 1) * KC])
            hrt[rows, 0:48] = part if k == 0 else hrt[rows, 0:48] + part

    build_first(*parts[0])
    for n in range(len(parts) - 1):
        if n + LATE < len(parts):
            first_stage(n)
        if n > 0:
            halo(parts[n][0])
        build_first(*parts[n + 1])
    halo(NK - 1)
    for lo in range(0, HALF, W):
        build_wd(lo, range(16))
        left_a_piece(0, lo)
    hs[...] = hrt[...].T[0:48]
    to_next = pltpu.make_async_remote_copy(
        src_ref=hs.at[0:16], dst_ref=hr.at[0:16], send_sem=hsend_sem.at[0], recv_sem=hrecv_sem.at[0],
        device_id={'rows': nxt}, device_id_type=MESH)
    to_prev = pltpu.make_async_remote_copy(
        src_ref=hs.at[16:48], dst_ref=hr.at[16:48], send_sem=hsend_sem.at[1], recv_sem=hrecv_sem.at[1],
        device_id={'rows': prv}, device_id_type=MESH)
    to_next.start()
    to_prev.start()
    for c in tabs[:2]:
        c.wait()

    for n in range(len(parts) - LATE, len(parts)):
        first_stage(n)
    transform(None)
    send(None)

    def spread_head(c, first=False):
        for h in range(2):
            rows = slice(h * 320, h * 320 + 320)
            acc[rows, :] = nt(rts[0][rows, :], lefts[0][...])
        for lo in range(HALF, SLOTS, W):
            if first:
                build_wd(lo, range(16))
            left_a_piece(c, lo)

    lane = lax.broadcasted_iota(jnp.int32, (1, 128), 1)
    edge = (lane == 0) | (lane == 16) | (lane == 32)

    def spread_tail(c):
        for h in range(2):
            rows = slice(h * 320, h * 320 + 320)
            part = nt(rts[1][rows, :], lefts[1][...])
            for q in range(2):
                cs = slice(q * 128, q * 128 + 128)
                rolled = pltpu.roll(hrt[rows, :], 128 - (q * 8 + c), 1)
                gb[rows, cs] = (acc[rows, cs] + part[:, cs] + jnp.where(edge, rolled, 0.0)).astype(BF)

    def image_first():
        for c in range(NC):
            blocks = [recvb[p, b * COLS:(b + 1) * COLS, c * 32:c * 32 + 32] for b in range(2) for p in range(ROWS)]
            lhs = jnp.concatenate(blocks, axis=1)
            ib[c] = jnp.dot(lhs, t3b[...].reshape(256, 2 * LANES), preferred_element_type=F32)

    def image_coil(c):
        lhs = jnp.concatenate([recv[c, p] for p in range(ROWS)], axis=1)
        for g in range(3):
            lanes = slice(g * 256, g * 256 + 256)
            tot = jnp.dot(lhs, t3a[:, :, lanes].reshape(4 * 128, 256), preferred_element_type=F32)
            re = ib[c, :, g * 256:g * 256 + 128] + (tot[0:COLS, 0:128] - tot[COLS:, 128:])
            im = ib[c, :, g * 256 + 128:g * 256 + 256] + (tot[0:COLS, 128:] + tot[COLS:, 0:128])
            n = min(128, N_IMG - g * 128)
            at = slice(g * 128, g * 128 + n)
            sr = s_v[0, c, :, at]
            si = s_v[1, c, :, at]
            img[0, :, at] += sr * re[:, 0:n] + si * im[:, 0:n]
            img[1, :, at] += sr * im[:, 0:n] - si * re[:, 0:n]

    spread_head(0, True)

    def advance(c):
        spread_tail(c)
        build_left_a(c + 1, 0)
        transform(c)
        spread_head(c + 1)
        send(c)

    to_next.wait()
    to_prev.wait()
    hrt[...] = jnp.concatenate([hr[...], jnp.zeros((80, N_GRID), F32)], axis=0).T
    advance(0)

    @pl.loop(1, NC - 2)
    def _(c):
        advance(c)

    c = NC - 2
    spread_tail(c)
    build_left_a(c + 1, 0)
    transform(c)
    send(c)
    spread_head(c + 1)
    spread_tail(c + 1)
    last = NC - 1
    here = me // 2

    def start(to):
        d = lax.rem(to - me + ROWS, ROWS)
        pltpu.make_async_remote_copy(
            src_ref=hbuf.at[last, to], dst_ref=recv.at[last, me],
            send_sem=send_sem.at[last, d - 1], recv_sem=recv_sem.at[last, 3 - d],
            device_id={'rows': to}, device_id_type=MESH).start()

    for chip in (1 - here, here):
        for q in range(2):
            to = 2 * chip + q
            both = jnp.dot(t2[to].reshape(2 * COLS, N_GRID), gb[...], preferred_element_type=F32)
            hbuf[last, to, 0:COLS] = (both[0:COLS, 0:128] - both[COLS:, 128:]).astype(BF)
            hbuf[last, to, COLS:] = (both[COLS:, 0:128] + both[0:COLS, 128:]).astype(BF)
        if chip is not here:
            start(2 * chip)
            start(2 * chip + 1)
    start(2 * here + 1 - lax.rem(me, 2))
    recv[last, me] = hbuf[last, me]

    for c in tabs[2:]:
        c.wait()
    for g in range(3):
        t3b[1, :, g * 256:g * 256 + 128] = -t3b[0, :, g * 256 + 128:g * 256 + 256]
    drow[...] = din[...].reshape(1, N_IMG)
    dcol[...] = jnp.broadcast_to(din[...].reshape(1, N_IMG), (8, N_IMG)).T
    mine = jnp.where(cid == 0, drow[:, 0:BLK], drow[:, BLK:])
    dd[...] = dcol[pl.ds(pl.multiple_of(me * COLS, COLS), COLS), 0:1] * mine
    img[...] = jnp.zeros_like(img)
    for c in received(None):
        c.wait_recv()
    image_first()

    @pl.loop(0, NC)
    def _(c):
        for x in received(c):
            x.wait_recv()
        image_coil(c)

    halves = [jnp.where(cid == 0, img[e, :, BLK:N_IMG], img[e, :, 0:BLK]) for e in range(2)]
    ysend[...] = jnp.concatenate([x[r:r + COLS // 2] for x in halves for r in (0, COLS // 2)], axis=1)
    swap = pltpu.make_async_remote_copy(
        src_ref=ysend, dst_ref=yrecv, send_sem=ysend_sem, recv_sem=yrecv_sem,
        device_id={'coil': other}, device_id_type=MESH)
    swap.start()
    for e in range(2):
        own[e] = jnp.where(cid == 0, img[e, :, 0:BLK], img[e, :, BLK:N_IMG])
    for stage in [None] + list(range(NC)):
        for c in received(stage):
            c.wait_send()
    swap.wait()
    for e in range(2):
        lo = e * 2 * BLK
        theirs = jnp.concatenate([yrecv[:, lo:lo + BLK], yrecv[:, lo + BLK:lo + 2 * BLK]], axis=0)
        out_ref[e] = ((own[e] + theirs) * dd[...]).T


def solution(mesh):
    t2c, t3ac, t3bc = constants()

    def local_part(kspace, weight_row, weight_col, grid_row, grid_col, valid_count, coil_maps, deapod):
        any_spec = pl.BlockSpec(memory_space=pl.ANY)
        dma = pltpu.SemaphoreType.DMA
        return pl.pallas_call(
            body,
            out_shape=pltpu.VMEM((2, BLK, COLS), F32),
            in_specs=[any_spec] * 5 + [pl.BlockSpec(memory_space=pltpu.SMEM)] + [any_spec] * 5,
            out_specs=pl.BlockSpec(memory_space=pltpu.VMEM),
            scratch_shapes=[
                pltpu.VMEM((2 * NC, SLOTS), F32),
                pltpu.VMEM((4, SLOTS), F32),
                pltpu.VMEM((4, SLOTS), F32),
                pltpu.VMEM((1, SLOTS), jnp.int32),
                pltpu.VMEM((1, SLOTS), jnp.int32),
                pltpu.VMEM((2, NC, COLS, N_IMG), F32),
                pltpu.VMEM((N_IMG,), F32),
                pltpu.VMEM((1, N_IMG), F32),
                pltpu.VMEM((N_IMG, 8), F32),
                pltpu.VMEM((COLS, BLK), F32),
                pltpu.VMEM((N_GRID, HALF), BF),
                pltpu.VMEM((N_GRID, HALF), BF),
                pltpu.VMEM((168, SLOTS), F32),
                pltpu.VMEM((512, KC), BF),
                pltpu.VMEM((512, KC), BF),
                pltpu.VMEM((256, HALF), BF),
                pltpu.VMEM((256, HALF), BF),
                pltpu.VMEM((48, SLOTS), BF),
                pltpu.VMEM((N_GRID, 512), F32),
                pltpu.VMEM((N_GRID, 256), F32),
                pltpu.VMEM((N_GRID, 512), BF),
                pltpu.VMEM((N_GRID, 256), BF),
                pltpu.VMEM((ROWS, 2 * COLS, 256), BF),
                pltpu.VMEM((ROWS, 2 * COLS, 256), BF),
                pltpu.VMEM((NC, ROWS, 2 * COLS, 128), BF),
                pltpu.VMEM((NC, ROWS, 2 * COLS, 128), BF),
                pltpu.VMEM((48, N_GRID), F32),
                pltpu.VMEM((48, N_GRID), F32),
                pltpu.VMEM((N_GRID, 128), F32),
                pltpu.VMEM((ROWS, 2, COLS, N_GRID), BF),
                pltpu.VMEM((ROWS, 128, 2 * LANES), BF),
                pltpu.VMEM((2, ROWS * B_ROWS, 2 * LANES), BF),
                pltpu.VMEM((NC, COLS, 2 * LANES), F32),
                pltpu.VMEM((2, COLS, N_IMG), F32),
                pltpu.VMEM((2, COLS, BLK), F32),
                pltpu.VMEM((COLS // 2, 4 * BLK), F32),
                pltpu.VMEM((COLS // 2, 4 * BLK), F32),
                dma((6,)), dma((19,)), dma((9, 3)), dma((9, 3)), dma((2,)), dma((2,)), dma, dma,
            ],
            compiler_params=pltpu.CompilerParams(collective_id=0, has_side_effects=True, vmem_limit_bytes=60 * 1024 * 1024),
            name='nufft_adjoint',
        )(kspace, weight_row, weight_col, grid_row.reshape(1, SLOTS), grid_col.reshape(1, SLOTS), valid_count,
          jnp.swapaxes(coil_maps, 2, 3), deapod, jnp.asarray(t2c), jnp.asarray(t3ac), jnp.asarray(t3bc))

    spec_samples = P(None, 'coil', ('slab', 'rows'))
    spec_weights = P(None, ('slab', 'rows'))
    spec_index = P(('slab', 'rows'))
    return jax.shard_map(local_part, mesh=mesh, in_specs=(spec_samples, spec_weights, spec_weights, spec_index, spec_index, spec_index, P(None, 'coil', 'slab', 'rows'), P()), out_specs=P(None, ('slab', 'coil'), 'rows'), check_vma=False)
```

```python
import functools
import numpy as np
import jax
import jax.numpy as jnp
from jax import lax
from jax.experimental import pallas as pl
from jax.experimental.pallas import tpu as pltpu
from jax.sharding import PartitionSpec as P

MESH = pl.DeviceIdType.MESH
BF = jnp.bfloat16
F32 = jnp.float32

N_IMG = 320
N_GRID = 640
ROWS = 4
BLK = 160
COLS = 80
NC = 8
SLOTS = 5120
KC = 1280
NK = SLOTS // KC
LANES = 384
HALF = SLOTS // 2
LATE = 1
W = 256
B_FIRST = 64
B_ROWS = 32


def row_order():
    pos = np.arange(128)
    rows = pos + np.where(pos >= B_FIRST, B_ROWS, 0)
    rows[126], rows[16] = 16, 158
    rows[127], rows[32] = 32, 159
    return rows


def constants():
    k = np.arange(N_GRID)
    j = np.arange(N_IMG)
    ang = np.mod((k[:, None] - N_IMG) * (j[None, :] - N_IMG // 2), N_GRID) * (2.0 * np.pi / N_GRID)
    cos_t = np.cos(ang)
    sin_t = np.sin(ang)
    lanes = np.full((LANES,), -1)
    lanes[0:N_IMG] = np.arange(N_IMG)
    used = (lanes >= 0)[None, :]
    src = np.maximum(lanes, 0)
    pick = lambda t: np.where(used, t[:, src], 0.0)
    base = np.arange(ROWS)[:, None] * BLK
    ra = (base + row_order()[None, :]).reshape(-1)
    rb = (base + B_FIRST + np.arange(B_ROWS)[None, :]).reshape(-1)
    bf = jnp.bfloat16
    t3a = np.stack([pick(cos_t)[ra], pick(sin_t)[ra]]).reshape(2, ROWS, 128, LANES).astype(bf)
    t3b = np.stack([pick(cos_t)[rb], pick(sin_t)[rb]]).reshape(2, ROWS * B_ROWS, LANES).astype(bf)
    t2 = np.stack([cos_t.T, sin_t.T]).reshape(2, ROWS, COLS, N_GRID).astype(bf)
    return t2, t3a, t3b


def body(y_h, wr_h, wc_h, gr_h, gc_h, vc, s_h, d_h, t2_h, t3a_h, t3b_h, out_ref,
         y, wr, wc, gr, gc, s_v, din, drow, dcol, dd, rt0, rt1, wd, lb0, lb1, la0, la1, lh, accb, acc, gbb, gb,
         hbufb, recvb, hbuf, recv,
         hs, hr, hrt, t2, t3a, t3b, ib, img, own, ysend, yrecv,
         in_sem, tab_sem, send_sem, recv_sem, hsend_sem, hrecv_sem, ysend_sem, yrecv_sem):
    rts = (rt0, rt1)
    lefts_b = (lb0, lb1)
    lefts = (la0, la1)
    me = lax.axis_index('rows')
    cid = lax.axis_index('coil')
    nxt = lax.rem(me + 1, ROWS)
    prv = lax.rem(me + ROWS - 1, ROWS)
    other = 1 - cid

    ins = [pltpu.make_async_copy(a, b, in_sem.at[n]) for n, (a, b) in enumerate(
        ((gc_h, gc), (wc_h, wc), (gr_h, gr), (wr_h, wr), (y_h.at[0], y.at[0:8]), (y_h.at[1], y.at[8:16])))]
    for c in ins:
        c.start()
    tabs = [(t2_h.at[0], t2.at[:, 0]), (t2_h.at[1], t2.at[:, 1])]
    for g in range(3):
        src = slice(g * 128, g * 128 + 128)
        re = slice(g * 256, g * 256 + 128)
        im = slice(g * 256 + 128, g * 256 + 256)
        tabs += [
            (t3b_h.at[0, :, src], t3b.at[0, :, re]),
            (t3b_h.at[1, :, src], t3b.at[0, :, im]),
            (t3b_h.at[0, :, src], t3b.at[1, :, im]),
            (t3a_h.at[0, :, :, src], t3a.at[:, :, re]),
            (t3a_h.at[1, :, :, src], t3a.at[:, :, im]),
        ]
    tabs += [(s_h, s_v), (d_h, din)]
    tabs = [pltpu.make_async_copy(a, b, tab_sem.at[n]) for n, (a, b) in enumerate(tabs)]
    barrier = pltpu.get_barrier_semaphore()
    for d in range(1, ROWS):
        pl.semaphore_signal(barrier, inc=1, device_id={'rows': lax.rem(me + d, ROWS)}, device_id_type=MESH)
    pl.semaphore_signal(barrier, inc=1, device_id={'coil': other}, device_id_type=MESH)
    for c in ins:
        c.wait()
    for c in tabs:
        c.start()
    pl.semaphore_wait(barrier, 4)

    def build_wd(lo, groups):
        sl = pl.ds(lo, W)
        keep = (lax.broadcasted_iota(jnp.int32, (1, W), 1) + lo < vc[0]).astype(F32)
        start = gr[:, sl] - me * BLK - 2
        ids = lax.broadcasted_iota(jnp.int32, (8, W), 0)
        taps = [jnp.broadcast_to(wr[a:a + 1, sl] * keep, (8, W)) for a in range(4)]
        group = jnp.broadcast_to(lax.shift_right_arithmetic(start + 8, 3) - 1, (8, W))
        within = jnp.broadcast_to(start + 8 & 7, (8, W))
        head = jnp.zeros((8, W), F32)
        over = jnp.zeros((8, W), F32)
        for a in range(4):
            head = jnp.where(ids == within + a, taps[a], head)
            over = jnp.where(ids == within + (a - 8), taps[a], over)

        def rows_of(n):
            return jnp.where(group == n, head, jnp.where(group == n - 1, over, 0.0))

        for n in groups:
            if n < 16:
                w = rows_of(n + (B_ROWS // 8 if n * 8 >= B_FIRST else 0))
            elif n < 20:
                w = rows_of(n - 16 + B_FIRST // 8)
            else:
                w = jnp.where(ids == 0, rows_of(BLK // 8), pltpu.roll(rows_of(-1), 3, 0))
            wd[n * 8:n * 8 + 8, sl] = w
        if 15 in groups:
            for p, v in ((126, 16), (127, 32)):
                one, two = wd[p:p + 1, sl], wd[v:v + 1, sl]
                wd[p:p + 1, sl] = two
                wd[v:v + 1, sl] = one

    def build_rt(lo):
        sl = pl.ds(lo, W)
        k, off = lo // HALF, lo % HALF
        start = gc[:, sl] - 2
        start = jnp.where(start < 0, start + N_GRID, start)
        group = lax.shift_right_arithmetic(start, 4)
        after = jnp.where(group == N_GRID // 16 - 1, 0, group + 1)
        group = jnp.broadcast_to(group, (16, W)).astype(jnp.int16)
        after = jnp.broadcast_to(after, (16, W)).astype(jnp.int16)
        within = jnp.broadcast_to(start & 15, (16, W))
        ids = lax.broadcasted_iota(jnp.int16, (16, W), 0)
        head = jnp.zeros((16, W), BF)
        over = jnp.zeros((16, W), BF)
        for b in range(4):
            v = jnp.broadcast_to(wc[b:b + 1, sl], (16, W)).astype(BF)
            head = jnp.where(ids == (within + b).astype(jnp.int16), v, head)
            over = jnp.where(ids == (within + (b - 16)).astype(jnp.int16), v, over)
        zero = jnp.zeros((16, W), BF)
        for n in range(N_GRID // 16):
            w = jnp.where(group == jnp.int16(n), head, jnp.where(after == jnp.int16(n), over, zero))
            rts[k][n * 16:(n + 1) * 16, off:off + W] = w

    def build_left_b(k, off):
        sl = pl.ds(k * KC + off, W)
        w = wd[128:160, sl]
        for q in range(2):
            for c in range(NC):
                lo = q * 256 + c * 32
                lefts_b[k % 2][lo:lo + 32, off:off + W] = (y[q * 8 + c:q * 8 + c + 1, sl] * w).astype(BF)

    def build_halo(lo):
        sl = pl.ds(lo, W)
        for h in range(3):
            lh[h * 16:h * 16 + 16, sl] = (y[:, sl] * wd[160 + h:161 + h, sl]).astype(BF)

    def left_a_piece(c, lo):
        k, off = lo // HALF, lo % HALF
        sl = pl.ds(lo, W)
        rows = [jnp.broadcast_to(y[pl.ds(q * 8 + c, 1), sl], (16, W)) for q in range(2)]
        for n in range(8):
            w = wd[n * 16:n * 16 + 16, sl]
            for q, row in enumerate(rows):
                lefts[k][q * 128 + n * 16:q * 128 + n * 16 + 16, off:off + W] = (row * w).astype(BF)

    def build_left_a(c, k):
        for off in range(0, HALF, W):
            left_a_piece(c, k * HALF + off)

    def nt(a, b):
        return lax.dot_general(a, b, (((1,), (1,)), ((), ())), preferred_element_type=F32)

    def exchange(stage):
        if stage is None:
            src, dst, idx = hbufb, recvb, NC
        else:
            src, dst, idx = hbuf.at[stage], recv.at[stage], stage
        return [pltpu.make_async_remote_copy(
            src_ref=src.at[lax.rem(me + d, ROWS)], dst_ref=dst.at[me],
            send_sem=send_sem.at[idx, d - 1], recv_sem=recv_sem.at[idx, 3 - d],
            device_id={'rows': lax.rem(me + d, ROWS)}, device_id_type=MESH) for d in (2, 1, 3)]

    def received(stage):
        if stage is None:
            src, dst, idx = hbufb, recvb, NC
        else:
            src, dst, idx = hbuf.at[stage], recv.at[stage], stage
        return [pltpu.make_async_remote_copy(
            src_ref=src.at[0], dst_ref=dst.at[lax.rem(me + d, ROWS)],
            send_sem=send_sem.at[idx, d - 1], recv_sem=recv_sem.at[idx, d - 1],
            device_id={'rows': lax.rem(me + d, ROWS)}, device_id_type=MESH) for d in (1, 2, 3)]

    def transform(stage):
        g_ref, h_ref, r_ref = (gbb, hbufb, recvb) if stage is None else (gb, hbuf.at[stage], recv.at[stage])
        n = g_ref.shape[1] // 2
        for h in range(2):
            table = t2[2 * h:2 * h + 2].reshape(N_IMG, N_GRID)
            with_re = jnp.dot(table, g_ref[:, 0:n], preferred_element_type=F32) if n == 256 else None
            with_im = jnp.dot(table, g_ref[:, n:], preferred_element_type=F32) if n == 256 else None
            if n < 256:
                both = jnp.dot(table, g_ref[...], preferred_element_type=F32)
                with_re, with_im = both[:, 0:n], both[:, n:]
            for p in range(2):
                lo = p * 2 * COLS
                mid = lo + COLS
                end = mid + COLS
                h_ref[2 * h + p, 0:COLS] = (with_re[lo:mid] - with_im[mid:end]).astype(BF)
                h_ref[2 * h + p, COLS:] = (with_re[mid:end] + with_im[lo:mid]).astype(BF)

    def send(stage):
        h_ref, r_ref = (hbufb, recvb) if stage is None else (hbuf.at[stage], recv.at[stage])
        for c in exchange(stage):
            c.start()
        r_ref[me] = h_ref[me]

    parts = [(0, 0, 256), (0, 256, KC - 256)] + [(k, 0, KC) for k in range(1, NK)]

    def build_first(k, off, size):
        for o in range(off, off + size, W):
            build_rt(k * KC + o)
            build_wd(k * KC + o, (16, 17, 18, 19, 20))
            build_left_b(k, o)
            build_halo(k * KC + o)

    def first_stage(n):
        k, off, size = parts[n]
        lo = (k % 2) * KC + off
        for q in range(2):
            cs = slice(q * 256, q * 256 + 256)
            part = nt(rts[k // 2][:, lo:lo + size], lefts_b[k % 2][cs, off:off + size])
            if n == 0:
                accb[:, cs] = part
            elif n + 1 < len(parts):
                accb[:, cs] += part
            else:
                gbb[:, cs] = (accb[:, cs] + part).astype(BF)

    def halo(k):
        lo = (k % 2) * KC
        for h in range(2):
            rows = slice(h * 320, h * 320 + 320)
            part = nt(rts[k // 2][rows, lo:lo + KC], lh[:, k * KC:(k + 1) * KC])
            hrt[rows, 0:48] = part if k == 0 else hrt[rows, 0:48] + part

    build_first(*parts[0])
    for n in range(len(parts) - 1):
        if n + LATE < len(parts):
            first_stage(n)
        if n > 0:
            halo(parts[n][0])
        build_first(*parts[n + 1])
    halo(NK - 1)
    for lo in range(0, HALF, W):
        build_wd(lo, range(16))
        left_a_piece(0, lo)
    hs[...] = hrt[...].T[0:48]
    to_next = pltpu.make_async_remote_copy(
        src_ref=hs.at[0:16], dst_ref=hr.at[0:16], send_sem=hsend_sem.at[0], recv_sem=hrecv_sem.at[0],
        device_id={'rows': nxt}, device_id_type=MESH)
    to_prev = pltpu.make_async_remote_copy(
        src_ref=hs.at[16:48], dst_ref=hr.at[16:48], send_sem=hsend_sem.at[1], recv_sem=hrecv_sem.at[1],
        device_id={'rows': prv}, device_id_type=MESH)
    to_next.start()
    to_prev.start()
    for c in tabs:
        c.wait()

    for n in range(len(parts) - LATE, len(parts)):
        first_stage(n)
    for g in range(3):
        t3b[1, :, g * 256:g * 256 + 128] = -t3b[0, :, g * 256 + 128:g * 256 + 256]
    drow[...] = din[...].reshape(1, N_IMG)
    dcol[...] = jnp.broadcast_to(din[...].reshape(1, N_IMG), (8, N_IMG)).T
    mine = jnp.where(cid == 0, drow[:, 0:BLK], drow[:, BLK:])
    dd[...] = dcol[pl.ds(pl.multiple_of(me * COLS, COLS), COLS), 0:1] * mine
    img[...] = jnp.zeros_like(img)
    transform(None)
    send(None)

    def spread_head(c, first=False):
        for h in range(2):
            rows = slice(h * 320, h * 320 + 320)
            acc[rows, :] = nt(rts[0][rows, :], lefts[0][...])
        for lo in range(HALF, SLOTS, W):
            if first:
                build_wd(lo, range(16))
            left_a_piece(c, lo)

    lane = lax.broadcasted_iota(jnp.int32, (1, 128), 1)
    edge = (lane == 0) | (lane == 16) | (lane == 32)

    def spread_tail(c):
        for h in range(2):
            rows = slice(h * 320, h * 320 + 320)
            part = nt(rts[1][rows, :], lefts[1][...])
            for q in range(2):
                cs = slice(q * 128, q * 128 + 128)
                rolled = pltpu.roll(hrt[rows, :], 128 - (q * 8 + c), 1)
                gb[rows, cs] = (acc[rows, cs] + part[:, cs] + jnp.where(edge, rolled, 0.0)).astype(BF)

    def image_first():
        for c in range(NC):
            blocks = [recvb[p, b * COLS:(b + 1) * COLS, c * 32:c * 32 + 32] for b in range(2) for p in range(ROWS)]
            lhs = jnp.concatenate(blocks, axis=1)
            ib[c] = jnp.dot(lhs, t3b[...].reshape(256, 2 * LANES), preferred_element_type=F32)

    def image_coil(c):
        lhs = jnp.concatenate([recv[c, p] for p in range(ROWS)], axis=1)
        for g in range(3):
            lanes = slice(g * 256, g * 256 + 256)
            tot = jnp.dot(lhs, t3a[:, :, lanes].reshape(4 * 128, 256), preferred_element_type=F32)
            re = ib[c, :, g * 256:g * 256 + 128] + (tot[0:COLS, 0:128] - tot[COLS:, 128:])
            im = ib[c, :, g * 256 + 128:g * 256 + 256] + (tot[0:COLS, 128:] + tot[COLS:, 0:128])
            n = min(128, N_IMG - g * 128)
            at = slice(g * 128, g * 128 + n)
            sr = s_v[0, c, :, at]
            si = s_v[1, c, :, at]
            img[0, :, at] += sr * re[:, 0:n] + si * im[:, 0:n]
            img[1, :, at] += sr * im[:, 0:n] - si * re[:, 0:n]

    spread_head(0, True)

    def advance(c):
        spread_tail(c)
        build_left_a(c + 1, 0)
        transform(c)
        spread_head(c + 1)
        send(c)

    to_next.wait()
    to_prev.wait()
    hrt[...] = jnp.concatenate([hr[...], jnp.zeros((80, N_GRID), F32)], axis=0).T
    advance(0)

    @pl.loop(1, NC - 2)
    def _(c):
        advance(c)

    c = NC - 2
    spread_tail(c)
    build_left_a(c + 1, 0)
    transform(c)
    send(c)
    spread_head(c + 1)
    spread_tail(c + 1)
    transform(c + 1)
    send(c + 1)

    for c in received(None):
        c.wait_recv()
    image_first()

    @pl.loop(0, NC)
    def _(c):
        for x in received(c):
            x.wait_recv()
        image_coil(c)

    halves = [jnp.where(cid == 0, img[e, :, BLK:N_IMG], img[e, :, 0:BLK]) for e in range(2)]
    ysend[...] = jnp.concatenate([x[r:r + COLS // 2] for x in halves for r in (0, COLS // 2)], axis=1)
    swap = pltpu.make_async_remote_copy(
        src_ref=ysend, dst_ref=yrecv, send_sem=ysend_sem, recv_sem=yrecv_sem,
        device_id={'coil': other}, device_id_type=MESH)
    swap.start()
    for e in range(2):
        own[e] = jnp.where(cid == 0, img[e, :, 0:BLK], img[e, :, BLK:N_IMG])
    for stage in [None] + list(range(NC)):
        for c in received(stage):
            c.wait_send()
    swap.wait()
    for e in range(2):
        lo = e * 2 * BLK
        theirs = jnp.concatenate([yrecv[:, lo:lo + BLK], yrecv[:, lo + BLK:lo + 2 * BLK]], axis=0)
        out_ref[e] = ((own[e] + theirs) * dd[...]).T


def solution(mesh):
    t2c, t3ac, t3bc = constants()

    def local_part(kspace, weight_row, weight_col, grid_row, grid_col, valid_count, coil_maps, deapod):
        any_spec = pl.BlockSpec(memory_space=pl.ANY)
        dma = pltpu.SemaphoreType.DMA
        return pl.pallas_call(
            body,
            out_shape=pltpu.VMEM((2, BLK, COLS), F32),
            in_specs=[any_spec] * 5 + [pl.BlockSpec(memory_space=pltpu.SMEM)] + [any_spec] * 5,
            out_specs=pl.BlockSpec(memory_space=pltpu.VMEM),
            scratch_shapes=[
                pltpu.VMEM((2 * NC, SLOTS), F32),
                pltpu.VMEM((4, SLOTS), F32),
                pltpu.VMEM((4, SLOTS), F32),
                pltpu.VMEM((1, SLOTS), jnp.int32),
                pltpu.VMEM((1, SLOTS), jnp.int32),
                pltpu.VMEM((2, NC, COLS, N_IMG), F32),
                pltpu.VMEM((N_IMG,), F32),
                pltpu.VMEM((1, N_IMG), F32),
                pltpu.VMEM((N_IMG, 8), F32),
                pltpu.VMEM((COLS, BLK), F32),
                pltpu.VMEM((N_GRID, HALF), BF),
                pltpu.VMEM((N_GRID, HALF), BF),
                pltpu.VMEM((168, SLOTS), F32),
                pltpu.VMEM((512, KC), BF),
                pltpu.VMEM((512, KC), BF),
                pltpu.VMEM((256, HALF), BF),
                pltpu.VMEM((256, HALF), BF),
                pltpu.VMEM((48, SLOTS), BF),
                pltpu.VMEM((N_GRID, 512), F32),
                pltpu.VMEM((N_GRID, 256), F32),
                pltpu.VMEM((N_GRID, 512), BF),
                pltpu.VMEM((N_GRID, 256), BF),
                pltpu.VMEM((ROWS, 2 * COLS, 256), BF),
                pltpu.VMEM((ROWS, 2 * COLS, 256), BF),
                pltpu.VMEM((NC, ROWS, 2 * COLS, 128), BF),
                pltpu.VMEM((NC, ROWS, 2 * COLS, 128), BF),
                pltpu.VMEM((48, N_GRID), F32),
                pltpu.VMEM((48, N_GRID), F32),
                pltpu.VMEM((N_GRID, 128), F32),
                pltpu.VMEM((ROWS, 2, COLS, N_GRID), BF),
                pltpu.VMEM((ROWS, 128, 2 * LANES), BF),
                pltpu.VMEM((2, ROWS * B_ROWS, 2 * LANES), BF),
                pltpu.VMEM((NC, COLS, 2 * LANES), F32),
                pltpu.VMEM((2, COLS, N_IMG), F32),
                pltpu.VMEM((2, COLS, BLK), F32),
                pltpu.VMEM((COLS // 2, 4 * BLK), F32),
                pltpu.VMEM((COLS // 2, 4 * BLK), F32),
                dma((6,)), dma((19,)), dma((9, 3)), dma((9, 3)), dma((2,)), dma((2,)), dma, dma,
            ],
            compiler_params=pltpu.CompilerParams(collective_id=0, has_side_effects=True, vmem_limit_bytes=60 * 1024 * 1024),
            name='nufft_adjoint',
        )(kspace, weight_row, weight_col, grid_row.reshape(1, SLOTS), grid_col.reshape(1, SLOTS), valid_count,
          jnp.swapaxes(coil_maps, 2, 3), deapod, jnp.asarray(t2c), jnp.asarray(t3ac), jnp.asarray(t3bc))

    spec_samples = P(None, 'coil', ('slab', 'rows'))
    spec_weights = P(None, ('slab', 'rows'))
    spec_index = P(('slab', 'rows'))
    return jax.shard_map(local_part, mesh=mesh, in_specs=(spec_samples, spec_weights, spec_weights, spec_index, spec_index, spec_index, P(None, 'coil', 'slab', 'rows'), P()), out_specs=P(None, ('slab', 'coil'), 'rows'), check_vma=False)
```
